8 devices in a mesh: dp: 2 (over z, y), tp: 4 (over x, core).
Axes of the slice: x: 2, y: 2, z: 1, core: 2. Of those that a mesh axis runs over, the one named last changes fastest.
Arguments:
- x: bfloat16 [2, 128, 2560], P('dp', 'tp'), parts along dimension 0
- ln1_gamma: float32 [2560], replicated
- ln1_beta: float32 [2560], replicated
- w_qkv: bfloat16 [2560, 32, 3, 80], P(None, 'tp')
- b_qkv: float32 [32, 3, 80], P('tp')
- w_out: bfloat16 [2560, 2560], P('tp')
- b_out: float32 [2560], replicated
- ln2_gamma: float32 [2560], replicated
- ln2_beta: float32 [2560], replicated
- w_up: bfloat16 [2560, 10240], P(None, 'tp')
- b_up: float32 [10240], P('tp')
- w_down: bfloat16 [10240, 2560], P('tp')
- b_down: float32 [2560], replicated
- grad_y: bfloat16 [2, 128, 2560], P('dp', 'tp'), parts along dimension 0
Outputs:
- output 1: bfloat16 [2, 128, 2560], P('dp', 'tp'), parts along dimension 0
- output 2: bfloat16 [2, 128, 2560], P('dp', 'tp'), parts along dimension 0
- output 3: float32 [5120], P('dp'), parts along dimension 0
- output 4: float32 [5120], P('dp'), parts along dimension 0
- output 5: bfloat16 [5120, 32, 3, 80], P('dp', 'tp'), parts along dimension 0
- output 6: float32 [64, 3, 80], P(('dp', 'tp')), parts along dimension 0
- output 7: bfloat16 [5120, 2560], P(('dp', 'tp')), parts along dimension 0
- output 8: float32 [5120], P('dp'), parts along dimension 0
- output 9: float32 [5120], P('dp'), parts along dimension 0
- output 10: float32 [5120], P('dp'), parts along dimension 0
- output 11: bfloat16 [5120, 10240], P('dp', 'tp'), parts along dimension 0
- output 12: float32 [20480], P(('dp', 'tp')), parts along dimension 0
- output 13: bfloat16 [20480, 2560], P(('dp', 'tp')), parts along dimension 0
- output 14: float32 [5120], P('dp'), parts along dimension 0
There are 2 independent parts. The reference program is written for one: setup_inputs(seed, part) draws one part's arguments, and reference() takes and returns one part's arrays. A program takes and returns all parts, laid end to end along the dimension named above; an argument that names none is the same for every part.
All inputs are finite; a program needn't handle non-finite values.
Results may differ from the reference program's by a relative error of at most 0.0177361.
Values are sent between devices in bfloat16 or wider.
A program may use at most 1 GiB of HBM per device.

```python
import math
import jax
import jax.numpy as jnp
from jax import lax

BATCH = 1
SEQ = 128
D = 2560
HEADS = 32
HEAD = 80
FF = 10240
EPS = 1e-5
MASK_VALUE = -1e30


def alibi_slopes(n_heads):
    closest = 2 ** int(math.floor(math.log2(n_heads)))
    base_ratio = 2.0 ** (-8.0 / closest)
    extra_ratio = 2.0 ** (-4.0 / closest)
    remaining = min(closest, n_heads - closest)
    slopes = [base_ratio ** (i + 1) for i in range(closest)]
    slopes = slopes + [extra_ratio ** (2 * i + 1) for i in range(remaining)]
    return jnp.array(slopes, dtype=jnp.float32)


def layer_norm(values, ln_gain, ln_bias):
    row_mean = jnp.mean(values, axis=-1, keepdims=True)
    centered = values - row_mean
    variance = jnp.mean(centered * centered, axis=-1, keepdims=True)
    return centered * lax.rsqrt(variance + EPS) * ln_gain + ln_bias


def layer_forward(x, ln1_gamma, ln1_beta, w_qkv, b_qkv, w_out, b_out, ln2_gamma, ln2_beta, w_up, b_up, w_down, b_down):
    positions = jnp.arange(SEQ)
    causal = positions[None, :] <= positions[:, None]
    key_pos = positions.astype(jnp.float32)
    x_f = x.astype(jnp.float32)
    h_norm = layer_norm(x_f, ln1_gamma, ln1_beta).astype(jnp.bfloat16)
    qkv_vals = (jnp.einsum('bsd,dhte->bshte', h_norm.astype(jnp.float32), w_qkv.astype(jnp.float32)) + b_qkv).astype(jnp.bfloat16)
    per_head = jnp.moveaxis(qkv_vals, 2, 0)

    def head_attention(operands):
        head_qkv, head_slope = operands
        q_one = head_qkv[:, :, 0].astype(jnp.float32)
        k_one = head_qkv[:, :, 1].astype(jnp.float32)
        v_one = head_qkv[:, :, 2].astype(jnp.float32)
        scores = jnp.einsum('bie,bje->bij', q_one, k_one) * (HEAD ** -0.5) + head_slope * key_pos
        scores = jnp.where(causal, scores, MASK_VALUE)
        prob_bf = jax.nn.softmax(scores, axis=-1).astype(jnp.bfloat16)
        return jnp.einsum('bij,bje->bie', prob_bf.astype(jnp.float32), v_one).astype(jnp.bfloat16)

    context = lax.map(jax.checkpoint(head_attention), (per_head, alibi_slopes(HEADS)))
    context_flat = jnp.moveaxis(context, 0, 2).reshape(BATCH, SEQ, D)
    attn_out = jnp.einsum('bsc,cd->bsd', context_flat.astype(jnp.float32), w_out.astype(jnp.float32)).astype(jnp.bfloat16)
    x_mid = x_f + attn_out.astype(jnp.float32) + b_out
    g_norm = layer_norm(x_mid, ln2_gamma, ln2_beta).astype(jnp.bfloat16)
    pre_act = jnp.einsum('bsd,df->bsf', g_norm.astype(jnp.float32), w_up.astype(jnp.float32)) + b_up
    activated = jax.nn.gelu(pre_act, approximate=True).astype(jnp.bfloat16)
    mlp_out = jnp.einsum('bsf,fd->bsd', activated.astype(jnp.float32), w_down.astype(jnp.float32)).astype(jnp.bfloat16)
    return (x_mid + mlp_out.astype(jnp.float32) + b_down).astype(jnp.bfloat16)


def setup_inputs(seed: int = 0, part: int = 0) -> dict:
    key_list = jax.random.split(jax.random.key(seed), 14)

    def normal(rng_key, out_shape, std_dev):
        return std_dev * jax.random.normal(rng_key, out_shape, jnp.float32)

    return {
        'x': normal(jax.random.fold_in(key_list[0], part), (BATCH, SEQ, D), 1.0).astype(jnp.bfloat16),
        'ln1_gamma': 1.0 + normal(key_list[1], (D,), 0.2),
        'ln1_beta': normal(key_list[2], (D,), 0.2),
        'w_qkv': normal(key_list[3], (D, HEADS, 3, HEAD), D ** -0.5).astype(jnp.bfloat16),
        'b_qkv': normal(key_list[4], (HEADS, 3, HEAD), 0.5),
        'w_out': normal(key_list[5], (D, D), D ** -0.5).astype(jnp.bfloat16),
        'b_out': normal(key_list[6], (D,), 0.5),
        'ln2_gamma': 1.0 + normal(key_list[7], (D,), 0.2),
        'ln2_beta': normal(key_list[8], (D,), 0.2),
        'w_up': normal(key_list[9], (D, FF), D ** -0.5).astype(jnp.bfloat16),
        'b_up': normal(key_list[10], (FF,), 0.5),
        'w_down': normal(key_list[11], (FF, D), FF ** -0.5).astype(jnp.bfloat16),
        'b_down': normal(key_list[12], (D,), 0.5),
        'grad_y': normal(jax.random.fold_in(key_list[13], part), (BATCH, SEQ, D), 1.0).astype(jnp.bfloat16),
    }


def reference(x, ln1_gamma, ln1_beta, w_qkv, b_qkv, w_out, b_out, ln2_gamma, ln2_beta, w_up, b_up, w_down, b_down, grad_y):
    y, pullback = jax.vjp(layer_forward, x, ln1_gamma, ln1_beta, w_qkv, b_qkv, w_out, b_out, ln2_gamma, ln2_beta, w_up, b_up, w_down, b_down)
    (grad_x, grad_ln1_gamma, grad_ln1_beta, grad_w_qkv, grad_b_qkv, grad_w_out, grad_b_out,
     grad_ln2_gamma, grad_ln2_beta, grad_w_up, grad_b_up, grad_w_down, grad_b_down) = pullback(grad_y)
    return (y, grad_x, grad_ln1_gamma, grad_ln1_beta, grad_w_qkv, grad_b_qkv, grad_w_out, grad_b_out,
            grad_ln2_gamma, grad_ln2_beta, grad_w_up, grad_b_up, grad_w_down, grad_b_down)
```

```python
import functools
import math
import jax
import jax.numpy as jnp
from jax import lax
from jax.experimental import pallas as pl
from jax.experimental.pallas import tpu as pltpu
from jax.sharding import PartitionSpec as P

EPS = 1e-5
MASK_VALUE = -1e30
BF = jnp.bfloat16
F32 = jnp.float32
MESH = pl.DeviceIdType.MESH
GELU_C = math.sqrt(2.0 / math.pi)
GELU_A = 0.044715
TP = 4
NCH = 5
LANES = 128


def alibi_slopes(n_heads):
    closest = 2 ** int(math.floor(math.log2(n_heads)))
    base_ratio = 2.0 ** (-8.0 / closest)
    extra_ratio = 2.0 ** (-4.0 / closest)
    remaining = min(closest, n_heads - closest)
    slopes = [base_ratio ** (i + 1) for i in range(closest)]
    return slopes + [extra_ratio ** (2 * i + 1) for i in range(remaining)]


def dot(lhs, rhs):
    return lax.dot_general(lhs, rhs, (((1,), (0,)), ((), ())), preferred_element_type=F32)


def dot_t(lhs, rhs):
    return lax.dot_general(lhs, rhs, (((1,), (1,)), ((), ())), preferred_element_type=F32)


def layer_kernel(x_h, gy_h, wqkv_h, bqkv_h, wout_h, wup_h, wdn_h, ln1g_h, ln1b_h, ln2g_h, ln2b_h, bout_h, bdown_h, bup_h,
                 y_o, gx_o, vec_o, h_o, ga_o, dpre_o, gy_o, dqkv_o, ctx_o, gt_o, rt_o,
                 wqkv, wout, wup, wdn, bqkv, vecs, xg, gyg, h, bias, qkv, prob, probb, ctx, x1, xhat, g, gt, rt, gact, r, dpre,
                 gmid, ga, dctx, dqkv, ybuf, gxbuf, xh1, vec, part,
                 p1, rd1, s1, rs1, t1, p2, rd2, s2, rs2, t2, py, rdy, sy, rsy, ph, rdh, sh, rsh,
                 lsem, osem, ssem, rsem):
    D = x_h.shape[1]
    seq = TP * 32
    head = bqkv_h.shape[2]
    n_heads = bqkv_h.shape[1]
    cw = D // NCH
    nlc = D // LANES
    t = lax.axis_index('tp')
    core = lax.rem(t, 2)
    chip = t // 2
    sib = t + 1 - 2 * core
    cross = lax.rem(t + 2, TP)
    sibcross = lax.rem(sib + 2, TP)

    def slot(dev):
        return lax.rem(dev, 2) * 2 + dev // 2

    def rows(dev):
        return pl.ds(pl.multiple_of(slot(dev) * 32, 32), 32)

    own = rows(t)
    half = pl.ds(pl.multiple_of(core * 64, 64), 64)
    sibhalf = pl.ds(pl.multiple_of((1 - core) * 64, 64), 64)
    blk_own = pl.ds(pl.multiple_of(chip * 32, 32), 32)
    blk_cross = pl.ds(pl.multiple_of((1 - chip) * 32, 32), 32)

    counter = [0, 0, 0]

    def load(src, dst):
        k = counter[0]
        counter[0] += 1
        copy = pltpu.make_async_copy(src, dst, lsem.at[k])
        copy.start()
        return copy

    outs = []

    def store(src, dst):
        k = counter[1]
        counter[1] += 1
        copy = pltpu.make_async_copy(src, dst, osem.at[k])
        copy.start()
        outs.append(copy)

    sent = []

    def remote(src, dst, dev):
        k = counter[2]
        counter[2] += 1
        copy = pltpu.make_async_remote_copy(src_ref=src, dst_ref=dst, send_sem=ssem.at[k], recv_sem=rsem.at[k],
                                            device_id={'tp': dev}, device_id_type=MESH)
        copy.start()
        sent.append(copy)
        return copy

    def lc(c):
        return slice(c * LANES, (c + 1) * LANES)

    def ch(j):
        return slice(j * cw, (j + 1) * cw)

    lx = load(x_h, xg.at[own, :])
    lg = load(gy_h, gyg.at[own, :])
    lvec = [load(src, vecs.at[k]) for k, src in enumerate((ln1g_h, ln1b_h, ln2g_h, ln2b_h, bout_h, bdown_h, bup_h))]
    lb = load(bqkv_h, bqkv)
    lwqkv = load(wqkv_h, wqkv)
    lwout = load(wout_h, wout)
    barrier = pltpu.get_barrier_semaphore()
    for dev in (sib, cross, sibcross):
        pl.semaphore_signal(barrier, inc=1, device_id={'tp': dev}, device_id_type=MESH)
    pl.semaphore_wait(barrier, 3)
    lx.wait()
    x_to_cross = remote(xg.at[own, :], xg.at[own, :], cross)
    x_to_sib = remote(xg.at[own, :], xg.at[own, :], sib)
    lg.wait()
    gy_to_sib = remote(gyg.at[own, :], gyg.at[own, :], sib)
    lwdn = load(wdn_h, wdn)
    lwup = load(wup_h, wup)
    for copy in lvec:
        copy.wait()

    def ln_block(rr, n, src, gain, shift, dst):
        acc = jnp.zeros((n, LANES), F32)
        for c in range(nlc):
            acc = acc + src[rr, lc(c)].astype(F32)
        mean = jnp.sum(acc, axis=1, keepdims=True) / D
        acc = jnp.zeros((n, LANES), F32)
        for c in range(nlc):
            z = src[rr, lc(c)].astype(F32) - mean
            acc = acc + z * z
        rstd = lax.rsqrt(jnp.sum(acc, axis=1, keepdims=True) / D + EPS)
        for c in range(nlc):
            z = (src[rr, lc(c)].astype(F32) - mean) * rstd
            if dst is not None:
                dst[rr, lc(c)] = (z * vecs[gain, :, lc(c)] + vecs[shift, :, lc(c)]).astype(BF)
            else:
                xh1[:, lc(c)] = z
        return rstd

    ln_block(own, 32, xg, 0, 1, h)
    lb.wait()
    for k in range(3):
        bt = bqkv[k].T
        for hd in range(n_heads):
            at = (hd * 3 + k) * head
            bias[at:at + head, :] = jnp.broadcast_to(bt[:head, hd:hd + 1], (head, seq))
    x_to_sib.wait_recv()
    ln_block(rows(sib), 32, xg, 0, 1, h)
    x_to_cross.wait_recv()
    x_fwd = remote(xg.at[rows(cross), :], xg.at[rows(cross), :], sib)
    gy_to_cross = remote(gyg.at[own, :], gyg.at[own, :], cross)
    ln_block(rows(cross), 32, xg, 0, 1, h)
    x_fwd.wait_recv()
    ln_block(rows(sibcross), 32, xg, 0, 1, h)
    lwqkv.wait()

    hr = 2 * 3 * head
    hv = h[...]
    for m in range(n_heads // 2):
        mm = slice(m * hr, (m + 1) * hr)
        qkv[mm, :] = (dot_t(wqkv[mm, :], hv) + bias[mm, :]).astype(BF)
    store(h, h_o)

    def position(axis):
        i = lax.broadcasted_iota(jnp.int32, (seq, seq), axis)
        b = i >> 5
        return ((((b & 1) << 1) | (b >> 1)) << 5) | (i & 31)

    pos_k = position(0)
    causal = pos_k <= position(1)
    key_f = pos_k.astype(F32)
    slopes = alibi_slopes(n_heads * TP)
    score_scale = head ** -0.5

    def part_of(hd, k):
        at = (hd * 3 + k) * head
        return slice(at, at + head)

    def slope(hd):
        v = jnp.float32(slopes[hd])
        for dev in range(1, TP):
            v = jnp.where(t == dev, jnp.float32(slopes[dev * n_heads + hd]), v)
        return v

    for hd in range(n_heads):
        s = dot(qkv[part_of(hd, 1), :].T, qkv[part_of(hd, 0), :]) * score_scale + slope(hd) * key_f
        s = jnp.where(causal, s, MASK_VALUE)
        e = jnp.exp(s - jnp.max(s, axis=0, keepdims=True))
        pr = e * (1.0 / jnp.sum(e, axis=0, keepdims=True))
        prob[hd] = pr
        probb[hd] = pr.astype(BF)
    for hd in range(n_heads):
        ctx[hd * head:(hd + 1) * head, :] = dot(qkv[part_of(hd, 2), :], probb[hd]).astype(BF)

    class AllSum:
        def __init__(self, p, rd, s, rs, tt):
            self.p, self.rd, self.s, self.rs, self.tt = p, rd, s, rs, tt
            self.a, self.b, self.c = {}, {}, {}

        def put(self, j, value):
            self.p[:, ch(j)] = value
            self.a[j] = remote(self.p.at[sibhalf, ch(j)], self.rd.at[:, ch(j)], sib)

        def step_cross(self, j):
            self.a[j].wait_recv()
            self.s[:, ch(j)] = (self.p[half, ch(j)].astype(F32) + self.rd[:, ch(j)].astype(F32)).astype(BF)
            self.b[j] = remote(self.s.at[:, ch(j)], self.rs.at[:, ch(j)], cross)

        def step_back(self, j):
            self.b[j].wait_recv()
            self.tt[half, ch(j)] = (self.s[:, ch(j)].astype(F32) + self.rs[:, ch(j)].astype(F32)).astype(BF)
            self.c[j] = remote(self.tt.at[half, ch(j)], self.tt.at[half, ch(j)], sib)

        def finish(self, j):
            self.c[j].wait_recv()

    class ScatterSum(AllSum):
        def step_cross(self, j):
            self.a[j].wait_recv()
            self.s[:, ch(j)] = (self.p[half, ch(j)].astype(F32) + self.rd[:, ch(j)].astype(F32)).astype(BF)
            self.b[j] = remote(self.s.at[blk_cross, ch(j)], self.rs.at[:, ch(j)], cross)

        def result(self, j, c):
            return (self.s[blk_own, c].astype(F32) + self.rs[:, c].astype(F32)).astype(BF).astype(F32)

    lwout.wait()
    o_flat = ctx[...].T
    sum_a = AllSum(p1, rd1, s1, rs1, t1)
    for j in range(NCH):
        sum_a.put(j, dot(o_flat, wout[:, ch(j)]).astype(BF))
        if j:
            sum_a.step_cross(j - 1)
    sum_a.step_cross(NCH - 1)
    store(ctx, ctx_o)

    gy_to_sib.wait_recv()
    gy_to_cross.wait_recv()
    gy_fwd = remote(gyg.at[rows(cross), :], gyg.at[rows(cross), :], sib)
    gy_fwd.wait_recv()
    store(gyg, gy_o)
    lwdn.wait()
    fw = wdn_h.shape[0] // NCH
    acc = jnp.zeros((seq, LANES), F32)

    def x1_chunk(j, acc):
        sum_a.finish(j)
        for c in range(j * (cw // LANES), (j + 1) * (cw // LANES)):
            z = xg[:, lc(c)].astype(F32) + t1[:, lc(c)].astype(F32) + vecs[4, :, lc(c)]
            x1[:, lc(c)] = z
            acc = acc + z
        return acc

    gyv = gyg[...]
    for j in range(NCH):
        ff = slice(j * fw, (j + 1) * fw)
        gact[:, ff] = dot_t(gyv, wdn[ff, :]).astype(BF)
        sum_a.step_back(j)
        if j:
            acc = x1_chunk(j - 1, acc)
    acc = x1_chunk(NCH - 1, acc)

    mean = jnp.sum(acc, axis=1, keepdims=True) / D
    acc = jnp.zeros((seq, LANES), F32)
    for c in range(nlc):
        z = x1[:, lc(c)] - mean
        acc = acc + z * z
    rstd2 = lax.rsqrt(jnp.sum(acc, axis=1, keepdims=True) / D + EPS)
    for c in range(nlc):
        z = (x1[:, lc(c)] - mean) * rstd2
        xhat[:, lc(c)] = z
        g[:, lc(c)] = (z * vecs[2, :, lc(c)] + vecs[3, :, lc(c)]).astype(BF)

    lwup.wait()
    gv = g[...]
    for j in range(NCH):
        ff = slice(j * fw, (j + 1) * fw)
        pre = dot(gv, wup[:, ff]) + vecs[6, :, ff]
        sq = pre * pre
        th = jnp.tanh(GELU_C * (pre + GELU_A * (pre * sq)))
        one = 0.5 * (1.0 + th)
        r[:, ff] = (pre * one).astype(BF)
        slope_g = one + 0.5 * pre * (1.0 - th * th) * (GELU_C * (1.0 + 3.0 * GELU_A * sq))
        gp = gact[:, ff].astype(F32) * slope_g
        vec[6:7, ff] = jnp.sum(gp, axis=0, keepdims=True)
        dpre[:, ff] = gp.astype(BF)

    dv = dpre[...]
    sum_g = AllSum(p2, rd2, s2, rs2, t2)
    for j in range(NCH):
        sum_g.put(j, dot_t(dv, wup[ch(j), :]).astype(BF))
        if j:
            sum_g.step_cross(j - 1)
    sum_g.step_cross(NCH - 1)
    store(dpre, dpre_o)

    acc1 = jnp.zeros((seq, LANES), F32)
    acc2 = jnp.zeros((seq, LANES), F32)

    def ln2_back_chunk(j, acc1, acc2):
        sum_g.finish(j)
        for c in range(j * (cw // LANES), (j + 1) * (cw // LANES)):
            dg = t2[:, lc(c)].astype(F32)
            z = xhat[:, lc(c)]
            dgz = dg * z
            vec[2:3, lc(c)] = jnp.sum(dgz, axis=0, keepdims=True)
            vec[3:4, lc(c)] = jnp.sum(dg, axis=0, keepdims=True)
            gain = vecs[2, :, lc(c)]
            acc1 = acc1 + dg * gain
            acc2 = acc2 + dgz * gain
        return acc1, acc2

    rv = r[...]
    sum_y = ScatterSum(py, rdy, sy, rsy, None)
    for j in range(NCH):
        py[:, ch(j)] = dot(rv, wdn[:, ch(j)]).astype(BF)
        for c in range(j * (cw // LANES), (j + 1) * (cw // LANES)):
            gt[lc(c), :] = g[:, lc(c)].T
            rt[lc(c), :] = r[:, lc(c)].T
            vec[5:6, lc(c)] = jnp.sum(gyg[:, lc(c)].astype(F32), axis=0, keepdims=True)
        sum_g.step_back(j)
        if j:
            acc1, acc2 = ln2_back_chunk(j - 1, acc1, acc2)
    acc1, acc2 = ln2_back_chunk(NCH - 1, acc1, acc2)

    mean1 = jnp.sum(acc1, axis=1, keepdims=True) / D
    mean2 = jnp.sum(acc2, axis=1, keepdims=True) / D
    for c in range(nlc):
        dz = t2[:, lc(c)].astype(F32) * vecs[2, :, lc(c)]
        gm = gyg[:, lc(c)].astype(F32) + rstd2 * (dz - mean1 - xhat[:, lc(c)] * mean2)
        gmid[:, lc(c)] = gm
        vec[4:5, lc(c)] = jnp.sum(gm, axis=0, keepdims=True)
        ga[:, lc(c)] = gm.astype(BF)

    y_sib = remote(py.at[sibhalf, :], rdy, sib)
    store(gt, gt_o)
    store(rt, rt_o)
    store(ga, ga_o)

    dctx[...] = dot_t(wout[...], ga[...]).astype(BF)
    for hd in range(n_heads):
        hh = slice(hd * head, (hd + 1) * head)
        do = dctx[hh, :]
        pr = prob[hd]
        dp = dot(qkv[part_of(hd, 2), :].T, do).astype(BF).astype(F32)
        dqkv[part_of(hd, 2), :] = dot_t(do, probb[hd]).astype(BF)
        ds = (pr * (dp - jnp.sum(dp * pr, axis=0, keepdims=True))).astype(BF)
        dqkv[part_of(hd, 0), :] = (dot(qkv[part_of(hd, 1), :], ds) * score_scale).astype(BF)
        dqkv[part_of(hd, 1), :] = (dot_t(qkv[part_of(hd, 0), :], ds) * score_scale).astype(BF)

    y_sib.wait_recv()
    sy[...] = (py[half, :].astype(F32) + rdy[...].astype(F32)).astype(BF)
    y_cross = remote(sy.at[blk_cross, :], rsy, cross)

    sum_h = ScatterSum(ph, rdh, sh, rsh, None)
    dq = dqkv[...].T
    for j in range(NCH):
        sum_h.put(j, dot(dq, wqkv[:, ch(j)]).astype(BF))
        if j:
            sum_h.step_cross(j - 1)
    sum_h.step_cross(NCH - 1)
    store(dqkv, dqkv_o)

    rstd1 = ln_block(own, 32, xg, 0, 1, None)
    y_cross.wait_recv()
    for c in range(nlc):
        z = (sy[blk_own, lc(c)].astype(F32) + rsy[:, lc(c)].astype(F32)).astype(BF).astype(F32)
        ybuf[:, lc(c)] = (x1[own, lc(c)] + z + vecs[5, :, lc(c)]).astype(BF)
    store(ybuf, y_o)

    me = slot(t)
    acc1 = jnp.zeros((32, LANES), F32)
    acc2 = jnp.zeros((32, LANES), F32)
    for j in range(NCH):
        sum_h.b[j].wait_recv()
        for c in range(j * (cw // LANES), (j + 1) * (cw // LANES)):
            dh = sum_h.result(j, lc(c))
            z = xh1[:, lc(c)]
            dhz = dh * z
            part[me, 0:1, lc(c)] = jnp.sum(dhz, axis=0, keepdims=True)
            part[me, 1:2, lc(c)] = jnp.sum(dh, axis=0, keepdims=True)
            gain = vecs[0, :, lc(c)]
            acc1 = acc1 + dh * gain
            acc2 = acc2 + dhz * gain
    parts = [remote(part.at[me], part.at[me], dev) for dev in (cross, sibcross, sib)]
    mean1 = jnp.sum(acc1, axis=1, keepdims=True) / D
    mean2 = jnp.sum(acc2, axis=1, keepdims=True) / D
    for c in range(nlc):
        dz = sum_h.result(None, lc(c)) * vecs[0, :, lc(c)]
        gxbuf[:, lc(c)] = (gmid[own, lc(c)] + rstd1 * (dz - mean1 - xh1[:, lc(c)] * mean2)).astype(BF)
    store(gxbuf, gx_o)
    for copy in parts:
        copy.wait_recv()
    vec[0:2, :] = (part[0] + part[1]) + (part[2] + part[3])
    store(vec, vec_o)
    for copy in sent:
        copy.wait_send()
    for copy in outs:
        copy.wait()


def grad_kernel(h_h, ga_h, dpre_h, gy_h, dqkv_h, ctx_h, gt_h, rt_h, vec_h, y_h, gx_h,
                dwqkv_o, dwout_o, dwup_o, dwdn_o, dbqkv_o, y_o, gx_o, v0, v1, v2, v3, v4, v5, v6,
                h, ga, dpre, gy, dqkv, ctx, gt, rt, vec, y, gx, buf, isem, osem):
    n_heads, head = dbqkv_o.shape[1], dbqkv_o.shape[2]
    block = 320
    slots = buf.shape[0]
    loads = []
    for k, (src, dst) in enumerate(((rt_h, rt), (gy_h, gy), (gt_h, gt), (dpre_h, dpre), (dqkv_h, dqkv), (h_h, h), (ctx_h, ctx),
                                    (ga_h, ga), (vec_h, vec), (y_h, y), (gx_h, gx))):
        copy = pltpu.make_async_copy(src, dst, isem.at[k])
        copy.start()
        loads.append(copy)

    step = 0
    pending = []
    for n, (left, right, out, la, lb) in enumerate(((rt, gy, dwdn_o, 0, 1), (gt, dpre, dwup_o, 2, 3), (dqkv, h, dwqkv_o, 4, 5),
                                                    (ctx, ga, dwout_o, 6, 7))):
        loads[la].wait()
        loads[lb].wait()
        rv = right[...]
        for m in range(left.shape[0] // block):
            s = step % slots
            if step >= slots:
                pending[step - slots].wait()
            mm = slice(m * block, (m + 1) * block)
            buf[s] = dot(left[mm, :], rv).astype(BF)
            copy = pltpu.make_async_copy(buf.at[s], out.at[pl.ds(m * block, block), :], osem.at[s])
            copy.start()
            pending.append(copy)
            step += 1
    ones = jnp.ones((8, dqkv.shape[1]), BF)
    sums = dot_t(ones, dqkv[...])[0:1]
    for k in range(3):
        for hd in range(n_heads):
            at = (hd * 3 + k) * head
            dbqkv_o[k, hd:hd + 1, :] = sums[:, at:at + head]
    for k in range(8, 11):
        loads[k].wait()
    y_o[...] = y[...]
    gx_o[...] = gx[...]
    for k, o in enumerate((v0, v1, v2, v3, v4, v5, v6)):
        o[...] = vec[k, :]
    for k in range(max(0, step - slots), step):
        pending[k].wait()


def solution(mesh):
    def local_step(x, ln1_gamma, ln1_beta, w_qkv, b_qkv, w_out, b_out, ln2_gamma, ln2_beta, w_up, b_up, w_down, b_down, grad_y):
        D = x.shape[2]
        S = TP * x.shape[1]
        nh, head = w_qkv.shape[1], w_qkv.shape[3]
        Q = nh * 3 * head
        C = nh * head
        FL = w_up.shape[1]
        any_spec = pl.BlockSpec(memory_space=pl.ANY)
        vm = pltpu.VMEM
        wqkv_t = jnp.transpose(w_qkv, (1, 2, 3, 0)).reshape(Q, D)
        bq = jnp.transpose(b_qkv, (1, 0, 2))
        sds = jax.ShapeDtypeStruct
        n_loads = 2 + 7 + 1 + 4
        n_remote = 64
        red = [vm((S, D), BF), vm((S // 2, D), BF), vm((S // 2, D), BF), vm((S // 2, D), BF), vm((S, D), BF)]
        scat = [vm((S, D), BF), vm((S // 2, D), BF), vm((S // 2, D), BF), vm((S // TP, D), BF)]
        row = lambda v: v.reshape(1, D)
        res = pl.pallas_call(
            layer_kernel,
            name='layer',
            out_shape=[sds((S // TP, D), BF), sds((S // TP, D), BF), sds((8, D), F32), sds((S, D), BF), sds((S, D), BF),
                       sds((S, FL), BF), sds((S, D), BF), sds((Q, S), BF), sds((C, S), BF), sds((D, S), BF), sds((FL, S), BF)],
            in_specs=[any_spec] * 14,
            out_specs=[any_spec] * 11,
            scratch_shapes=[
                vm((Q, D), BF), vm((C, D), BF), vm((D, FL), BF), vm((FL, D), BF), vm((3, nh, head), F32), vm((7, 1, D), F32),
                vm((S, D), BF), vm((S, D), BF), vm((S, D), BF), vm((Q, S), F32), vm((Q, S), BF), vm((nh, S, S), F32),
                vm((nh, S, S), BF), vm((C, S), BF), vm((S, D), F32), vm((S, D), F32), vm((S, D), BF), vm((D, S), BF), vm((FL, S), BF),
                vm((S, FL), BF), vm((S, FL), BF), vm((S, FL), BF), vm((S, D), F32), vm((S, D), BF), vm((C, S), BF), vm((Q, S), BF),
                vm((S // TP, D), BF), vm((S // TP, D), BF), vm((S // TP, D), F32), vm((8, D), F32), vm((TP, 2, D), F32),
                *red, *red, *scat, *scat,
                pltpu.SemaphoreType.DMA((n_loads,)), pltpu.SemaphoreType.DMA((16,)),
                pltpu.SemaphoreType.DMA((n_remote,)), pltpu.SemaphoreType.DMA((n_remote,)),
            ],
            compiler_params=pltpu.CompilerParams(collective_id=0, has_side_effects=True, vmem_limit_bytes=67043328),
        )(x.reshape(x.shape[1], D), grad_y.reshape(x.shape[1], D), wqkv_t, bq, w_out, w_up, w_down, row(ln1_gamma), row(ln1_beta),
          row(ln2_gamma), row(ln2_beta), row(b_out), row(b_down), row(b_up))
        y, gx, vec, h, ga, dpre, gyf, dqkv, ctx, gt, rt = res
        vspec = pl.BlockSpec(memory_space=pltpu.VMEM)
        vshape = sds((D,), F32)
        outs = pl.pallas_call(
            grad_kernel,
            name='weight_grads',
            out_shape=[sds((Q, D), BF), sds((C, D), BF), sds((D, FL), BF), sds((FL, D), BF), sds((3, nh, head), F32),
                       sds((S // TP, D), BF), sds((S // TP, D), BF)] + [vshape] * 7,
            in_specs=[any_spec] * 11,
            out_specs=[any_spec] * 4 + [vspec] * 10,
            scratch_shapes=[
                vm((S, D), BF), vm((S, D), BF), vm((S, FL), BF), vm((S, D), BF), vm((Q, S), BF), vm((C, S), BF), vm((D, S), BF),
                vm((FL, S), BF), vm((8, D), F32), vm((S // TP, D), BF), vm((S // TP, D), BF), vm((4, 320, D), BF),
                pltpu.SemaphoreType.DMA((11,)), pltpu.SemaphoreType.DMA((4,)),
            ],
            compiler_params=pltpu.CompilerParams(vmem_limit_bytes=60 * 1024 * 1024),
        )(h, ga, dpre, gyf, dqkv, ctx, gt, rt, vec, y, gx)
        dwqkv, dwout, dwup, dwdn, dbqkv, y, gx, g_ln1g, g_ln1b, g_ln2g, g_ln2b, g_bout, g_bdown, g_bup = outs
        dwqkv = jnp.transpose(dwqkv.reshape(nh, 3, head, D), (3, 0, 1, 2))
        dbqkv = jnp.transpose(dbqkv, (1, 0, 2))
        return (y.reshape(x.shape), gx.reshape(x.shape), g_ln1g, g_ln1b, dwqkv, dbqkv, dwout, g_bout,
                g_ln2g, g_ln2b, dwup, g_bup, dwdn, g_bdown)

    row_spec = P('dp', 'tp', None)
    in_specs = (row_spec, P(), P(), P(None, 'tp', None, None), P('tp', None, None), P('tp', None), P(), P(), P(),
                P(None, 'tp'), P('tp'), P('tp', None), P(), row_spec)
    out_specs = (row_spec, row_spec, P('dp'), P('dp'), P('dp', 'tp', None, None), P(('dp', 'tp'), None, None),
                 P(('dp', 'tp'), None), P('dp'), P('dp'), P('dp'), P('dp', 'tp'), P(('dp', 'tp')), P(('dp', 'tp'), None), P('dp'))
    return jax.shard_map(local_step, mesh=mesh, in_specs=in_specs, out_specs=out_specs, check_vma=False)
```

```python
import functools
import math
import jax
import jax.numpy as jnp
from jax import lax
from jax.experimental import pallas as pl
from jax.experimental.pallas import tpu as pltpu
from jax.sharding import PartitionSpec as P

EPS = 1e-5
MASK_VALUE = -1e30
BF = jnp.bfloat16
F32 = jnp.float32
MESH = pl.DeviceIdType.MESH
GELU_C = math.sqrt(2.0 / math.pi)
GELU_A = 0.044715
TP = 4
NCH = 5
LANES = 128


def alibi_slopes(n_heads):
    closest = 2 ** int(math.floor(math.log2(n_heads)))
    base_ratio = 2.0 ** (-8.0 / closest)
    extra_ratio = 2.0 ** (-4.0 / closest)
    remaining = min(closest, n_heads - closest)
    slopes = [base_ratio ** (i + 1) for i in range(closest)]
    return slopes + [extra_ratio ** (2 * i + 1) for i in range(remaining)]


def dot(lhs, rhs):
    return lax.dot_general(lhs, rhs, (((1,), (0,)), ((), ())), preferred_element_type=F32)


def dot_t(lhs, rhs):
    return lax.dot_general(lhs, rhs, (((1,), (1,)), ((), ())), preferred_element_type=F32)


def layer_kernel(x_h, gy_h, wqkv_h, bqkv_h, wout_h, wup_h, wdn_h, ln1g_h, ln1b_h, ln2g_h, ln2b_h, bout_h, bdown_h, bup_h,
                 y_o, gx_o, vec_o, h_o, ga_o, dpre_o, gy_o, dqkv_o, ctx_o, gt_o, rt_o,
                 wqkv, wout, wup, wdn, bqkv, vecs, xg, gyg, h, bias, qkv, prob, probb, ctx, x1, xhat, g, gt, rt, gact, r, dpre,
                 gmid, ga, dctx, dqkv, ybuf, gxbuf, xh1, vec, part,
                 p1, rd1, s1, rs1, t1, p2, rd2, s2, rs2, t2, py, rdy, sy, rsy, ph, rdh, sh, rsh,
                 lsem, osem, ssem, rsem):
    D = x_h.shape[1]
    seq = TP * 32
    head = bqkv_h.shape[2]
    n_heads = bqkv_h.shape[1]
    cw = D // NCH
    nlc = D // LANES
    t = lax.axis_index('tp')
    core = lax.rem(t, 2)
    chip = t // 2
    sib = t + 1 - 2 * core
    cross = lax.rem(t + 2, TP)
    sibcross = lax.rem(sib + 2, TP)

    def slot(dev):
        return lax.rem(dev, 2) * 2 + dev // 2

    def rows(dev):
        return pl.ds(pl.multiple_of(slot(dev) * 32, 32), 32)

    own = rows(t)
    half = pl.ds(pl.multiple_of(core * 64, 64), 64)
    sibhalf = pl.ds(pl.multiple_of((1 - core) * 64, 64), 64)
    blk_own = pl.ds(pl.multiple_of(chip * 32, 32), 32)
    blk_cross = pl.ds(pl.multiple_of((1 - chip) * 32, 32), 32)

    counter = [0, 0, 0]

    def load(src, dst):
        k = counter[0]
        counter[0] += 1
        copy = pltpu.make_async_copy(src, dst, lsem.at[k])
        copy.start()
        return copy

    outs = []

    def store(src, dst):
        k = counter[1]
        counter[1] += 1
        copy = pltpu.make_async_copy(src, dst, osem.at[k])
        copy.start()
        outs.append(copy)

    sent = []

    def remote(src, dst, dev):
        k = counter[2]
        counter[2] += 1
        copy = pltpu.make_async_remote_copy(src_ref=src, dst_ref=dst, send_sem=ssem.at[k], recv_sem=rsem.at[k],
                                            device_id={'tp': dev}, device_id_type=MESH)
        copy.start()
        sent.append(copy)
        return copy

    def lc(c):
        return slice(c * LANES, (c + 1) * LANES)

    def ch(j):
        return slice(j * cw, (j + 1) * cw)

    lx = load(x_h, xg.at[own, :])
    lg = load(gy_h, gyg.at[own, :])
    lvec = [load(src, vecs.at[k, 0]) for k, src in enumerate((ln1g_h, ln1b_h, ln2g_h, ln2b_h, bout_h, bdown_h, bup_h))]
    lb = load(bqkv_h, bqkv)
    lwqkv = load(wqkv_h, wqkv)
    lwout = load(wout_h, wout)
    barrier = pltpu.get_barrier_semaphore()
    for dev in (sib, cross, sibcross):
        pl.semaphore_signal(barrier, inc=1, device_id={'tp': dev}, device_id_type=MESH)
    pl.semaphore_wait(barrier, 3)
    lx.wait()
    x_to_cross = remote(xg.at[own, :], xg.at[own, :], cross)
    x_to_sib = remote(xg.at[own, :], xg.at[own, :], sib)
    lg.wait()
    gy_to_sib = remote(gyg.at[own, :], gyg.at[own, :], sib)
    lwdn = load(wdn_h, wdn)
    lwup = load(wup_h, wup)
    for copy in lvec:
        copy.wait()

    def ln_block(rr, n, src, gain, shift, dst):
        acc = jnp.zeros((n, LANES), F32)
        for c in range(nlc):
            acc = acc + src[rr, lc(c)].astype(F32)
        mean = jnp.sum(acc, axis=1, keepdims=True) / D
        acc = jnp.zeros((n, LANES), F32)
        for c in range(nlc):
            z = src[rr, lc(c)].astype(F32) - mean
            acc = acc + z * z
        rstd = lax.rsqrt(jnp.sum(acc, axis=1, keepdims=True) / D + EPS)
        for c in range(nlc):
            z = (src[rr, lc(c)].astype(F32) - mean) * rstd
            if dst is not None:
                dst[rr, lc(c)] = (z * vecs[gain, :, lc(c)] + vecs[shift, :, lc(c)]).astype(BF)
            else:
                xh1[:, lc(c)] = z
        return rstd

    ln_block(own, 32, xg, 0, 1, h)
    lb.wait()
    for k in range(3):
        bt = bqkv[k].T
        for hd in range(n_heads):
            at = (hd * 3 + k) * head
            bias[at:at + head, :] = jnp.broadcast_to(bt[:head, hd:hd + 1], (head, seq))
    x_to_sib.wait_recv()
    ln_block(rows(sib), 32, xg, 0, 1, h)
    x_to_cross.wait_recv()
    x_fwd = remote(xg.at[rows(cross), :], xg.at[rows(cross), :], sib)
    gy_to_cross = remote(gyg.at[own, :], gyg.at[own, :], cross)
    ln_block(rows(cross), 32, xg, 0, 1, h)
    x_fwd.wait_recv()
    ln_block(rows(sibcross), 32, xg, 0, 1, h)
    lwqkv.wait()

    hr = 2 * 3 * head
    hv = h[...]
    for m in range(n_heads // 2):
        mm = slice(m * hr, (m + 1) * hr)
        qkv[mm, :] = (dot_t(wqkv[mm, :], hv) + bias[mm, :]).astype(BF)
    store(h, h_o)

    def position(axis):
        i = lax.broadcasted_iota(jnp.int32, (seq, seq), axis)
        b = i >> 5
        return ((((b & 1) << 1) | (b >> 1)) << 5) | (i & 31)

    pos_k = position(0)
    causal = pos_k <= position(1)
    key_f = pos_k.astype(F32)
    slopes = alibi_slopes(n_heads * TP)
    score_scale = head ** -0.5

    def part_of(hd, k):
        at = (hd * 3 + k) * head
        return slice(at, at + head)

    def slope(hd):
        v = jnp.float32(slopes[hd])
        for dev in range(1, TP):
            v = jnp.where(t == dev, jnp.float32(slopes[dev * n_heads + hd]), v)
        return v

    for hd in range(n_heads):
        s = dot(qkv[part_of(hd, 1), :].T, qkv[part_of(hd, 0), :]) * score_scale + slope(hd) * key_f
        s = jnp.where(causal, s, MASK_VALUE)
        e = jnp.exp(s - jnp.max(s, axis=0, keepdims=True))
        pr = e * (1.0 / jnp.sum(e, axis=0, keepdims=True))
        prob[hd] = pr
        probb[hd] = pr.astype(BF)
    for hd in range(n_heads):
        ctx[hd * head:(hd + 1) * head, :] = dot(qkv[part_of(hd, 2), :], probb[hd]).astype(BF)

    class AllSum:
        def __init__(self, p, rd, s, rs, tt):
            self.p, self.rd, self.s, self.rs, self.tt = p, rd, s, rs, tt
            self.a, self.b, self.c = {}, {}, {}

        def put(self, j, value):
            self.p[:, ch(j)] = value
            self.a[j] = remote(self.p.at[sibhalf, ch(j)], self.rd.at[:, ch(j)], sib)

        def step_cross(self, j):
            self.a[j].wait_recv()
            self.s[:, ch(j)] = (self.p[half, ch(j)].astype(F32) + self.rd[:, ch(j)].astype(F32)).astype(BF)
            self.b[j] = remote(self.s.at[:, ch(j)], self.rs.at[:, ch(j)], cross)

        def step_back(self, j):
            self.b[j].wait_recv()
            self.tt[half, ch(j)] = (self.s[:, ch(j)].astype(F32) + self.rs[:, ch(j)].astype(F32)).astype(BF)
            self.c[j] = remote(self.tt.at[half, ch(j)], self.tt.at[half, ch(j)], sib)

        def finish(self, j):
            self.c[j].wait_recv()

    class ScatterSum(AllSum):
        def step_cross(self, j):
            self.a[j].wait_recv()
            self.s[:, ch(j)] = (self.p[half, ch(j)].astype(F32) + self.rd[:, ch(j)].astype(F32)).astype(BF)
            self.b[j] = remote(self.s.at[blk_cross, ch(j)], self.rs.at[:, ch(j)], cross)

        def result(self, j, c):
            return (self.s[blk_own, c].astype(F32) + self.rs[:, c].astype(F32)).astype(BF).astype(F32)

    lwout.wait()
    o_flat = ctx[...].T
    sum_a = AllSum(p1, rd1, s1, rs1, t1)
    for j in range(NCH):
        sum_a.put(j, dot(o_flat, wout[:, ch(j)]).astype(BF))
        if j:
            sum_a.step_cross(j - 1)
    sum_a.step_cross(NCH - 1)
    store(ctx, ctx_o)

    gy_to_sib.wait_recv()
    gy_to_cross.wait_recv()
    gy_fwd = remote(gyg.at[rows(cross), :], gyg.at[rows(cross), :], sib)
    gy_fwd.wait_recv()
    store(gyg, gy_o)
    lwdn.wait()
    fw = wdn_h.shape[0] // NCH
    acc = jnp.zeros((seq, LANES), F32)

    def x1_chunk(j, acc):
        sum_a.finish(j)
        for c in range(j * (cw // LANES), (j + 1) * (cw // LANES)):
            z = xg[:, lc(c)].astype(F32) + t1[:, lc(c)].astype(F32) + vecs[4, :, lc(c)]
            x1[:, lc(c)] = z
            acc = acc + z
        return acc

    gyv = gyg[...]
    for j in range(NCH):
        ff = slice(j * fw, (j + 1) * fw)
        gact[:, ff] = dot_t(gyv, wdn[ff, :]).astype(BF)
        sum_a.step_back(j)
        if j:
            acc = x1_chunk(j - 1, acc)
    acc = x1_chunk(NCH - 1, acc)

    mean = jnp.sum(acc, axis=1, keepdims=True) / D
    acc = jnp.zeros((seq, LANES), F32)
    for c in range(nlc):
        z = x1[:, lc(c)] - mean
        acc = acc + z * z
    rstd2 = lax.rsqrt(jnp.sum(acc, axis=1, keepdims=True) / D + EPS)
    for c in range(nlc):
        z = (x1[:, lc(c)] - mean) * rstd2
        xhat[:, lc(c)] = z
        g[:, lc(c)] = (z * vecs[2, :, lc(c)] + vecs[3, :, lc(c)]).astype(BF)

    lwup.wait()
    gv = g[...]
    for j in range(NCH):
        ff = slice(j * fw, (j + 1) * fw)
        pre = dot(gv, wup[:, ff]) + vecs[6, :, ff]
        sq = pre * pre
        th = jnp.tanh(GELU_C * (pre + GELU_A * (pre * sq)))
        one = 0.5 * (1.0 + th)
        r[:, ff] = (pre * one).astype(BF)
        slope_g = one + 0.5 * pre * (1.0 - th * th) * (GELU_C * (1.0 + 3.0 * GELU_A * sq))
        gp = gact[:, ff].astype(F32) * slope_g
        vec[6:7, ff] = jnp.sum(gp, axis=0, keepdims=True)
        dpre[:, ff] = gp.astype(BF)

    dv = dpre[...]
    sum_g = AllSum(p2, rd2, s2, rs2, t2)
    for j in range(NCH):
        sum_g.put(j, dot_t(dv, wup[ch(j), :]).astype(BF))
        if j:
            sum_g.step_cross(j - 1)
    sum_g.step_cross(NCH - 1)
    store(dpre, dpre_o)

    acc1 = jnp.zeros((seq, LANES), F32)
    acc2 = jnp.zeros((seq, LANES), F32)

    def ln2_back_chunk(j, acc1, acc2):
        sum_g.finish(j)
        for c in range(j * (cw // LANES), (j + 1) * (cw // LANES)):
            dg = t2[:, lc(c)].astype(F32)
            z = xhat[:, lc(c)]
            dgz = dg * z
            vec[2:3, lc(c)] = jnp.sum(dgz, axis=0, keepdims=True)
            vec[3:4, lc(c)] = jnp.sum(dg, axis=0, keepdims=True)
            gain = vecs[2, :, lc(c)]
            acc1 = acc1 + dg * gain
            acc2 = acc2 + dgz * gain
        return acc1, acc2

    rv = r[...]
    sum_y = ScatterSum(py, rdy, sy, rsy, None)
    for j in range(NCH):
        py[:, ch(j)] = dot(rv, wdn[:, ch(j)]).astype(BF)
        for c in range(j * (cw // LANES), (j + 1) * (cw // LANES)):
            gt[lc(c), :] = g[:, lc(c)].T
            rt[lc(c), :] = r[:, lc(c)].T
            vec[5:6, lc(c)] = jnp.sum(gyg[:, lc(c)].astype(F32), axis=0, keepdims=True)
        sum_g.step_back(j)
        if j:
            acc1, acc2 = ln2_back_chunk(j - 1, acc1, acc2)
    acc1, acc2 = ln2_back_chunk(NCH - 1, acc1, acc2)

    mean1 = jnp.sum(acc1, axis=1, keepdims=True) / D
    mean2 = jnp.sum(acc2, axis=1, keepdims=True) / D
    for c in range(nlc):
        dz = t2[:, lc(c)].astype(F32) * vecs[2, :, lc(c)]
        gm = gyg[:, lc(c)].astype(F32) + rstd2 * (dz - mean1 - xhat[:, lc(c)] * mean2)
        gmid[:, lc(c)] = gm
        vec[4:5, lc(c)] = jnp.sum(gm, axis=0, keepdims=True)
        ga[:, lc(c)] = gm.astype(BF)

    y_sib = remote(py.at[sibhalf, :], rdy, sib)
    store(gt, gt_o)
    store(rt, rt_o)
    store(ga, ga_o)

    dctx[...] = dot_t(wout[...], ga[...]).astype(BF)
    for hd in range(n_heads):
        hh = slice(hd * head, (hd + 1) * head)
        do = dctx[hh, :]
        pr = prob[hd]
        dp = dot(qkv[part_of(hd, 2), :].T, do).astype(BF).astype(F32)
        dqkv[part_of(hd, 2), :] = dot_t(do, probb[hd]).astype(BF)
        ds = (pr * (dp - jnp.sum(dp * pr, axis=0, keepdims=True))).astype(BF)
        dqkv[part_of(hd, 0), :] = (dot(qkv[part_of(hd, 1), :], ds) * score_scale).astype(BF)
        dqkv[part_of(hd, 1), :] = (dot_t(qkv[part_of(hd, 0), :], ds) * score_scale).astype(BF)

    y_sib.wait_recv()
    sy[...] = (py[half, :].astype(F32) + rdy[...].astype(F32)).astype(BF)
    y_cross = remote(sy.at[blk_cross, :], rsy, cross)

    sum_h = ScatterSum(ph, rdh, sh, rsh, None)
    dq = dqkv[...].T
    for j in range(NCH):
        sum_h.put(j, dot(dq, wqkv[:, ch(j)]).astype(BF))
        if j:
            sum_h.step_cross(j - 1)
    sum_h.step_cross(NCH - 1)
    store(dqkv, dqkv_o)

    rstd1 = ln_block(own, 32, xg, 0, 1, None)
    y_cross.wait_recv()
    for c in range(nlc):
        z = (sy[blk_own, lc(c)].astype(F32) + rsy[:, lc(c)].astype(F32)).astype(BF).astype(F32)
        ybuf[:, lc(c)] = (x1[own, lc(c)] + z + vecs[5, :, lc(c)]).astype(BF)
    store(ybuf, y_o)

    me = slot(t)
    acc1 = jnp.zeros((32, LANES), F32)
    acc2 = jnp.zeros((32, LANES), F32)
    for j in range(NCH):
        sum_h.b[j].wait_recv()
        for c in range(j * (cw // LANES), (j + 1) * (cw // LANES)):
            dh = sum_h.result(j, lc(c))
            z = xh1[:, lc(c)]
            dhz = dh * z
            part[me, 0:1, lc(c)] = jnp.sum(dhz, axis=0, keepdims=True)
            part[me, 1:2, lc(c)] = jnp.sum(dh, axis=0, keepdims=True)
            gain = vecs[0, :, lc(c)]
            acc1 = acc1 + dh * gain
            acc2 = acc2 + dhz * gain
    parts = [remote(part.at[me], part.at[me], dev) for dev in (cross, sibcross, sib)]
    mean1 = jnp.sum(acc1, axis=1, keepdims=True) / D
    mean2 = jnp.sum(acc2, axis=1, keepdims=True) / D
    for c in range(nlc):
        dz = sum_h.result(None, lc(c)) * vecs[0, :, lc(c)]
        gxbuf[:, lc(c)] = (gmid[own, lc(c)] + rstd1 * (dz - mean1 - xh1[:, lc(c)] * mean2)).astype(BF)
    store(gxbuf, gx_o)
    for copy in parts:
        copy.wait_recv()
    vec[0:2, :] = (part[0] + part[1]) + (part[2] + part[3])
    store(vec, vec_o)
    for copy in sent:
        copy.wait_send()
    for copy in outs:
        copy.wait()


def grad_kernel(h_h, ga_h, dpre_h, gy_h, dqkv_h, ctx_h, gt_h, rt_h, vec_h, y_h, gx_h,
                dwqkv_o, dwout_o, dwup_o, dwdn_o, dbqkv_o, y_o, gx_o, v0, v1, v2, v3, v4, v5, v6,
                h, ga, dpre, gy, dqkv, ctx, gt, rt, vec, y, gx, buf, isem, osem):
    n_heads, head = dbqkv_o.shape[1], dbqkv_o.shape[2]
    block = 320
    slots = buf.shape[0]
    loads = []
    for k, (src, dst) in enumerate(((rt_h, rt), (gy_h, gy), (gt_h, gt), (dpre_h, dpre), (dqkv_h, dqkv), (h_h, h), (ctx_h, ctx),
                                    (ga_h, ga), (vec_h, vec), (y_h, y), (gx_h, gx))):
        copy = pltpu.make_async_copy(src, dst, isem.at[k])
        copy.start()
        loads.append(copy)

    step = 0
    pending = []
    for n, (left, right, out, la, lb) in enumerate(((rt, gy, dwdn_o, 0, 1), (gt, dpre, dwup_o, 2, 3), (dqkv, h, dwqkv_o, 4, 5),
                                                    (ctx, ga, dwout_o, 6, 7))):
        loads[la].wait()
        loads[lb].wait()
        rv = right[...]
        for m in range(left.shape[0] // block):
            s = step % slots
            if step >= slots:
                pending[step - slots].wait()
            mm = slice(m * block, (m + 1) * block)
            buf[s] = dot(left[mm, :], rv).astype(BF)
            copy = pltpu.make_async_copy(buf.at[s], out.at[pl.ds(m * block, block), :], osem.at[s])
            copy.start()
            pending.append(copy)
            step += 1
    ones = jnp.ones((8, dqkv.shape[1]), BF)
    sums = dot_t(ones, dqkv[...])[0:1]
    for k in range(3):
        for hd in range(n_heads):
            at = (hd * 3 + k) * head
            dbqkv_o[k, hd:hd + 1, :] = sums[:, at:at + head]
    for k in range(8, 11):
        loads[k].wait()
    y_o[...] = y[...]
    gx_o[...] = gx[...]
    for k, o in enumerate((v0, v1, v2, v3, v4, v5, v6)):
        o[...] = vec[k, :]
    for k in range(max(0, step - slots), step):
        pending[k].wait()


def solution(mesh):
    def local_step(x, ln1_gamma, ln1_beta, w_qkv, b_qkv, w_out, b_out, ln2_gamma, ln2_beta, w_up, b_up, w_down, b_down, grad_y):
        D = x.shape[2]
        S = TP * x.shape[1]
        nh, head = w_qkv.shape[1], w_qkv.shape[3]
        Q = nh * 3 * head
        C = nh * head
        FL = w_up.shape[1]
        any_spec = pl.BlockSpec(memory_space=pl.ANY)
        vm = pltpu.VMEM
        wqkv_t = jnp.transpose(w_qkv, (1, 2, 3, 0)).reshape(Q, D)
        bq = jnp.transpose(b_qkv, (1, 0, 2))
        sds = jax.ShapeDtypeStruct
        n_loads = 2 + 7 + 1 + 4
        n_remote = 64
        red = [vm((S, D), BF), vm((S // 2, D), BF), vm((S // 2, D), BF), vm((S // 2, D), BF), vm((S, D), BF)]
        scat = [vm((S, D), BF), vm((S // 2, D), BF), vm((S // 2, D), BF), vm((S // TP, D), BF)]
        row = lambda v: v
        res = pl.pallas_call(
            layer_kernel,
            name='layer',
            out_shape=[sds((S // TP, D), BF), sds((S // TP, D), BF), sds((8, D), F32), sds((S, D), BF), sds((S, D), BF),
                       sds((S, FL), BF), sds((S, D), BF), sds((Q, S), BF), sds((C, S), BF), sds((D, S), BF), sds((FL, S), BF)],
            in_specs=[any_spec] * 14,
            out_specs=[any_spec] * 11,
            scratch_shapes=[
                vm((Q, D), BF), vm((C, D), BF), vm((D, FL), BF), vm((FL, D), BF), vm((3, nh, head), F32), vm((7, 1, D), F32),
                vm((S, D), BF), vm((S, D), BF), vm((S, D), BF), vm((Q, S), F32), vm((Q, S), BF), vm((nh, S, S), F32),
                vm((nh, S, S), BF), vm((C, S), BF), vm((S, D), F32), vm((S, D), F32), vm((S, D), BF), vm((D, S), BF), vm((FL, S), BF),
                vm((S, FL), BF), vm((S, FL), BF), vm((S, FL), BF), vm((S, D), F32), vm((S, D), BF), vm((C, S), BF), vm((Q, S), BF),
                vm((S // TP, D), BF), vm((S // TP, D), BF), vm((S // TP, D), F32), vm((8, D), F32), vm((TP, 2, D), F32),
                *red, *red, *scat, *scat,
                pltpu.SemaphoreType.DMA((n_loads,)), pltpu.SemaphoreType.DMA((16,)),
                pltpu.SemaphoreType.DMA((n_remote,)), pltpu.SemaphoreType.DMA((n_remote,)),
            ],
            compiler_params=pltpu.CompilerParams(collective_id=0, has_side_effects=True, vmem_limit_bytes=67043328),
        )(x.reshape(x.shape[1], D), grad_y.reshape(x.shape[1], D), wqkv_t, bq, w_out, w_up, w_down, row(ln1_gamma), row(ln1_beta),
          row(ln2_gamma), row(ln2_beta), row(b_out), row(b_down), row(b_up))
        y, gx, vec, h, ga, dpre, gyf, dqkv, ctx, gt, rt = res
        vspec = pl.BlockSpec(memory_space=pltpu.VMEM)
        vshape = sds((D,), F32)
        outs = pl.pallas_call(
            grad_kernel,
            name='weight_grads',
            out_shape=[sds((Q, D), BF), sds((C, D), BF), sds((D, FL), BF), sds((FL, D), BF), sds((3, nh, head), F32),
                       sds((S // TP, D), BF), sds((S // TP, D), BF)] + [vshape] * 7,
            in_specs=[any_spec] * 11,
            out_specs=[any_spec] * 4 + [vspec] * 10,
            scratch_shapes=[
                vm((S, D), BF), vm((S, D), BF), vm((S, FL), BF), vm((S, D), BF), vm((Q, S), BF), vm((C, S), BF), vm((D, S), BF),
                vm((FL, S), BF), vm((8, D), F32), vm((S // TP, D), BF), vm((S // TP, D), BF), vm((4, 320, D), BF),
                pltpu.SemaphoreType.DMA((11,)), pltpu.SemaphoreType.DMA((4,)),
            ],
            compiler_params=pltpu.CompilerParams(vmem_limit_bytes=60 * 1024 * 1024),
        )(h, ga, dpre, gyf, dqkv, ctx, gt, rt, vec, y, gx)
        dwqkv, dwout, dwup, dwdn, dbqkv, y, gx, g_ln1g, g_ln1b, g_ln2g, g_ln2b, g_bout, g_bdown, g_bup = outs
        dwqkv = jnp.transpose(dwqkv.reshape(nh, 3, head, D), (3, 0, 1, 2))
        dbqkv = jnp.transpose(dbqkv, (1, 0, 2))
        return (y.reshape(x.shape), gx.reshape(x.shape), g_ln1g, g_ln1b, dwqkv, dbqkv, dwout, g_bout,
                g_ln2g, g_ln2b, dwup, g_bup, dwdn, g_bdown)

    row_spec = P('dp', 'tp', None)
    in_specs = (row_spec, P(), P(), P(None, 'tp', None, None), P('tp', None, None), P('tp', None), P(), P(), P(),
                P(None, 'tp'), P('tp'), P('tp', None), P(), row_spec)
    out_specs = (row_spec, row_spec, P('dp'), P('dp'), P('dp', 'tp', None, None), P(('dp', 'tp'), None, None),
                 P(('dp', 'tp'), None), P('dp'), P('dp'), P('dp'), P('dp', 'tp'), P(('dp', 'tp')), P(('dp', 'tp'), None), P('dp'))
    return jax.shard_map(local_step, mesh=mesh, in_specs=in_specs, out_specs=out_specs, check_vma=False)
```

```python
import functools
import math
import jax
import jax.numpy as jnp
from jax import lax
from jax.experimental import pallas as pl
from jax.experimental.pallas import tpu as pltpu
from jax.sharding import PartitionSpec as P

EPS = 1e-5
MASK_VALUE = -1e30
BF = jnp.bfloat16
F32 = jnp.float32
MESH = pl.DeviceIdType.MESH
GELU_C = math.sqrt(2.0 / math.pi)
GELU_A = 0.044715
TP = 4
LANES = 128
ALL_CHUNKS = (2, 4, 4, 5, 4, 1)
SCATTER_CHUNKS = (2, 4, 5, 5, 4)
N_BLK = 5
N_REMOTE = 61
N_STORE = 12


def alibi_slopes(n_heads):
    closest = 2 ** int(math.floor(math.log2(n_heads)))
    base_ratio = 2.0 ** (-8.0 / closest)
    extra_ratio = 2.0 ** (-4.0 / closest)
    remaining = min(closest, n_heads - closest)
    slopes = [base_ratio ** (i + 1) for i in range(closest)]
    return slopes + [extra_ratio ** (2 * i + 1) for i in range(remaining)]


def dot(lhs, rhs):
    return lax.dot_general(lhs, rhs, (((1,), (0,)), ((), ())), preferred_element_type=F32)


def dot_t(lhs, rhs):
    return lax.dot_general(lhs, rhs, (((1,), (1,)), ((), ())), preferred_element_type=F32)


def layer_kernel(x_h, gy_h, wqkv_h, bqkv_h, wout_h, wup_h, wdn_h, ln1g_h, ln1b_h, ln2g_h, ln2b_h, bout_h, bdown_h, bup_h,
                 y_o, gx_o, vec_o, part_o, h_o, ga_o, dpre_o, gy_o, dqkv_o, ctx_o, gt_o, rt_o,
                 wqkv, wout, wup, wdn, bqkv, vecs, xg, gyg, h, bias, qkv, prob, probb, ctx, x1, xhat, g, gt, rt, gact, r, dpre,
                 gmid, ga, dctx, dqkv, ybuf, gxbuf, xh1, vec, part, ubuf, xr, vt, dpb, dsb,
                 p1, rd1, s1, rs1, t1, q1, e1, p2, rd2, s2, rs2, t2, q2, e2, py, rdy, sy, rsy, ph, rdh, sh, rsh,
                 lsem, osem, ssem, rsem):
    D = x_h.shape[1]
    seq = TP * 32
    head = bqkv_h.shape[2]
    n_heads = bqkv_h.shape[1]
    nlc = D // LANES
    t = lax.axis_index('tp')
    core = lax.rem(t, 2)
    chip = t // 2
    sib = t + 1 - 2 * core
    cross = lax.rem(t + 2, TP)
    sibcross = lax.rem(sib + 2, TP)

    def slot(dev):
        return lax.rem(dev, 2) * 2 + dev // 2

    def rows(dev):
        return pl.ds(pl.multiple_of(slot(dev) * 32, 32), 32)

    own = rows(t)
    half = pl.ds(pl.multiple_of(core * 64, 64), 64)
    sibhalf = pl.ds(pl.multiple_of((1 - core) * 64, 64), 64)
    blk_own = pl.ds(pl.multiple_of(chip * 32, 32), 32)
    blk_cross = pl.ds(pl.multiple_of((1 - chip) * 32, 32), 32)

    counter = [0, 0, 0]

    def load(src, dst):
        k = counter[0]
        counter[0] += 1
        copy = pltpu.make_async_copy(src, dst, lsem.at[k])
        copy.start()
        return copy

    outs = []

    def store(src, dst):
        k = counter[1]
        counter[1] += 1
        copy = pltpu.make_async_copy(src, dst, osem.at[k])
        copy.start()
        outs.append(copy)

    sent = []

    def remote(src, dst, dev):
        k = counter[2]
        counter[2] += 1
        copy = pltpu.make_async_remote_copy(src_ref=src, dst_ref=dst, send_sem=ssem.at[k], recv_sem=rsem.at[k],
                                            device_id={'tp': dev}, device_id_type=MESH)
        copy.start()
        sent.append(copy)
        return copy

    def lc(c):
        return slice(c * LANES, (c + 1) * LANES)

    def groups(widths, j):
        start = sum(widths[:j])
        return range(start, start + widths[j])

    def cols(widths, j):
        return slice(sum(widths[:j]) * LANES, sum(widths[:j + 1]) * LANES)

    lx = load(x_h, xg.at[own, :])
    lg = load(gy_h, gyg.at[own, :])
    lvec = [load(src, vecs.at[k, 0]) for k, src in enumerate((ln1g_h, ln1b_h, ln2g_h, ln2b_h, bout_h, bdown_h, bup_h))]
    lb = load(bqkv_h, bqkv)
    lwqkv = load(wqkv_h, wqkv)
    lwout = load(wout_h, wout)
    barrier = pltpu.get_barrier_semaphore()
    for dev in (sib, cross, sibcross):
        pl.semaphore_signal(barrier, inc=1, device_id={'tp': dev}, device_id_type=MESH)
    pl.semaphore_wait(barrier, 3)
    lx.wait()
    def piece(dev, k):
        return pl.ds(pl.multiple_of(slot(dev) * 32 + 16 * k, 16), 16)

    x_to_cross = [remote(xg.at[piece(t, k), :], xg.at[piece(t, k), :], cross) for k in range(2)]
    x_to_sib = remote(xg.at[own, :], xg.at[own, :], sib)
    lg.wait()
    gy_to_sib = remote(gyg.at[own, :], gyg.at[own, :], sib)
    lwdn = load(wdn_h, wdn)
    lwup = load(wup_h, wup)
    for copy in lvec:
        copy.wait()

    def ln_block(rr, n, src, gain, shift, dst):
        acc = jnp.zeros((n, LANES), F32)
        for c in range(nlc):
            acc = acc + src[rr, lc(c)].astype(F32)
        mean = jnp.sum(acc, axis=1, keepdims=True) / D
        acc = jnp.zeros((n, LANES), F32)
        for c in range(nlc):
            z = src[rr, lc(c)].astype(F32) - mean
            acc = acc + z * z
        rstd = lax.rsqrt(jnp.sum(acc, axis=1, keepdims=True) / D + EPS)
        for c in range(nlc):
            z = (src[rr, lc(c)].astype(F32) - mean) * rstd
            if dst is not None:
                dst[rr, lc(c)] = (z * vecs[gain, :, lc(c)] + vecs[shift, :, lc(c)]).astype(BF)
            else:
                xh1[:, lc(c)] = z
        return rstd

    ln_block(own, 32, xg, 0, 1, h)
    lb.wait()
    for k in range(3):
        bt = bqkv[k].T
        for hd in range(n_heads):
            at = (hd * 3 + k) * head
            bias[at:at + head, :] = jnp.broadcast_to(bt[:head, hd:hd + 1], (head, seq))
    x_to_sib.wait_recv()
    ln_block(rows(sib), 32, xg, 0, 1, h)
    x_fwd = []
    for k in range(2):
        x_to_cross[k].wait_recv()
        x_fwd.append(remote(xg.at[piece(cross, k), :], xg.at[piece(cross, k), :], sib))
    gy_to_cross = remote(gyg.at[own, :], gyg.at[own, :], cross)
    lwqkv.wait()
    lwout.wait()
    ln_block(rows(cross), 32, xg, 0, 1, h)
    for k in range(2):
        x_fwd[k].wait_recv()
    ln_block(rows(sibcross), 32, xg, 0, 1, h)

    hr = 2 * 3 * head
    hv = h[...]
    for m in range(n_heads // 2):
        mm = slice(m * hr, (m + 1) * hr)
        qkv[mm, :] = (dot_t(wqkv[mm, :], hv) + bias[mm, :]).astype(BF)

    def position(axis):
        i = lax.broadcasted_iota(jnp.int32, (seq, seq), axis)
        b = i >> 5
        return ((((b & 1) << 1) | (b >> 1)) << 5) | (i & 31)

    pos_k = position(0)
    causal = pos_k <= position(1)
    key_f = pos_k.astype(F32)
    slopes = alibi_slopes(n_heads * TP)
    score_scale = head ** -0.5

    def part_of(hd, k):
        at = (hd * 3 + k) * head
        return slice(at, at + head)

    def slope(hd):
        v = jnp.float32(slopes[hd])
        for dev in range(1, TP):
            v = jnp.where(t == dev, jnp.float32(slopes[dev * n_heads + hd]), v)
        return v

    for hd in range(n_heads):
        s = dot(qkv[part_of(hd, 1), :].T, qkv[part_of(hd, 0), :]) * score_scale + slope(hd) * key_f
        s = jnp.where(causal, s, MASK_VALUE)
        e = jnp.exp(s - jnp.max(s, axis=0, keepdims=True))
        pr = e * (1.0 / jnp.sum(e, axis=0, keepdims=True))
        prob[hd] = pr
        probb[hd] = pr.astype(BF)
    for hd in range(n_heads):
        ctx[hd * head:(hd + 1) * head, :] = dot(qkv[part_of(hd, 2), :], probb[hd]).astype(BF)

    class AllSum:
        widths = ALL_CHUNKS

        def __init__(self, p, rd, s, rs, tt, q, e):
            self.p, self.rd, self.s, self.rs, self.tt, self.q, self.e = p, rd, s, rs, tt, q, e
            self.a, self.b, self.c = {}, {}, {}
            self.last = len(self.widths) - 1

        def ch(self, j):
            return cols(self.widths, j)

        def fill(self, j, value):
            self.p[:, self.ch(j)] = value

        def put(self, j):
            self.a[j] = remote(self.p.at[sibhalf, self.ch(j)], self.rd.at[:, self.ch(j)], sib)

        def pair(self, j):
            self.a[j].wait_recv()
            c = self.ch(j)
            self.s[:, c] = (self.p[half, c].astype(F32) + self.rd[:, c].astype(F32)).astype(BF)

        def step_cross(self, j):
            self.pair(j)
            c = self.ch(j)
            self.b[j] = remote(self.s.at[:, c], self.rs.at[:, c], cross)
            if j == self.last:
                self.c[j] = (remote(self.s.at[:, c], self.e.at[:, :], sibcross), remote(self.s.at[:, c], self.q.at[:, :], sib))

        def step_back(self, j):
            self.b[j].wait_recv()
            c = self.ch(j)
            self.tt[half, c] = (self.s[:, c].astype(F32) + self.rs[:, c].astype(F32)).astype(BF)
            if j < self.last:
                self.c[j] = remote(self.tt.at[half, c], self.tt.at[half, c], sib)

        def finish(self, j):
            if j < self.last:
                self.c[j].wait_recv()
            else:
                for copy in self.c[j]:
                    copy.wait_recv()
                self.tt[sibhalf, self.ch(j)] = (self.q[...].astype(F32) + self.e[...].astype(F32)).astype(BF)

    class ScatterSum(AllSum):
        widths = SCATTER_CHUNKS

        def step_cross(self, j):
            self.pair(j)
            c = self.ch(j)
            self.b[j] = remote(self.s.at[blk_cross, c], self.rs.at[:, c], cross)

        def result(self, c):
            return (self.s[blk_own, c].astype(F32) + self.rs[:, c].astype(F32)).astype(BF).astype(F32)

    o_flat = ctx[...].T
    sum_a = AllSum(p1, rd1, s1, rs1, t1, q1, e1)
    n_all = len(ALL_CHUNKS)
    sum_a.fill(0, dot(o_flat, wout[:, sum_a.ch(0)]).astype(BF))
    sum_a.put(0)
    for j in range(1, n_all):
        sum_a.fill(j, dot(o_flat, wout[:, sum_a.ch(j)]).astype(BF))
    for j in range(1, n_all):
        sum_a.put(j)
    for j in range(n_all):
        sum_a.step_cross(j)
    store(h, h_o)
    store(ctx, ctx_o)

    gy_to_sib.wait_recv()
    gy_to_cross.wait_recv()
    gy_fwd = remote(gyg.at[rows(cross), :], gyg.at[rows(cross), :], sib)
    for hd in range(n_heads):
        vt[hd] = qkv[part_of(hd, 2), :].T
    gy_fwd.wait_recv()
    store(gyg, gy_o)
    lwdn.wait()
    lwup.wait()
    fw = wdn_h.shape[0] // N_BLK
    acc = jnp.zeros((seq, LANES), F32)

    def x1_chunk(j, acc):
        sum_a.finish(j)
        for c in groups(ALL_CHUNKS, j):
            z = xg[:, lc(c)].astype(F32) + t1[:, lc(c)].astype(F32) + vecs[4, :, lc(c)]
            x1[:, lc(c)] = z
            acc = acc + z
        return acc

    gyv = gyg[...]
    for j in range(n_all):
        if j < N_BLK:
            ff = slice(j * fw, (j + 1) * fw)
            gact[:, ff] = dot_t(gyv, wdn[ff, :]).astype(BF)
        sum_a.step_back(j)
        if j:
            acc = x1_chunk(j - 1, acc)
    acc = x1_chunk(n_all - 1, acc)

    mean = jnp.sum(acc, axis=1, keepdims=True) / D
    halves = (slice(0, seq // 2), slice(seq // 2, seq))
    rstd2 = []
    for n, hh in enumerate(halves):
        acc = jnp.zeros((seq // 2, LANES), F32)
        for c in range(nlc):
            z = x1[hh, lc(c)] - mean[hh]
            acc = acc + z * z
        rstd2.append(lax.rsqrt(jnp.sum(acc, axis=1, keepdims=True) / D + EPS))
    for n, hh in enumerate(halves):
        for c in range(nlc):
            z = (x1[hh, lc(c)] - mean[hh]) * rstd2[n]
            xhat[hh, lc(c)] = z
            g[hh, lc(c)] = (z * vecs[2, :, lc(c)] + vecs[3, :, lc(c)]).astype(BF)

    gv = g[...]
    for j in range(N_BLK):
        ff = slice(j * fw, (j + 1) * fw)
        pre = dot(gv, wup[:, ff]) + vecs[6, :, ff]
        w = (GELU_C * GELU_A) * (pre * pre)
        th = jnp.tanh(pre * (GELU_C + w))
        hp = 0.5 * pre
        r[:, ff] = (hp + hp * th).astype(BF)
        slope_g = (0.5 + 0.5 * th) + (hp * (1.0 - th * th)) * (GELU_C + 3.0 * w)
        gp = gact[:, ff].astype(F32) * slope_g
        vec[6:7, ff] = jnp.sum(gp, axis=0, keepdims=True)
        dpre[:, ff] = gp.astype(BF)

    dv = dpre[...]
    sum_g = AllSum(p2, rd2, s2, rs2, t2, q2, e2)
    for j in range(n_all):
        sum_g.fill(j, dot_t(dv, wup[sum_g.ch(j), :]).astype(BF))
        sum_g.put(j)
        if j:
            sum_g.step_cross(j - 1)
    sum_g.step_cross(n_all - 1)
    store(dpre, dpre_o)

    acc1 = jnp.zeros((seq, LANES), F32)
    acc2 = jnp.zeros((seq, LANES), F32)

    def ln2_back_chunk(j, acc1, acc2):
        sum_g.finish(j)
        for c in groups(ALL_CHUNKS, j):
            dg = t2[:, lc(c)].astype(F32)
            z = xhat[:, lc(c)]
            dgz = dg * z
            vec[2:3, lc(c)] = jnp.sum(dgz, axis=0, keepdims=True)
            vec[3:4, lc(c)] = jnp.sum(dg, axis=0, keepdims=True)
            gain = vecs[2, :, lc(c)]
            dz = dg * gain
            acc1 = acc1 + dz
            acc2 = acc2 + dgz * gain
            for n, hh in enumerate(halves):
                ubuf[hh, lc(c)] = gyg[hh, lc(c)].astype(F32) + rstd2[n] * dz[hh]
        return acc1, acc2

    rv = r[...]
    yw = D // N_BLK
    for j in range(n_all):
        if j < N_BLK:
            yy = slice(j * yw, (j + 1) * yw)
            py[:, yy] = dot(rv, wdn[:, yy]).astype(BF)
            for c in range(j * (yw // LANES), (j + 1) * (yw // LANES)):
                gt[lc(c), :] = g[:, lc(c)].T
                rt[lc(c), :] = r[:, lc(c)].T
                vec[5:6, lc(c)] = jnp.sum(gyg[:, lc(c)].astype(F32), axis=0, keepdims=True)
                for n, hh in enumerate(halves):
                    xr[hh, lc(c)] = xhat[hh, lc(c)] * rstd2[n]
        if j == N_BLK:
            y_sib = remote(py.at[sibhalf, :], rdy, sib)
            store(gt, gt_o)
            store(rt, rt_o)
        sum_g.step_back(j)
        if j:
            acc1, acc2 = ln2_back_chunk(j - 1, acc1, acc2)
    y_sib.wait_recv()
    sy[...] = (py[half, :].astype(F32) + rdy[...].astype(F32)).astype(BF)
    y_cross = remote(sy.at[blk_cross, :], rsy, cross)
    acc1, acc2 = ln2_back_chunk(n_all - 1, acc1, acc2)

    for n, hh in enumerate(halves):
        mean1 = rstd2[n] * (jnp.sum(acc1[hh], axis=1, keepdims=True) / D)
        mean2 = jnp.sum(acc2[hh], axis=1, keepdims=True) / D
        for c in range(nlc):
            gm = ubuf[hh, lc(c)] - (mean1 + xr[hh, lc(c)] * mean2)
            gmid[hh, lc(c)] = gm
            ga[hh, lc(c)] = gm.astype(BF)

    gav = ga[...]
    hc = ctx.shape[0] // 2
    for k in range(2):
        dctx[k * hc:(k + 1) * hc, :] = dot_t(wout[k * hc:(k + 1) * hc, :], gav).astype(BF)

    def head_rows(hd):
        return slice(hd * head, (hd + 1) * head)

    for hd in range(n_heads):
        dpb[hd] = dot(vt[hd], dctx[head_rows(hd), :]).astype(BF)
    for hd in range(n_heads):
        dqkv[part_of(hd, 2), :] = dot_t(dctx[head_rows(hd), :], probb[hd]).astype(BF)
    for hd in range(n_heads):
        pr = prob[hd]
        dp = dpb[hd].astype(F32)
        dsb[hd] = (pr * (dp - jnp.sum(dp * pr, axis=0, keepdims=True))).astype(BF)
    for hd in range(n_heads):
        dqkv[part_of(hd, 0), :] = (dot(qkv[part_of(hd, 1), :], dsb[hd]) * score_scale).astype(BF)
        dqkv[part_of(hd, 1), :] = (dot_t(qkv[part_of(hd, 0), :], dsb[hd]) * score_scale).astype(BF)

    sum_h = ScatterSum(ph, rdh, sh, rsh, None, None, None)
    n_scat = len(SCATTER_CHUNKS)
    dq = dqkv[...].T
    for j in range(n_scat):
        sum_h.fill(j, dot(dq, wqkv[:, sum_h.ch(j)]).astype(BF))
        sum_h.put(j)
        if j:
            sum_h.step_cross(j - 1)
    sum_h.step_cross(n_scat - 1)
    store(ga, ga_o)
    store(dqkv, dqkv_o)

    rstd1 = ln_block(own, 32, xg, 0, 1, None)
    y_cross.wait_recv()
    for c in range(nlc):
        z = (sy[blk_own, lc(c)].astype(F32) + rsy[:, lc(c)].astype(F32)).astype(BF).astype(F32)
        ybuf[:, lc(c)] = (x1[own, lc(c)] + z + vecs[5, :, lc(c)]).astype(BF)
        vec[4:5, lc(c)] = jnp.sum(gmid[:, lc(c)], axis=0, keepdims=True)
    store(ybuf, y_o)
    store(vec, vec_o)

    me = slot(t)
    acc1 = jnp.zeros((32, LANES), F32)
    acc2 = jnp.zeros((32, LANES), F32)
    for j in range(n_scat):
        sum_h.b[j].wait_recv()
        for c in groups(SCATTER_CHUNKS, j):
            dh = sum_h.result(lc(c))
            z = xh1[:, lc(c)]
            dhz = dh * z
            part[0:1, lc(c)] = jnp.sum(dhz, axis=0, keepdims=True)
            part[1:2, lc(c)] = jnp.sum(dh, axis=0, keepdims=True)
            gain = vecs[0, :, lc(c)]
            acc1 = acc1 + dh * gain
            acc2 = acc2 + dhz * gain
    parts = [remote(part, part_o.at[me], dev) for dev in (cross, sibcross, sib)]
    store(part, part_o.at[me])
    mean1 = jnp.sum(acc1, axis=1, keepdims=True) / D
    mean2 = jnp.sum(acc2, axis=1, keepdims=True) / D
    for c in range(nlc):
        dz = sum_h.result(lc(c)) * vecs[0, :, lc(c)]
        gxbuf[:, lc(c)] = (gmid[own, lc(c)] + rstd1 * (dz - mean1 - xh1[:, lc(c)] * mean2)).astype(BF)
    store(gxbuf, gx_o)
    for copy in sent:
        copy.wait_send()
    for copy in outs:
        copy.wait()
    for copy in parts:
        copy.wait_recv()


def grad_kernel(h_h, ga_h, dpre_h, gy_h, dqkv_h, ctx_h, gt_h, rt_h, vec_h, part_h, y_h, gx_h,
                dwqkv_o, dwout_o, dwup_o, dwdn_o, dbqkv_o, y_o, gx_o, v0, v1, v2, v3, v4, v5, v6,
                h, ga, dpre, gy, dqkv, ctx, gt, rt, vec, part, y, gx, buf, isem, osem):
    n_heads, head = dbqkv_o.shape[1], dbqkv_o.shape[2]
    block = 320
    slots = buf.shape[0]
    pairs = ((rt_h, rt), (gy_h, gy), (gt_h, gt), (dpre_h, dpre), (dqkv_h, dqkv), (h_h, h), (ctx_h, ctx), (ga_h, ga), (vec_h, vec),
             (part_h, part), (y_h, y), (gx_h, gx))
    loads = []

    def fetch(n):
        for src, dst in pairs[len(loads):n]:
            copy = pltpu.make_async_copy(src, dst, isem.at[len(loads)])
            copy.start()
            loads.append(copy)

    fetch(2)
    step = 0
    pending = []
    for n, (left, right, out) in enumerate(((rt, gy, dwdn_o), (gt, dpre, dwup_o), (dqkv, h, dwqkv_o), (ctx, ga, dwout_o))):
        loads[2 * n].wait()
        loads[2 * n + 1].wait()
        if n == 0:
            fetch(len(pairs))
        rv = right[...]
        for m in range(left.shape[0] // block):
            s = step % slots
            if step >= slots:
                pending[step - slots].wait()
            mm = slice(m * block, (m + 1) * block)
            buf[s] = dot(left[mm, :], rv).astype(BF)
            copy = pltpu.make_async_copy(buf.at[s], out.at[pl.ds(m * block, block), :], osem.at[s])
            copy.start()
            pending.append(copy)
            step += 1
    ones = jnp.ones((8, dqkv.shape[1]), BF)
    sums = dot_t(ones, dqkv[...])[0:1]
    for k in range(3):
        for hd in range(n_heads):
            at = (hd * 3 + k) * head
            dbqkv_o[k, hd:hd + 1, :] = sums[:, at:at + head]
    for k in range(8, 12):
        loads[k].wait()
    y_o[...] = y[...]
    gx_o[...] = gx[...]
    for k, o in enumerate((v0, v1)):
        o[...] = (part[0, k, :] + part[1, k, :]) + (part[2, k, :] + part[3, k, :])
    for k, o in enumerate((v2, v3, v4, v5, v6)):
        o[...] = vec[2 + k, :]
    for k in range(max(0, step - slots), step):
        pending[k].wait()


def solution(mesh):
    def local_step(x, ln1_gamma, ln1_beta, w_qkv, b_qkv, w_out, b_out, ln2_gamma, ln2_beta, w_up, b_up, w_down, b_down, grad_y):
        D = x.shape[2]
        S = TP * x.shape[1]
        nh, head = w_qkv.shape[1], w_qkv.shape[3]
        Q = nh * 3 * head
        C = nh * head
        FL = w_up.shape[1]
        any_spec = pl.BlockSpec(memory_space=pl.ANY)
        vm = pltpu.VMEM
        wqkv_t = jnp.transpose(w_qkv, (1, 2, 3, 0)).reshape(Q, D)
        bq = jnp.transpose(b_qkv, (1, 0, 2))
        sds = jax.ShapeDtypeStruct
        n_loads = 2 + 7 + 1 + 4
        red = [vm((S, D), BF), vm((S // 2, D), BF), vm((S // 2, D), BF), vm((S // 2, D), BF), vm((S, D), BF),
               vm((S // 2, ALL_CHUNKS[-1] * LANES), BF), vm((S // 2, ALL_CHUNKS[-1] * LANES), BF)]
        scat = [vm((S, D), BF), vm((S // 2, D), BF), vm((S // 2, D), BF), vm((S // TP, D), BF)]
        row = lambda v: v
        res = pl.pallas_call(
            layer_kernel,
            name='layer',
            out_shape=[sds((S // TP, D), BF), sds((S // TP, D), BF), sds((8, D), F32), sds((TP, 2, D), F32), sds((S, D), BF), sds((S, D), BF),
                       sds((S, FL), BF), sds((S, D), BF), sds((Q, S), BF), sds((C, S), BF), sds((D, S), BF), sds((FL, S), BF)],
            in_specs=[any_spec] * 14,
            out_specs=[any_spec] * 12,
            scratch_shapes=[
                vm((Q, D), BF), vm((C, D), BF), vm((D, FL), BF), vm((FL, D), BF), vm((3, nh, head), F32), vm((7, 1, D), F32),
                vm((S, D), BF), vm((S, D), BF), vm((S, D), BF), vm((Q, S), F32), vm((Q, S), BF), vm((nh, S, S), F32),
                vm((nh, S, S), BF), vm((C, S), BF), vm((S, D), F32), vm((S, D), F32), vm((S, D), BF), vm((D, S), BF), vm((FL, S), BF),
                vm((S, FL), BF), vm((S, FL), BF), vm((S, FL), BF), vm((S, D), F32), vm((S, D), BF), vm((C, S), BF), vm((Q, S), BF),
                vm((S // TP, D), BF), vm((S // TP, D), BF), vm((S // TP, D), F32), vm((8, D), F32), vm((2, D), F32), vm((S, D), F32), vm((S, D), F32),
                vm((nh, S, head), BF), vm((nh, S, S), BF), vm((nh, S, S), BF),
                *red, *red, *scat, *scat,
                pltpu.SemaphoreType.DMA((n_loads,)), pltpu.SemaphoreType.DMA((N_STORE,)),
                pltpu.SemaphoreType.DMA((N_REMOTE,)), pltpu.SemaphoreType.DMA((N_REMOTE,)),
            ],
            compiler_params=pltpu.CompilerParams(collective_id=0, has_side_effects=True, vmem_limit_bytes=67043328),
        )(x.reshape(x.shape[1], D), grad_y.reshape(x.shape[1], D), wqkv_t, bq, w_out, w_up, w_down, row(ln1_gamma), row(ln1_beta),
          row(ln2_gamma), row(ln2_beta), row(b_out), row(b_down), row(b_up))
        y, gx, vec, part, h, ga, dpre, gyf, dqkv, ctx, gt, rt = res
        vspec = pl.BlockSpec(memory_space=pltpu.VMEM)
        vshape = sds((D,), F32)
        outs = pl.pallas_call(
            grad_kernel,
            name='weight_grads',
            out_shape=[sds((Q, D), BF), sds((C, D), BF), sds((D, FL), BF), sds((FL, D), BF), sds((3, nh, head), F32),
                       sds((S // TP, D), BF), sds((S // TP, D), BF)] + [vshape] * 7,
            in_specs=[any_spec] * 12,
            out_specs=[any_spec] * 4 + [vspec] * 10,
            scratch_shapes=[
                vm((S, D), BF), vm((S, D), BF), vm((S, FL), BF), vm((S, D), BF), vm((Q, S), BF), vm((C, S), BF), vm((D, S), BF),
                vm((FL, S), BF), vm((8, D), F32), vm((TP, 2, D), F32), vm((S // TP, D), BF), vm((S // TP, D), BF), vm((4, 320, D), BF),
                pltpu.SemaphoreType.DMA((12,)), pltpu.SemaphoreType.DMA((4,)),
            ],
            compiler_params=pltpu.CompilerParams(vmem_limit_bytes=60 * 1024 * 1024),
        )(h, ga, dpre, gyf, dqkv, ctx, gt, rt, vec, part, y, gx)
        dwqkv, dwout, dwup, dwdn, dbqkv, y, gx, g_ln1g, g_ln1b, g_ln2g, g_ln2b, g_bout, g_bdown, g_bup = outs
        dwqkv = jnp.transpose(dwqkv.reshape(nh, 3, head, D), (3, 0, 1, 2))
        dbqkv = jnp.transpose(dbqkv, (1, 0, 2))
        return (y.reshape(x.shape), gx.reshape(x.shape), g_ln1g, g_ln1b, dwqkv, dbqkv, dwout, g_bout,
                g_ln2g, g_ln2b, dwup, g_bup, dwdn, g_bdown)

    row_spec = P('dp', 'tp', None)
    in_specs = (row_spec, P(), P(), P(None, 'tp', None, None), P('tp', None, None), P('tp', None), P(), P(), P(),
                P(None, 'tp'), P('tp'), P('tp', None), P(), row_spec)
    out_specs = (row_spec, row_spec, P('dp'), P('dp'), P('dp', 'tp', None, None), P(('dp', 'tp'), None, None),
                 P(('dp', 'tp'), None), P('dp'), P('dp'), P('dp'), P('dp', 'tp'), P(('dp', 'tp')), P(('dp', 'tp'), None), P('dp'))
    return jax.shard_map(local_step, mesh=mesh, in_specs=in_specs, out_specs=out_specs, check_vma=False)
```

```python
import functools
import math
import jax
import jax.numpy as jnp
from jax import lax
from jax.experimental import pallas as pl
from jax.experimental.pallas import tpu as pltpu
from jax.sharding import PartitionSpec as P

EPS = 1e-5
MASK_VALUE = -1e30
BF = jnp.bfloat16
F32 = jnp.float32
MESH = pl.DeviceIdType.MESH
GELU_C = math.sqrt(2.0 / math.pi)
GELU_A = 0.044715
TP = 4
LANES = 128
ALL_CHUNKS = (2, 4, 4, 5, 4, 1)
SCATTER_CHUNKS = (6, 6, 5, 3)
N_BLK = 5
N_REMOTE = 59
N_STORE = 12


def alibi_slopes(n_heads):
    closest = 2 ** int(math.floor(math.log2(n_heads)))
    base_ratio = 2.0 ** (-8.0 / closest)
    extra_ratio = 2.0 ** (-4.0 / closest)
    remaining = min(closest, n_heads - closest)
    slopes = [base_ratio ** (i + 1) for i in range(closest)]
    return slopes + [extra_ratio ** (2 * i + 1) for i in range(remaining)]


def dot(lhs, rhs):
    return lax.dot_general(lhs, rhs, (((1,), (0,)), ((), ())), preferred_element_type=F32)


def dot_t(lhs, rhs):
    return lax.dot_general(lhs, rhs, (((1,), (1,)), ((), ())), preferred_element_type=F32)


def layer_kernel(x_h, gy_h, wqkv_h, bqkv_h, wout_h, wup_h, wdn_h, ln1g_h, ln1b_h, ln2g_h, ln2b_h, bout_h, bdown_h, bup_h,
                 y_o, gx_o, vec_o, part_o, h_o, ga_o, dpre_o, gy_o, dqkv_o, ctx_o, gt_o, rt_o,
                 wqkv, wout, wup, wdn, bqkv, vecs, xg, gyg, h, bias, qkv, prob, probb, ctx, x1, xhat, g, gt, rt, gact, r, dpre,
                 gmid, ga, dctx, dqkv, ybuf, gxbuf, xh1, vec, part, ubuf, xr, vt, dpb, dsb,
                 p1, rd1, s1, rs1, t1, q1, e1, p2, rd2, s2, rs2, t2, q2, e2, py, rdy, sy, rsy, ph, rdh, sh, rsh,
                 lsem, osem, ssem, rsem):
    D = x_h.shape[1]
    seq = TP * 32
    head = bqkv_h.shape[2]
    n_heads = bqkv_h.shape[1]
    nlc = D // LANES
    t = lax.axis_index('tp')
    core = lax.rem(t, 2)
    chip = t // 2
    sib = t + 1 - 2 * core
    cross = lax.rem(t + 2, TP)
    sibcross = lax.rem(sib + 2, TP)

    def slot(dev):
        return lax.rem(dev, 2) * 2 + dev // 2

    def rows(dev):
        return pl.ds(pl.multiple_of(slot(dev) * 32, 32), 32)

    own = rows(t)
    half = pl.ds(pl.multiple_of(core * 64, 64), 64)
    sibhalf = pl.ds(pl.multiple_of((1 - core) * 64, 64), 64)
    blk_own = pl.ds(pl.multiple_of(chip * 32, 32), 32)
    blk_cross = pl.ds(pl.multiple_of((1 - chip) * 32, 32), 32)

    counter = [0, 0, 0]

    def load(src, dst):
        k = counter[0]
        counter[0] += 1
        copy = pltpu.make_async_copy(src, dst, lsem.at[k])
        copy.start()
        return copy

    outs = []

    def store(src, dst):
        k = counter[1]
        counter[1] += 1
        copy = pltpu.make_async_copy(src, dst, osem.at[k])
        copy.start()
        outs.append(copy)

    sent = []

    def remote(src, dst, dev):
        k = counter[2]
        counter[2] += 1
        copy = pltpu.make_async_remote_copy(src_ref=src, dst_ref=dst, send_sem=ssem.at[k], recv_sem=rsem.at[k],
                                            device_id={'tp': dev}, device_id_type=MESH)
        copy.start()
        sent.append(copy)
        return copy

    def lc(c):
        return slice(c * LANES, (c + 1) * LANES)

    def groups(widths, j):
        start = sum(widths[:j])
        return range(start, start + widths[j])

    def cols(widths, j):
        return slice(sum(widths[:j]) * LANES, sum(widths[:j + 1]) * LANES)

    lx = load(x_h, xg.at[own, :])
    lg = load(gy_h, gyg.at[own, :])
    lvec = [load(src, vecs.at[k, 0]) for k, src in enumerate((ln1g_h, ln1b_h, ln2g_h, ln2b_h, bout_h, bdown_h, bup_h))]
    lb = load(bqkv_h, bqkv)
    lwqkv = load(wqkv_h, wqkv)
    lwout = load(wout_h, wout)
    barrier = pltpu.get_barrier_semaphore()
    for dev in (sib, cross, sibcross):
        pl.semaphore_signal(barrier, inc=1, device_id={'tp': dev}, device_id_type=MESH)
    pl.semaphore_wait(barrier, 3)
    lx.wait()
    def piece(dev, k):
        return pl.ds(pl.multiple_of(slot(dev) * 32 + 16 * k, 16), 16)

    x_to_cross = [remote(xg.at[piece(t, k), :], xg.at[piece(t, k), :], cross) for k in range(2)]
    x_to_sib = remote(xg.at[own, :], xg.at[own, :], sib)
    lg.wait()
    gy_to_sib = remote(gyg.at[own, :], gyg.at[own, :], sib)
    lwdn = load(wdn_h, wdn)
    lwup = load(wup_h, wup)
    for copy in lvec:
        copy.wait()

    def ln_block(rr, n, src, gain, shift, dst):
        acc = jnp.zeros((n, LANES), F32)
        for c in range(nlc):
            acc = acc + src[rr, lc(c)].astype(F32)
        mean = jnp.sum(acc, axis=1, keepdims=True) / D
        acc = jnp.zeros((n, LANES), F32)
        for c in range(nlc):
            z = src[rr, lc(c)].astype(F32) - mean
            acc = acc + z * z
        rstd = lax.rsqrt(jnp.sum(acc, axis=1, keepdims=True) / D + EPS)
        for c in range(nlc):
            z = (src[rr, lc(c)].astype(F32) - mean) * rstd
            if dst is not None:
                dst[rr, lc(c)] = (z * vecs[gain, :, lc(c)] + vecs[shift, :, lc(c)]).astype(BF)
            else:
                xh1[:, lc(c)] = z
        return rstd

    ln_block(own, 32, xg, 0, 1, h)
    lb.wait()
    for k in range(3):
        bt = bqkv[k].T
        for hd in range(n_heads):
            at = (hd * 3 + k) * head
            bias[at:at + head, :] = jnp.broadcast_to(bt[:head, hd:hd + 1], (head, seq))
    x_to_sib.wait_recv()
    ln_block(rows(sib), 32, xg, 0, 1, h)
    x_fwd = []
    for k in range(2):
        x_to_cross[k].wait_recv()
        x_fwd.append(remote(xg.at[piece(cross, k), :], xg.at[piece(cross, k), :], sib))
    gy_to_cross = remote(gyg.at[own, :], gyg.at[own, :], cross)
    lwqkv.wait()
    lwout.wait()
    ln_block(rows(cross), 32, xg, 0, 1, h)
    for k in range(2):
        x_fwd[k].wait_recv()
    ln_block(rows(sibcross), 32, xg, 0, 1, h)

    hr = 2 * 3 * head
    hv = h[...]
    for m in range(n_heads // 2):
        mm = slice(m * hr, (m + 1) * hr)
        qkv[mm, :] = (dot_t(wqkv[mm, :], hv) + bias[mm, :]).astype(BF)

    def position(axis):
        i = lax.broadcasted_iota(jnp.int32, (seq, seq), axis)
        b = i >> 5
        return ((((b & 1) << 1) | (b >> 1)) << 5) | (i & 31)

    pos_k = position(0)
    causal = pos_k <= position(1)
    key_f = pos_k.astype(F32)
    slopes = alibi_slopes(n_heads * TP)
    score_scale = head ** -0.5

    def part_of(hd, k):
        at = (hd * 3 + k) * head
        return slice(at, at + head)

    def slope(hd):
        v = jnp.float32(slopes[hd])
        for dev in range(1, TP):
            v = jnp.where(t == dev, jnp.float32(slopes[dev * n_heads + hd]), v)
        return v

    for hd in range(n_heads):
        prob[hd] = dot(qkv[part_of(hd, 1), :].T, qkv[part_of(hd, 0), :])
    for hd in range(n_heads):
        s = jnp.where(causal, prob[hd] * score_scale + slope(hd) * key_f, MASK_VALUE)
        e = jnp.exp(s - jnp.max(s, axis=0, keepdims=True))
        pr = e * (1.0 / jnp.sum(e, axis=0, keepdims=True))
        prob[hd] = pr
        probb[hd] = pr.astype(BF)
    for hd in range(n_heads):
        ctx[hd * head:(hd + 1) * head, :] = dot(qkv[part_of(hd, 2), :], probb[hd]).astype(BF)

    class AllSum:
        widths = ALL_CHUNKS

        def __init__(self, p, rd, s, rs, tt, q, e):
            self.p, self.rd, self.s, self.rs, self.tt, self.q, self.e = p, rd, s, rs, tt, q, e
            self.a, self.b, self.c = {}, {}, {}
            self.last = len(self.widths) - 1

        def ch(self, j):
            return cols(self.widths, j)

        def fill(self, j, value):
            self.p[:, self.ch(j)] = value

        def put(self, j):
            self.a[j] = remote(self.p.at[sibhalf, self.ch(j)], self.rd.at[:, self.ch(j)], sib)

        def pair(self, j):
            self.a[j].wait_recv()
            c = self.ch(j)
            self.s[:, c] = (self.p[half, c].astype(F32) + self.rd[:, c].astype(F32)).astype(BF)

        def step_cross(self, j):
            self.pair(j)
            c = self.ch(j)
            self.b[j] = remote(self.s.at[:, c], self.rs.at[:, c], cross)
            if j == self.last:
                self.c[j] = (remote(self.s.at[:, c], self.e.at[:, :], sibcross), remote(self.s.at[:, c], self.q.at[:, :], sib))

        def step_back(self, j):
            self.b[j].wait_recv()
            c = self.ch(j)
            self.tt[half, c] = (self.s[:, c].astype(F32) + self.rs[:, c].astype(F32)).astype(BF)
            if j < self.last:
                self.c[j] = remote(self.tt.at[half, c], self.tt.at[half, c], sib)

        def finish(self, j):
            if j < self.last:
                self.c[j].wait_recv()
            else:
                for copy in self.c[j]:
                    copy.wait_recv()
                self.tt[sibhalf, self.ch(j)] = (self.q[...].astype(F32) + self.e[...].astype(F32)).astype(BF)

    class ScatterSum(AllSum):
        widths = SCATTER_CHUNKS

        def step_cross(self, j):
            self.pair(j)
            c = self.ch(j)
            self.b[j] = remote(self.s.at[blk_cross, c], self.rs.at[:, c], cross)

        def result(self, c):
            return (self.s[blk_own, c].astype(F32) + self.rs[:, c].astype(F32)).astype(BF).astype(F32)

    o_flat = ctx[...].T
    sum_a = AllSum(p1, rd1, s1, rs1, t1, q1, e1)
    n_all = len(ALL_CHUNKS)
    sum_a.fill(0, dot(o_flat, wout[:, sum_a.ch(0)]).astype(BF))
    sum_a.put(0)
    for j in range(1, n_all):
        sum_a.fill(j, dot(o_flat, wout[:, sum_a.ch(j)]).astype(BF))
    for j in range(1, n_all):
        sum_a.put(j)
    for j in range(n_all):
        sum_a.step_cross(j)
    store(h, h_o)
    store(ctx, ctx_o)

    gy_to_sib.wait_recv()
    gy_to_cross.wait_recv()
    gy_fwd = remote(gyg.at[rows(cross), :], gyg.at[rows(cross), :], sib)
    for hd in range(n_heads):
        vt[hd] = qkv[part_of(hd, 2), :].T
    gy_fwd.wait_recv()
    store(gyg, gy_o)
    lwdn.wait()
    lwup.wait()
    fw = wdn_h.shape[0] // N_BLK
    acc = jnp.zeros((seq, LANES), F32)

    def x1_chunk(j, acc):
        sum_a.finish(j)
        for c in groups(ALL_CHUNKS, j):
            z = xg[:, lc(c)].astype(F32) + t1[:, lc(c)].astype(F32) + vecs[4, :, lc(c)]
            x1[:, lc(c)] = z
            acc = acc + z
        return acc

    gyv = gyg[...]
    for j in range(n_all):
        if j < N_BLK:
            ff = slice(j * fw, (j + 1) * fw)
            gact[:, ff] = dot_t(gyv, wdn[ff, :]).astype(BF)
        sum_a.step_back(j)
        if j:
            acc = x1_chunk(j - 1, acc)
    acc = x1_chunk(n_all - 1, acc)

    mean = jnp.sum(acc, axis=1, keepdims=True) / D
    halves = (slice(0, seq // 2), slice(seq // 2, seq))
    rstd2 = []
    for n, hh in enumerate(halves):
        acc = jnp.zeros((seq // 2, LANES), F32)
        for c in range(nlc):
            z = x1[hh, lc(c)] - mean[hh]
            acc = acc + z * z
        rstd2.append(lax.rsqrt(jnp.sum(acc, axis=1, keepdims=True) / D + EPS))
    for n, hh in enumerate(halves):
        for c in range(nlc):
            z = (x1[hh, lc(c)] - mean[hh]) * rstd2[n]
            xhat[hh, lc(c)] = z
            g[hh, lc(c)] = (z * vecs[2, :, lc(c)] + vecs[3, :, lc(c)]).astype(BF)

    gv = g[...]
    for j in range(N_BLK):
        ff = slice(j * fw, (j + 1) * fw)
        pre = dot(gv, wup[:, ff]) + vecs[6, :, ff]
        w = (GELU_C * GELU_A) * (pre * pre)
        th = jnp.tanh(pre * (GELU_C + w))
        hp = 0.5 * pre
        r[:, ff] = (hp + hp * th).astype(BF)
        slope_g = (0.5 + 0.5 * th) + (hp * (1.0 - th * th)) * (GELU_C + 3.0 * w)
        gp = gact[:, ff].astype(F32) * slope_g
        vec[6:7, ff] = jnp.sum(gp, axis=0, keepdims=True)
        dpre[:, ff] = gp.astype(BF)

    dv = dpre[...]
    sum_g = AllSum(p2, rd2, s2, rs2, t2, q2, e2)
    for j in range(n_all):
        sum_g.fill(j, dot_t(dv, wup[sum_g.ch(j), :]).astype(BF))
        sum_g.put(j)
        if j:
            sum_g.step_cross(j - 1)
    sum_g.step_cross(n_all - 1)
    store(dpre, dpre_o)

    acc1 = jnp.zeros((seq, LANES), F32)
    acc2 = jnp.zeros((seq, LANES), F32)

    def ln2_back_chunk(j, acc1, acc2):
        sum_g.finish(j)
        for c in groups(ALL_CHUNKS, j):
            dg = t2[:, lc(c)].astype(F32)
            z = xhat[:, lc(c)]
            dgz = dg * z
            vec[2:3, lc(c)] = jnp.sum(dgz, axis=0, keepdims=True)
            vec[3:4, lc(c)] = jnp.sum(dg, axis=0, keepdims=True)
            gain = vecs[2, :, lc(c)]
            dz = dg * gain
            acc1 = acc1 + dz
            acc2 = acc2 + dgz * gain
            for n, hh in enumerate(halves):
                ubuf[hh, lc(c)] = gyg[hh, lc(c)].astype(F32) + rstd2[n] * dz[hh]
        return acc1, acc2

    rv = r[...]
    yw = D // N_BLK
    for j in range(n_all):
        if j < N_BLK:
            yy = slice(j * yw, (j + 1) * yw)
            py[:, yy] = dot(rv, wdn[:, yy]).astype(BF)
            for c in range(j * (yw // LANES), (j + 1) * (yw // LANES)):
                gt[lc(c), :] = g[:, lc(c)].T
                rt[lc(c), :] = r[:, lc(c)].T
                vec[5:6, lc(c)] = jnp.sum(gyg[:, lc(c)].astype(F32), axis=0, keepdims=True)
                for n, hh in enumerate(halves):
                    xr[hh, lc(c)] = xhat[hh, lc(c)] * rstd2[n]
        if j == N_BLK:
            y_sib = remote(py.at[sibhalf, :], rdy, sib)
            store(gt, gt_o)
            store(rt, rt_o)
        sum_g.step_back(j)
        if j:
            acc1, acc2 = ln2_back_chunk(j - 1, acc1, acc2)
    y_sib.wait_recv()
    sy[...] = (py[half, :].astype(F32) + rdy[...].astype(F32)).astype(BF)
    y_cross = remote(sy.at[blk_cross, :], rsy, cross)
    acc1, acc2 = ln2_back_chunk(n_all - 1, acc1, acc2)

    for n, hh in enumerate(halves):
        mean1 = rstd2[n] * (jnp.sum(acc1[hh], axis=1, keepdims=True) / D)
        mean2 = jnp.sum(acc2[hh], axis=1, keepdims=True) / D
        for c in range(nlc):
            gm = ubuf[hh, lc(c)] - (mean1 + xr[hh, lc(c)] * mean2)
            gmid[hh, lc(c)] = gm
            ga[hh, lc(c)] = gm.astype(BF)

    gav = ga[...]
    hc = ctx.shape[0] // 2
    for k in range(2):
        dctx[k * hc:(k + 1) * hc, :] = dot_t(wout[k * hc:(k + 1) * hc, :], gav).astype(BF)

    def head_rows(hd):
        return slice(hd * head, (hd + 1) * head)

    for hd in range(n_heads):
        dpb[hd] = dot(vt[hd], dctx[head_rows(hd), :]).astype(BF)
    for hd in range(n_heads):
        dqkv[part_of(hd, 2), :] = dot_t(dctx[head_rows(hd), :], probb[hd]).astype(BF)
    for hd in range(n_heads):
        pr = prob[hd]
        dp = dpb[hd].astype(F32)
        dsb[hd] = (pr * (dp - jnp.sum(dp * pr, axis=0, keepdims=True))).astype(BF)
    for hd in range(n_heads):
        dqkv[part_of(hd, 0), :] = (dot(qkv[part_of(hd, 1), :], dsb[hd]) * score_scale).astype(BF)
        dqkv[part_of(hd, 1), :] = (dot_t(qkv[part_of(hd, 0), :], dsb[hd]) * score_scale).astype(BF)

    sum_h = ScatterSum(ph, rdh, sh, rsh, None, None, None)
    n_scat = len(SCATTER_CHUNKS)
    dq = dqkv[...].T
    for j in range(n_scat):
        sum_h.fill(j, dot(dq, wqkv[:, sum_h.ch(j)]).astype(BF))
        sum_h.put(j)
        if j:
            sum_h.step_cross(j - 1)
    sum_h.step_cross(n_scat - 1)
    store(ga, ga_o)
    store(dqkv, dqkv_o)

    rstd1 = ln_block(own, 32, xg, 0, 1, None)
    y_cross.wait_recv()
    for c in range(nlc):
        z = (sy[blk_own, lc(c)].astype(F32) + rsy[:, lc(c)].astype(F32)).astype(BF).astype(F32)
        ybuf[:, lc(c)] = (x1[own, lc(c)] + z + vecs[5, :, lc(c)]).astype(BF)
        vec[4:5, lc(c)] = jnp.sum(gmid[:, lc(c)], axis=0, keepdims=True)
    store(ybuf, y_o)
    store(vec, vec_o)

    me = slot(t)
    acc1 = jnp.zeros((32, LANES), F32)
    acc2 = jnp.zeros((32, LANES), F32)
    for j in range(n_scat):
        sum_h.b[j].wait_recv()
        for c in groups(SCATTER_CHUNKS, j):
            dh = sum_h.result(lc(c))
            z = xh1[:, lc(c)]
            dhz = dh * z
            part[0:1, lc(c)] = jnp.sum(dhz, axis=0, keepdims=True)
            part[1:2, lc(c)] = jnp.sum(dh, axis=0, keepdims=True)
            gain = vecs[0, :, lc(c)]
            acc1 = acc1 + dh * gain
            acc2 = acc2 + dhz * gain
    parts = [remote(part, part_o.at[me], dev) for dev in (cross, sibcross, sib)]
    store(part, part_o.at[me])
    mean1 = jnp.sum(acc1, axis=1, keepdims=True) / D
    mean2 = jnp.sum(acc2, axis=1, keepdims=True) / D
    for c in range(nlc):
        dz = sum_h.result(lc(c)) * vecs[0, :, lc(c)]
        gxbuf[:, lc(c)] = (gmid[own, lc(c)] + rstd1 * (dz - mean1 - xh1[:, lc(c)] * mean2)).astype(BF)
    store(gxbuf, gx_o)
    for copy in sent:
        copy.wait_send()
    for copy in outs:
        copy.wait()
    for copy in parts:
        copy.wait_recv()


def grad_kernel(h_h, ga_h, dpre_h, gy_h, dqkv_h, ctx_h, gt_h, rt_h, vec_h, part_h, y_h, gx_h,
                dwqkv_o, dwout_o, dwup_o, dwdn_o, dbqkv_o, y_o, gx_o, v0, v1, v2, v3, v4, v5, v6,
                h, ga, dpre, gy, dqkv, ctx, gt, rt, vec, part, y, gx, buf, small, isem, osem, ssem):
    n_heads, head = dbqkv_o.shape[1], dbqkv_o.shape[2]
    slots, block = buf.shape[0], buf.shape[1]
    pairs = ((ctx_h, ctx), (ga_h, ga), (rt_h, rt), (gy_h, gy), (gt_h, gt), (dpre_h, dpre), (dqkv_h, dqkv), (h_h, h), (vec_h, vec),
             (part_h, part), (y_h, y), (gx_h, gx))
    loads = []

    def fetch(n):
        for src, dst in pairs[len(loads):n]:
            copy = pltpu.make_async_copy(src, dst, isem.at[len(loads)])
            copy.start()
            loads.append(copy)

    fetch(2)
    for copy in loads:
        copy.wait()
    fetch(len(pairs))
    tail = []

    def piece(k, start, size):
        small[k, pl.ds(0, size), :] = dot(ctx[start:start + size, :], ga[...]).astype(BF)
        copy = pltpu.make_async_copy(small.at[k, pl.ds(0, size), :], dwout_o.at[pl.ds(start, size), :], ssem.at[k])
        copy.start()
        tail.append(copy)

    def written(slot, out):
        return pltpu.make_async_copy(buf.at[slot], out.at[pl.ds(0, block), :], osem.at[slot])

    piece(0, 0, 160)
    first = 0
    for n, (left, right, out) in enumerate(((rt, gy, dwdn_o), (gt, dpre, dwup_o), (dqkv, h, dwqkv_o))):
        loads[2 * n + 2].wait()
        loads[2 * n + 3].wait()

        def body(m, carry, left=left, right=right, out=out, first=first):
            slot = lax.rem(first + m, slots)

            @pl.when(first + m >= slots)
            def _():
                written(slot, out).wait()

            at = pl.ds(pl.multiple_of(m * block, block), block)
            buf[slot] = dot(left[at, :], right[...]).astype(BF)
            pltpu.make_async_copy(buf.at[slot], out.at[at, :], osem.at[slot]).start()
            return carry

        count = left.shape[0] // block
        lax.fori_loop(0, count, body, 0)
        first += count
    piece(1, 160, 320)
    piece(2, 480, 160)
    ones = jnp.ones((8, dqkv.shape[1]), BF)
    sums = dot_t(ones, dqkv[...])[0:1]
    for k in range(3):
        for hd in range(n_heads):
            at = (hd * 3 + k) * head
            dbqkv_o[k, hd:hd + 1, :] = sums[:, at:at + head]
    for k in range(8, 12):
        loads[k].wait()
    y_o[...] = y[...]
    gx_o[...] = gx[...]
    for k, o in enumerate((v0, v1)):
        o[...] = (part[0, k, :] + part[1, k, :]) + (part[2, k, :] + part[3, k, :])
    for k, o in enumerate((v2, v3, v4, v5, v6)):
        o[...] = vec[2 + k, :]
    for k in range(slots):
        written(k, dwqkv_o).wait()
    for copy in tail:
        copy.wait()


def solution(mesh):
    def local_step(x, ln1_gamma, ln1_beta, w_qkv, b_qkv, w_out, b_out, ln2_gamma, ln2_beta, w_up, b_up, w_down, b_down, grad_y):
        D = x.shape[2]
        S = TP * x.shape[1]
        nh, head = w_qkv.shape[1], w_qkv.shape[3]
        Q = nh * 3 * head
        C = nh * head
        FL = w_up.shape[1]
        any_spec = pl.BlockSpec(memory_space=pl.ANY)
        vm = pltpu.VMEM
        wqkv_t = jnp.transpose(w_qkv, (1, 2, 3, 0)).reshape(Q, D)
        bq = jnp.transpose(b_qkv, (1, 0, 2))
        sds = jax.ShapeDtypeStruct
        n_loads = 2 + 7 + 1 + 4
        red = [vm((S, D), BF), vm((S // 2, D), BF), vm((S // 2, D), BF), vm((S // 2, D), BF), vm((S, D), BF),
               vm((S // 2, ALL_CHUNKS[-1] * LANES), BF), vm((S // 2, ALL_CHUNKS[-1] * LANES), BF)]
        scat = [vm((S, D), BF), vm((S // 2, D), BF), vm((S // 2, D), BF), vm((S // TP, D), BF)]
        row = lambda v: v
        res = pl.pallas_call(
            layer_kernel,
            name='layer',
            out_shape=[sds((S // TP, D), BF), sds((S // TP, D), BF), sds((8, D), F32), sds((TP, 2, D), F32), sds((S, D), BF), sds((S, D), BF),
                       sds((S, FL), BF), sds((S, D), BF), sds((Q, S), BF), sds((C, S), BF), sds((D, S), BF), sds((FL, S), BF)],
            in_specs=[any_spec] * 14,
            out_specs=[any_spec] * 12,
            scratch_shapes=[
                vm((Q, D), BF), vm((C, D), BF), vm((D, FL), BF), vm((FL, D), BF), vm((3, nh, head), F32), vm((7, 1, D), F32),
                vm((S, D), BF), vm((S, D), BF), vm((S, D), BF), vm((Q, S), F32), vm((Q, S), BF), vm((nh, S, S), F32),
                vm((nh, S, S), BF), vm((C, S), BF), vm((S, D), F32), vm((S, D), F32), vm((S, D), BF), vm((D, S), BF), vm((FL, S), BF),
                vm((S, FL), BF), vm((S, FL), BF), vm((S, FL), BF), vm((S, D), F32), vm((S, D), BF), vm((C, S), BF), vm((Q, S), BF),
                vm((S // TP, D), BF), vm((S // TP, D), BF), vm((S // TP, D), F32), vm((8, D), F32), vm((2, D), F32), vm((S, D), F32), vm((S, D), F32),
                vm((nh, S, head), BF), vm((nh, S, S), BF), vm((nh, S, S), BF),
                *red, *red, *scat, *scat,
                pltpu.SemaphoreType.DMA((n_loads,)), pltpu.SemaphoreType.DMA((N_STORE,)),
                pltpu.SemaphoreType.DMA((N_REMOTE,)), pltpu.SemaphoreType.DMA((N_REMOTE,)),
            ],
            compiler_params=pltpu.CompilerParams(collective_id=0, has_side_effects=True, vmem_limit_bytes=67043328),
        )(x.reshape(x.shape[1], D), grad_y.reshape(x.shape[1], D), wqkv_t, bq, w_out, w_up, w_down, row(ln1_gamma), row(ln1_beta),
          row(ln2_gamma), row(ln2_beta), row(b_out), row(b_down), row(b_up))
        y, gx, vec, part, h, ga, dpre, gyf, dqkv, ctx, gt, rt = res
        vspec = pl.BlockSpec(memory_space=pltpu.VMEM)
        vshape = sds((D,), F32)
        outs = pl.pallas_call(
            grad_kernel,
            name='weight_grads',
            out_shape=[sds((Q, D), BF), sds((C, D), BF), sds((D, FL), BF), sds((FL, D), BF), sds((3, nh, head), F32),
                       sds((S // TP, D), BF), sds((S // TP, D), BF)] + [vshape] * 7,
            in_specs=[any_spec] * 12,
            out_specs=[any_spec] * 4 + [vspec] * 10,
            scratch_shapes=[
                vm((S, D), BF), vm((S, D), BF), vm((S, FL), BF), vm((S, D), BF), vm((Q, S), BF), vm((C, S), BF), vm((D, S), BF),
                vm((FL, S), BF), vm((8, D), F32), vm((TP, 2, D), F32), vm((S // TP, D), BF), vm((S // TP, D), BF), vm((3, 640, D), BF), vm((3, 320, D), BF),
                pltpu.SemaphoreType.DMA((12,)), pltpu.SemaphoreType.DMA((3,)), pltpu.SemaphoreType.DMA((3,)),
            ],
            compiler_params=pltpu.CompilerParams(vmem_limit_bytes=60 * 1024 * 1024),
        )(h, ga, dpre, gyf, dqkv, ctx, gt, rt, vec, part, y, gx)
        dwqkv, dwout, dwup, dwdn, dbqkv, y, gx, g_ln1g, g_ln1b, g_ln2g, g_ln2b, g_bout, g_bdown, g_bup = outs
        dwqkv = jnp.transpose(dwqkv.reshape(nh, 3, head, D), (3, 0, 1, 2))
        dbqkv = jnp.transpose(dbqkv, (1, 0, 2))
        return (y.reshape(x.shape), gx.reshape(x.shape), g_ln1g, g_ln1b, dwqkv, dbqkv, dwout, g_bout,
                g_ln2g, g_ln2b, dwup, g_bup, dwdn, g_bdown)

    row_spec = P('dp', 'tp', None)
    in_specs = (row_spec, P(), P(), P(None, 'tp', None, None), P('tp', None, None), P('tp', None), P(), P(), P(),
                P(None, 'tp'), P('tp'), P('tp', None), P(), row_spec)
    out_specs = (row_spec, row_spec, P('dp'), P('dp'), P('dp', 'tp', None, None), P(('dp', 'tp'), None, None),
                 P(('dp', 'tp'), None), P('dp'), P('dp'), P('dp'), P('dp', 'tp'), P(('dp', 'tp')), P(('dp', 'tp'), None), P('dp'))
    return jax.shard_map(local_step, mesh=mesh, in_specs=in_specs, out_specs=out_specs, check_vma=False)
```

```python
import functools
import math
import jax
import jax.numpy as jnp
from jax import lax
from jax.experimental import pallas as pl
from jax.experimental.pallas import tpu as pltpu
from jax.sharding import PartitionSpec as P

EPS = 1e-5
MASK_VALUE = -1e30
BF = jnp.bfloat16
F32 = jnp.float32
MESH = pl.DeviceIdType.MESH
GELU_C = math.sqrt(2.0 / math.pi)
GELU_A = 0.044715
TP = 4
LANES = 128
ALL_CHUNKS = (2, 4, 4, 5, 4, 1)
SCATTER_CHUNKS = (6, 6, 5, 3)
N_BLK = 5
LAYER_VMEM = 59 * 1024 * 1024
GRAD_VMEM = 24 * 1024 * 1024
N_REMOTE = 59


def alibi_slopes(n_heads):
    closest = 2 ** int(math.floor(math.log2(n_heads)))
    base_ratio = 2.0 ** (-8.0 / closest)
    extra_ratio = 2.0 ** (-4.0 / closest)
    remaining = min(closest, n_heads - closest)
    slopes = [base_ratio ** (i + 1) for i in range(closest)]
    return slopes + [extra_ratio ** (2 * i + 1) for i in range(remaining)]


def dot(lhs, rhs):
    return lax.dot_general(lhs, rhs, (((1,), (0,)), ((), ())), preferred_element_type=F32)


def dot_t(lhs, rhs):
    return lax.dot_general(lhs, rhs, (((1,), (1,)), ((), ())), preferred_element_type=F32)


def layer_kernel(x_h, gy_h, wqkv_h, bqkv_h, wout_h, wup_h, wdn_h, ln1g_h, ln1b_h, ln2g_h, ln2b_h, bout_h, bdown_h, bup_h,
                 ybuf, gxbuf, vec, part_o, h, ga, dpre, gy_o, dqkv, ctx, gt, rt,
                 wqkv, wout, wup, wdn, bqkv, vecs, xg, gyg, bias, qkv, prob, probb, x1, xhat, g, gact, r,
                 gmid, dctx, xh1, ubuf, xr, vt, dpb, dsb,
                 p1, rd1, s1, rs1, t1, q1, e1, p2, rd2, s2, rs2, t2, q2, e2, py, rdy, sy, rsy, ph, rdh, sh, rsh,
                 lsem, ssem, rsem):
    D = x_h.shape[1]
    seq = TP * 32
    head = bqkv_h.shape[2]
    n_heads = bqkv_h.shape[1]
    nlc = D // LANES
    t = lax.axis_index('tp')
    core = lax.rem(t, 2)
    chip = t // 2
    sib = t + 1 - 2 * core
    cross = lax.rem(t + 2, TP)
    sibcross = lax.rem(sib + 2, TP)

    def slot(dev):
        return lax.rem(dev, 2) * 2 + dev // 2

    def rows(dev):
        return pl.ds(pl.multiple_of(slot(dev) * 32, 32), 32)

    own = rows(t)
    half = pl.ds(pl.multiple_of(core * 64, 64), 64)
    sibhalf = pl.ds(pl.multiple_of((1 - core) * 64, 64), 64)
    blk_own = pl.ds(pl.multiple_of(chip * 32, 32), 32)
    blk_cross = pl.ds(pl.multiple_of((1 - chip) * 32, 32), 32)

    counter = [0, 0]

    def load(src, dst):
        k = counter[0]
        counter[0] += 1
        copy = pltpu.make_async_copy(src, dst, lsem.at[k])
        copy.start()
        return copy

    sent = []

    def remote(src, dst, dev):
        k = counter[1]
        counter[1] += 1
        copy = pltpu.make_async_remote_copy(src_ref=src, dst_ref=dst, send_sem=ssem.at[k], recv_sem=rsem.at[k],
                                            device_id={'tp': dev}, device_id_type=MESH)
        copy.start()
        sent.append(copy)
        return copy

    def lc(c):
        return slice(c * LANES, (c + 1) * LANES)

    def groups(widths, j):
        start = sum(widths[:j])
        return range(start, start + widths[j])

    def cols(widths, j):
        return slice(sum(widths[:j]) * LANES, sum(widths[:j + 1]) * LANES)

    lx = load(x_h, xg.at[own, :])
    lg = load(gy_h, gyg.at[own, :])
    lvec = [load(src, vecs.at[k, 0]) for k, src in enumerate((ln1g_h, ln1b_h, ln2g_h, ln2b_h, bout_h, bdown_h, bup_h))]
    lb = load(bqkv_h, bqkv)
    lwqkv = load(wqkv_h, wqkv)
    lwout = load(wout_h, wout)
    barrier = pltpu.get_barrier_semaphore()
    for dev in (sib, cross, sibcross):
        pl.semaphore_signal(barrier, inc=1, device_id={'tp': dev}, device_id_type=MESH)
    pl.semaphore_wait(barrier, 3)
    lx.wait()
    def piece(dev, k):
        return pl.ds(pl.multiple_of(slot(dev) * 32 + 16 * k, 16), 16)

    x_to_cross = [remote(xg.at[piece(t, k), :], xg.at[piece(t, k), :], cross) for k in range(2)]
    x_to_sib = remote(xg.at[own, :], xg.at[own, :], sib)
    lg.wait()
    gy_to_sib = remote(gyg.at[own, :], gyg.at[own, :], sib)
    lwdn = load(wdn_h, wdn)
    lwup = load(wup_h, wup)
    for copy in lvec:
        copy.wait()

    def ln_block(rr, n, src, gain, shift, dst):
        acc = jnp.zeros((n, LANES), F32)
        for c in range(nlc):
            acc = acc + src[rr, lc(c)].astype(F32)
        mean = jnp.sum(acc, axis=1, keepdims=True) / D
        acc = jnp.zeros((n, LANES), F32)
        for c in range(nlc):
            z = src[rr, lc(c)].astype(F32) - mean
            acc = acc + z * z
        rstd = lax.rsqrt(jnp.sum(acc, axis=1, keepdims=True) / D + EPS)
        for c in range(nlc):
            z = (src[rr, lc(c)].astype(F32) - mean) * rstd
            if dst is not None:
                dst[rr, lc(c)] = (z * vecs[gain, :, lc(c)] + vecs[shift, :, lc(c)]).astype(BF)
            else:
                xh1[:, lc(c)] = z
        return rstd

    ln_block(own, 32, xg, 0, 1, h)
    lb.wait()
    for k in range(3):
        bt = bqkv[k].T
        for hd in range(n_heads):
            at = (hd * 3 + k) * head
            bias[at:at + head, :] = jnp.broadcast_to(bt[:head, hd:hd + 1], (head, seq))
    x_to_sib.wait_recv()
    ln_block(rows(sib), 32, xg, 0, 1, h)
    x_fwd = []
    for k in range(2):
        x_to_cross[k].wait_recv()
        x_fwd.append(remote(xg.at[piece(cross, k), :], xg.at[piece(cross, k), :], sib))
    gy_to_cross = remote(gyg.at[own, :], gyg.at[own, :], cross)
    lwqkv.wait()
    lwout.wait()
    ln_block(rows(cross), 32, xg, 0, 1, h)
    for k in range(2):
        x_fwd[k].wait_recv()
    ln_block(rows(sibcross), 32, xg, 0, 1, h)

    hr = 2 * 3 * head
    hv = h[...]
    for m in range(n_heads // 2):
        mm = slice(m * hr, (m + 1) * hr)
        qkv[mm, :] = (dot_t(wqkv[mm, :], hv) + bias[mm, :]).astype(BF)

    def position(axis):
        i = lax.broadcasted_iota(jnp.int32, (seq, seq), axis)
        b = i >> 5
        return ((((b & 1) << 1) | (b >> 1)) << 5) | (i & 31)

    pos_k = position(0)
    causal = pos_k <= position(1)
    key_f = pos_k.astype(F32)
    slopes = alibi_slopes(n_heads * TP)
    score_scale = head ** -0.5

    def part_of(hd, k):
        at = (hd * 3 + k) * head
        return slice(at, at + head)

    def slope(hd):
        v = jnp.float32(slopes[hd])
        for dev in range(1, TP):
            v = jnp.where(t == dev, jnp.float32(slopes[dev * n_heads + hd]), v)
        return v

    for hd in range(n_heads):
        prob[hd] = dot(qkv[part_of(hd, 1), :].T, qkv[part_of(hd, 0), :])
    for hd in range(n_heads):
        s = jnp.where(causal, prob[hd] * score_scale + slope(hd) * key_f, MASK_VALUE)
        e = jnp.exp(s - jnp.max(s, axis=0, keepdims=True))
        pr = e * (1.0 / jnp.sum(e, axis=0, keepdims=True))
        prob[hd] = pr
        probb[hd] = pr.astype(BF)
    for hd in range(n_heads):
        ctx[hd * head:(hd + 1) * head, :] = dot(qkv[part_of(hd, 2), :], probb[hd]).astype(BF)

    class AllSum:
        widths = ALL_CHUNKS

        def __init__(self, p, rd, s, rs, tt, q, e):
            self.p, self.rd, self.s, self.rs, self.tt, self.q, self.e = p, rd, s, rs, tt, q, e
            self.a, self.b, self.c = {}, {}, {}
            self.last = len(self.widths) - 1

        def ch(self, j):
            return cols(self.widths, j)

        def fill(self, j, value):
            self.p[:, self.ch(j)] = value

        def put(self, j):
            self.a[j] = remote(self.p.at[sibhalf, self.ch(j)], self.rd.at[:, self.ch(j)], sib)

        def pair(self, j):
            self.a[j].wait_recv()
            c = self.ch(j)
            self.s[:, c] = (self.p[half, c].astype(F32) + self.rd[:, c].astype(F32)).astype(BF)

        def step_cross(self, j):
            self.pair(j)
            c = self.ch(j)
            self.b[j] = remote(self.s.at[:, c], self.rs.at[:, c], cross)
            if j == self.last:
                self.c[j] = (remote(self.s.at[:, c], self.e.at[:, :], sibcross), remote(self.s.at[:, c], self.q.at[:, :], sib))

        def step_back(self, j):
            self.b[j].wait_recv()
            c = self.ch(j)
            self.tt[half, c] = (self.s[:, c].astype(F32) + self.rs[:, c].astype(F32)).astype(BF)
            if j < self.last:
                self.c[j] = remote(self.tt.at[half, c], self.tt.at[half, c], sib)

        def finish(self, j):
            if j < self.last:
                self.c[j].wait_recv()
            else:
                for copy in self.c[j]:
                    copy.wait_recv()
                self.tt[sibhalf, self.ch(j)] = (self.q[...].astype(F32) + self.e[...].astype(F32)).astype(BF)

    class ScatterSum(AllSum):
        widths = SCATTER_CHUNKS

        def step_cross(self, j):
            self.pair(j)
            c = self.ch(j)
            self.b[j] = remote(self.s.at[blk_cross, c], self.rs.at[:, c], cross)

        def result(self, c):
            return (self.s[blk_own, c].astype(F32) + self.rs[:, c].astype(F32)).astype(BF).astype(F32)

    o_flat = ctx[...].T
    sum_a = AllSum(p1, rd1, s1, rs1, t1, q1, e1)
    n_all = len(ALL_CHUNKS)
    sum_a.fill(0, dot(o_flat, wout[:, sum_a.ch(0)]).astype(BF))
    sum_a.put(0)
    for j in range(1, n_all):
        sum_a.fill(j, dot(o_flat, wout[:, sum_a.ch(j)]).astype(BF))
    for j in range(1, n_all):
        sum_a.put(j)
    for j in range(n_all):
        sum_a.step_cross(j)

    gy_to_sib.wait_recv()
    gy_to_cross.wait_recv()
    gy_fwd = remote(gyg.at[rows(cross), :], gyg.at[rows(cross), :], sib)
    for hd in range(n_heads):
        vt[hd] = qkv[part_of(hd, 2), :].T
    gy_fwd.wait_recv()
    gy_o[...] = gyg[...]
    lwdn.wait()
    lwup.wait()
    fw = wdn_h.shape[0] // N_BLK
    acc = jnp.zeros((seq, LANES), F32)

    def x1_chunk(j, acc):
        sum_a.finish(j)
        for c in groups(ALL_CHUNKS, j):
            z = xg[:, lc(c)].astype(F32) + t1[:, lc(c)].astype(F32) + vecs[4, :, lc(c)]
            x1[:, lc(c)] = z
            acc = acc + z
        return acc

    gyv = gyg[...]
    for j in range(n_all):
        if j < N_BLK:
            ff = slice(j * fw, (j + 1) * fw)
            gact[:, ff] = dot_t(gyv, wdn[ff, :]).astype(BF)
        sum_a.step_back(j)
        if j:
            acc = x1_chunk(j - 1, acc)
    acc = x1_chunk(n_all - 1, acc)

    mean = jnp.sum(acc, axis=1, keepdims=True) / D
    halves = (slice(0, seq // 2), slice(seq // 2, seq))
    rstd2 = []
    for n, hh in enumerate(halves):
        acc = jnp.zeros((seq // 2, LANES), F32)
        for c in range(nlc):
            z = x1[hh, lc(c)] - mean[hh]
            acc = acc + z * z
        rstd2.append(lax.rsqrt(jnp.sum(acc, axis=1, keepdims=True) / D + EPS))
    for n, hh in enumerate(halves):
        for c in range(nlc):
            z = (x1[hh, lc(c)] - mean[hh]) * rstd2[n]
            xhat[hh, lc(c)] = z
            g[hh, lc(c)] = (z * vecs[2, :, lc(c)] + vecs[3, :, lc(c)]).astype(BF)

    gv = g[...]
    for j in range(N_BLK):
        ff = slice(j * fw, (j + 1) * fw)
        pre = dot(gv, wup[:, ff]) + vecs[6, :, ff]
        w = (GELU_C * GELU_A) * (pre * pre)
        th = jnp.tanh(pre * (GELU_C + w))
        hp = 0.5 * pre
        r[:, ff] = (hp + hp * th).astype(BF)
        slope_g = (0.5 + 0.5 * th) + (hp * (1.0 - th * th)) * (GELU_C + 3.0 * w)
        gp = gact[:, ff].astype(F32) * slope_g
        vec[6, :, ff] = jnp.sum(gp, axis=0, keepdims=True)
        dpre[:, ff] = gp.astype(BF)

    dv = dpre[...]
    sum_g = AllSum(p2, rd2, s2, rs2, t2, q2, e2)
    for j in range(n_all):
        sum_g.fill(j, dot_t(dv, wup[sum_g.ch(j), :]).astype(BF))
        sum_g.put(j)
        if j:
            sum_g.step_cross(j - 1)
    sum_g.step_cross(n_all - 1)

    acc1 = jnp.zeros((seq, LANES), F32)
    acc2 = jnp.zeros((seq, LANES), F32)

    def ln2_back_chunk(j, acc1, acc2):
        sum_g.finish(j)
        for c in groups(ALL_CHUNKS, j):
            dg = t2[:, lc(c)].astype(F32)
            z = xhat[:, lc(c)]
            dgz = dg * z
            vec[2, :, lc(c)] = jnp.sum(dgz, axis=0, keepdims=True)
            vec[3, :, lc(c)] = jnp.sum(dg, axis=0, keepdims=True)
            gain = vecs[2, :, lc(c)]
            dz = dg * gain
            acc1 = acc1 + dz
            acc2 = acc2 + dgz * gain
            for n, hh in enumerate(halves):
                ubuf[hh, lc(c)] = gyg[hh, lc(c)].astype(F32) + rstd2[n] * dz[hh]
        return acc1, acc2

    rv = r[...]
    yw = D // N_BLK
    for j in range(n_all):
        if j < N_BLK:
            yy = slice(j * yw, (j + 1) * yw)
            py[:, yy] = dot(rv, wdn[:, yy]).astype(BF)
            for c in range(j * (yw // LANES), (j + 1) * (yw // LANES)):
                gt[lc(c), :] = g[:, lc(c)].T
                rt[lc(c), :] = r[:, lc(c)].T
                vec[5, :, lc(c)] = jnp.sum(gyg[:, lc(c)].astype(F32), axis=0, keepdims=True)
                for n, hh in enumerate(halves):
                    xr[hh, lc(c)] = xhat[hh, lc(c)] * rstd2[n]
        if j == N_BLK:
            y_sib = remote(py.at[sibhalf, :], rdy, sib)
        sum_g.step_back(j)
        if j:
            acc1, acc2 = ln2_back_chunk(j - 1, acc1, acc2)
    y_sib.wait_recv()
    sy[...] = (py[half, :].astype(F32) + rdy[...].astype(F32)).astype(BF)
    y_cross = remote(sy.at[blk_cross, :], rsy, cross)
    acc1, acc2 = ln2_back_chunk(n_all - 1, acc1, acc2)

    for n, hh in enumerate(halves):
        mean1 = rstd2[n] * (jnp.sum(acc1[hh], axis=1, keepdims=True) / D)
        mean2 = jnp.sum(acc2[hh], axis=1, keepdims=True) / D
        for c in range(nlc):
            gm = ubuf[hh, lc(c)] - (mean1 + xr[hh, lc(c)] * mean2)
            gmid[hh, lc(c)] = gm
            ga[hh, lc(c)] = gm.astype(BF)

    gav = ga[...]
    hc = ctx.shape[0] // 2
    for k in range(2):
        dctx[k * hc:(k + 1) * hc, :] = dot_t(wout[k * hc:(k + 1) * hc, :], gav).astype(BF)

    def head_rows(hd):
        return slice(hd * head, (hd + 1) * head)

    for hd in range(n_heads):
        dpb[hd] = dot(vt[hd], dctx[head_rows(hd), :]).astype(BF)
    for hd in range(n_heads):
        dqkv[part_of(hd, 2), :] = dot_t(dctx[head_rows(hd), :], probb[hd]).astype(BF)
    for hd in range(n_heads):
        pr = prob[hd]
        dp = dpb[hd].astype(F32)
        dsb[hd] = (pr * (dp - jnp.sum(dp * pr, axis=0, keepdims=True))).astype(BF)
    for hd in range(n_heads):
        dqkv[part_of(hd, 0), :] = (dot(qkv[part_of(hd, 1), :], dsb[hd]) * score_scale).astype(BF)
        dqkv[part_of(hd, 1), :] = (dot_t(qkv[part_of(hd, 0), :], dsb[hd]) * score_scale).astype(BF)

    sum_h = ScatterSum(ph, rdh, sh, rsh, None, None, None)
    n_scat = len(SCATTER_CHUNKS)
    dq = dqkv[...].T
    for j in range(n_scat):
        sum_h.fill(j, dot(dq, wqkv[:, sum_h.ch(j)]).astype(BF))
        sum_h.put(j)
        if j:
            sum_h.step_cross(j - 1)
    sum_h.step_cross(n_scat - 1)

    rstd1 = ln_block(own, 32, xg, 0, 1, None)
    y_cross.wait_recv()
    for c in range(nlc):
        z = (sy[blk_own, lc(c)].astype(F32) + rsy[:, lc(c)].astype(F32)).astype(BF).astype(F32)
        ybuf[:, lc(c)] = (x1[own, lc(c)] + z + vecs[5, :, lc(c)]).astype(BF)
        vec[4, :, lc(c)] = jnp.sum(gmid[:, lc(c)], axis=0, keepdims=True)

    me = slot(t)
    acc1 = jnp.zeros((32, LANES), F32)
    acc2 = jnp.zeros((32, LANES), F32)
    for j in range(n_scat):
        sum_h.b[j].wait_recv()
        for c in groups(SCATTER_CHUNKS, j):
            dh = sum_h.result(lc(c))
            z = xh1[:, lc(c)]
            dhz = dh * z
            part_o[me, 0:1, lc(c)] = jnp.sum(dhz, axis=0, keepdims=True)
            part_o[me, 1:2, lc(c)] = jnp.sum(dh, axis=0, keepdims=True)
            gain = vecs[0, :, lc(c)]
            acc1 = acc1 + dh * gain
            acc2 = acc2 + dhz * gain
    parts = [remote(part_o.at[me], part_o.at[me], dev) for dev in (cross, sibcross, sib)]
    mean1 = jnp.sum(acc1, axis=1, keepdims=True) / D
    mean2 = jnp.sum(acc2, axis=1, keepdims=True) / D
    for c in range(nlc):
        dz = sum_h.result(lc(c)) * vecs[0, :, lc(c)]
        gxbuf[:, lc(c)] = (gmid[own, lc(c)] + rstd1 * (dz - mean1 - xh1[:, lc(c)] * mean2)).astype(BF)
    for copy in sent:
        copy.wait_send()
    for copy in parts:
        copy.wait_recv()


def grad_kernel(h, ga, dpre, gy, dqkv, ctx, gt, rt, vec, part, y, gx,
                dwqkv_o, dwout_o, dwup_o, dwdn_o, dbqkv_o, y_o, gx_o, v0, v1, v2, v3, v4, v5, v6,
                buf, small, sums, bq, osem, ssem):
    n_heads, head = dbqkv_o.shape[1], dbqkv_o.shape[2]
    slots, block = buf.shape[0], buf.shape[1]
    tail = []

    def piece(k, start, size):
        small[k, pl.ds(0, size), :] = dot(ctx[start:start + size, :], ga[...]).astype(BF)
        copy = pltpu.make_async_copy(small.at[k, pl.ds(0, size), :], dwout_o.at[pl.ds(start, size), :], ssem.at[k])
        copy.start()
        tail.append(copy)

    def written(slot, out):
        return pltpu.make_async_copy(buf.at[slot], out.at[pl.ds(0, block), :], osem.at[slot])

    piece(0, 0, 160)
    for k in range(2):
        sums[k] = (part[0, k:k + 1, :] + part[1, k:k + 1, :]) + (part[2, k:k + 1, :] + part[3, k:k + 1, :])

    def send(src, dst):
        copy = pltpu.make_async_copy(src, dst, ssem.at[len(tail) + 2])
        copy.start()
        tail.append(copy)

    send(y, y_o)
    send(gx, gx_o)
    for k, o in enumerate((v2, v3, v4, v5, v6)):
        send(vec.at[k + 2, 0], o)
    for k, o in enumerate((v0, v1)):
        send(sums.at[k, 0], o)
    first = 0
    for left, right, out in ((rt, gy, dwdn_o), (gt, dpre, dwup_o), (dqkv, h, dwqkv_o)):

        def body(m, carry, left=left, right=right, out=out, first=first):
            slot = lax.rem(first + m, slots)

            @pl.when(first + m >= slots)
            def _():
                written(slot, out).wait()

            at = pl.ds(pl.multiple_of(m * block, block), block)
            buf[slot] = dot(left[at, :], right[...]).astype(BF)
            pltpu.make_async_copy(buf.at[slot], out.at[at, :], osem.at[slot]).start()
            return carry

        count = left.shape[0] // block
        lax.fori_loop(0, count, body, 0)
        first += count
    piece(1, 160, 320)
    ones = jnp.ones((8, dqkv.shape[1]), BF)
    total = dot_t(ones, dqkv[...])[0:1]
    for k in range(3):
        for hd in range(n_heads):
            at = (hd * 3 + k) * head
            bq[k, hd:hd + 1, :] = total[:, at:at + head]
    send(bq, dbqkv_o)
    piece(2, 480, 160)
    for k in range(slots):
        written(k, dwqkv_o).wait()
    for copy in tail:
        copy.wait()


def solution(mesh):
    def local_step(x, ln1_gamma, ln1_beta, w_qkv, b_qkv, w_out, b_out, ln2_gamma, ln2_beta, w_up, b_up, w_down, b_down, grad_y):
        D = x.shape[2]
        S = TP * x.shape[1]
        nh, head = w_qkv.shape[1], w_qkv.shape[3]
        Q = nh * 3 * head
        C = nh * head
        FL = w_up.shape[1]
        any_spec = pl.BlockSpec(memory_space=pl.ANY)
        vspec = pl.BlockSpec(memory_space=pltpu.VMEM)
        vm = pltpu.VMEM
        wqkv_t = jnp.transpose(w_qkv, (1, 2, 3, 0)).reshape(Q, D)
        bq = jnp.transpose(b_qkv, (1, 0, 2))
        sds = jax.ShapeDtypeStruct
        n_loads = 2 + 7 + 1 + 4
        red = [vm((S, D), BF), vm((S // 2, D), BF), vm((S // 2, D), BF), vm((S // 2, D), BF), vm((S, D), BF),
               vm((S // 2, ALL_CHUNKS[-1] * LANES), BF), vm((S // 2, ALL_CHUNKS[-1] * LANES), BF)]
        scat = [vm((S, D), BF), vm((S // 2, D), BF), vm((S // 2, D), BF), vm((S // TP, D), BF)]
        row = lambda v: v
        res = pl.pallas_call(
            layer_kernel,
            name='layer',
            out_shape=[vm((S // TP, D), BF), vm((S // TP, D), BF), vm((7, 1, D), F32), vm((TP, 2, D), F32), vm((S, D), BF), vm((S, D), BF),
                       vm((S, FL), BF), vm((S, D), BF), vm((Q, S), BF), vm((C, S), BF), vm((D, S), BF), vm((FL, S), BF)],
            in_specs=[any_spec] * 14,
            out_specs=[vspec] * 12,
            scratch_shapes=[
                vm((Q, D), BF), vm((C, D), BF), vm((D, FL), BF), vm((FL, D), BF), vm((3, nh, head), F32), vm((7, 1, D), F32),
                vm((S, D), BF), vm((S, D), BF), vm((Q, S), F32), vm((Q, S), BF), vm((nh, S, S), F32),
                vm((nh, S, S), BF), vm((S, D), F32), vm((S, D), F32), vm((S, D), BF),
                vm((S, FL), BF), vm((S, FL), BF), vm((S, D), F32), vm((C, S), BF),
                vm((S // TP, D), F32), vm((S, D), F32), vm((S, D), F32),
                vm((nh, S, head), BF), vm((nh, S, S), BF), vm((nh, S, S), BF),
                *red, *red, *scat, *scat,
                pltpu.SemaphoreType.DMA((n_loads,)),
                pltpu.SemaphoreType.DMA((N_REMOTE,)), pltpu.SemaphoreType.DMA((N_REMOTE,)),
            ],
            compiler_params=pltpu.CompilerParams(collective_id=0, has_side_effects=True, vmem_limit_bytes=LAYER_VMEM),
        )(x.reshape(x.shape[1], D), grad_y.reshape(x.shape[1], D), wqkv_t, bq, w_out, w_up, w_down, row(ln1_gamma), row(ln1_beta),
          row(ln2_gamma), row(ln2_beta), row(b_out), row(b_down), row(b_up))
        y, gx, vec, part, h, ga, dpre, gyf, dqkv, ctx, gt, rt = res
        vshape = sds((D,), F32)
        outs = pl.pallas_call(
            grad_kernel,
            name='weight_grads',
            out_shape=[sds((Q, D), BF), sds((C, D), BF), sds((D, FL), BF), sds((FL, D), BF), sds((3, nh, head), F32),
                       sds((S // TP, D), BF), sds((S // TP, D), BF)] + [vshape] * 7,
            in_specs=[vspec] * 12,
            out_specs=[any_spec] * 14,
            scratch_shapes=[
                vm((3, 640, D), BF), vm((3, 320, D), BF), vm((2, 1, D), F32), vm((3, nh, head), F32),
                pltpu.SemaphoreType.DMA((3,)), pltpu.SemaphoreType.DMA((14,)),
            ],
            compiler_params=pltpu.CompilerParams(vmem_limit_bytes=GRAD_VMEM),
        )(h, ga, dpre, gyf, dqkv, ctx, gt, rt, vec, part, y, gx)
        dwqkv, dwout, dwup, dwdn, dbqkv, y, gx, g_ln1g, g_ln1b, g_ln2g, g_ln2b, g_bout, g_bdown, g_bup = outs
        dwqkv = jnp.transpose(dwqkv.reshape(nh, 3, head, D), (3, 0, 1, 2))
        dbqkv = jnp.transpose(dbqkv, (1, 0, 2))
        return (y.reshape(x.shape), gx.reshape(x.shape), g_ln1g, g_ln1b, dwqkv, dbqkv, dwout, g_bout,
                g_ln2g, g_ln2b, dwup, g_bup, dwdn, g_bdown)

    row_spec = P('dp', 'tp', None)
    in_specs = (row_spec, P(), P(), P(None, 'tp', None, None), P('tp', None, None), P('tp', None), P(), P(), P(),
                P(None, 'tp'), P('tp'), P('tp', None), P(), row_spec)
    out_specs = (row_spec, row_spec, P('dp'), P('dp'), P('dp', 'tp', None, None), P(('dp', 'tp'), None, None),
                 P(('dp', 'tp'), None), P('dp'), P('dp'), P('dp'), P('dp', 'tp'), P(('dp', 'tp')), P(('dp', 'tp'), None), P('dp'))
    return jax.shard_map(local_step, mesh=mesh, in_specs=in_specs, out_specs=out_specs, check_vma=False)
```

```python
import functools
import math
import jax
import jax.numpy as jnp
from jax import lax
from jax.experimental import pallas as pl
from jax.experimental.pallas import tpu as pltpu
from jax.sharding import PartitionSpec as P

EPS = 1e-5
MASK_VALUE = -1e30
BF = jnp.bfloat16
F32 = jnp.float32
MESH = pl.DeviceIdType.MESH
GELU_C = math.sqrt(2.0 / math.pi)
GELU_A = 0.044715
TP = 4
LANES = 128
ALL_CHUNKS = (2, 4, 4, 5, 4, 1)
SCATTER_CHUNKS = (2, 6, 8, 4)
N_BLK = 5
GRAD_ROWS = 640
WORK_CUTS = (0, 3, 5, 6, 7, 7, 7)
LAYER_VMEM = 47 * 1024 * 1024
GRAD_VMEM = 24 * 1024 * 1024
N_REMOTE = 62


def alibi_slopes(n_heads):
    closest = 2 ** int(math.floor(math.log2(n_heads)))
    base_ratio = 2.0 ** (-8.0 / closest)
    extra_ratio = 2.0 ** (-4.0 / closest)
    remaining = min(closest, n_heads - closest)
    slopes = [base_ratio ** (i + 1) for i in range(closest)]
    return slopes + [extra_ratio ** (2 * i + 1) for i in range(remaining)]


def dot(lhs, rhs):
    return lax.dot_general(lhs, rhs, (((1,), (0,)), ((), ())), preferred_element_type=F32)


def dot_t(lhs, rhs):
    return lax.dot_general(lhs, rhs, (((1,), (1,)), ((), ())), preferred_element_type=F32)


def layer_kernel(x_h, gy_h, wqkv_h, bqkv_h, wout_h, wup_h, wdn_h, ln1g_h, ln1b_h, ln2g_h, ln2b_h, bout_h, bdown_h, bup_h,
                 ybuf, gxbuf, vec, part_o, h, ga, dpre, dqkv, ctx, gt, wdn,
                 wqkv, wout, wup, rt, bqkv, vecs, xg, gyg, bias, qkv, prob, probb, x1, xhat, g, gact, r,
                 gmid, dctx, xh1, ubuf, xr, vt, dpb, dsb,
                 p1, rd1, s1, rs1, t1, q1, e1, p2, rd2, s2, rs2, t2, q2, e2, py, rdy, sy, rsy, ph, rdh, sh, rsh,
                 lsem, ssem, rsem):
    D = x_h.shape[1]
    seq = TP * 32
    head = bqkv_h.shape[2]
    n_heads = bqkv_h.shape[1]
    nlc = D // LANES
    t = lax.axis_index('tp')
    core = lax.rem(t, 2)
    chip = t // 2
    sib = t + 1 - 2 * core
    cross = lax.rem(t + 2, TP)
    sibcross = lax.rem(sib + 2, TP)

    def slot(dev):
        return lax.rem(dev, 2) * 2 + dev // 2

    def rows(dev):
        return pl.ds(pl.multiple_of(slot(dev) * 32, 32), 32)

    own = rows(t)
    half = pl.ds(pl.multiple_of(core * 64, 64), 64)
    sibhalf = pl.ds(pl.multiple_of((1 - core) * 64, 64), 64)
    blk_own = pl.ds(pl.multiple_of(chip * 32, 32), 32)
    blk_cross = pl.ds(pl.multiple_of((1 - chip) * 32, 32), 32)

    counter = [0, 0]

    def load(src, dst):
        k = counter[0]
        counter[0] += 1
        copy = pltpu.make_async_copy(src, dst, lsem.at[k])
        copy.start()
        return copy

    sent = []

    def remote(src, dst, dev):
        k = counter[1]
        counter[1] += 1
        copy = pltpu.make_async_remote_copy(src_ref=src, dst_ref=dst, send_sem=ssem.at[k], recv_sem=rsem.at[k],
                                            device_id={'tp': dev}, device_id_type=MESH)
        copy.start()
        sent.append(copy)
        return copy

    def lc(c):
        return slice(c * LANES, (c + 1) * LANES)

    def groups(widths, j):
        start = sum(widths[:j])
        return range(start, start + widths[j])

    def cols(widths, j):
        return slice(sum(widths[:j]) * LANES, sum(widths[:j + 1]) * LANES)

    lx = load(x_h, xg.at[own, :])
    lg = load(gy_h, gyg.at[own, :])
    lvec = [load(src, vecs.at[k, 0]) for k, src in enumerate((ln1g_h, ln1b_h, ln2g_h, ln2b_h, bout_h, bdown_h, bup_h))]
    lb = load(bqkv_h, bqkv)
    lwqkv = load(wqkv_h, wqkv)
    lwout = load(wout_h, wout)
    barrier = pltpu.get_barrier_semaphore()
    for dev in (sib, cross, sibcross):
        pl.semaphore_signal(barrier, inc=1, device_id={'tp': dev}, device_id_type=MESH)
    pl.semaphore_wait(barrier, 3)
    lx.wait()
    def piece(dev, k):
        return pl.ds(pl.multiple_of(slot(dev) * 32 + 16 * k, 16), 16)

    x_to_cross = [remote(xg.at[piece(t, k), :], xg.at[piece(t, k), :], cross) for k in range(2)]
    x_to_sib = remote(xg.at[own, :], xg.at[own, :], sib)
    lg.wait()
    gy_to_sib = remote(gyg.at[own, :], gyg.at[own, :], sib)
    lwdn = load(wdn_h, wdn)
    lwup = load(wup_h, wup)
    for copy in lvec:
        copy.wait()

    def ln_block(rr, n, src, gain, shift, dst):
        acc = jnp.zeros((n, LANES), F32)
        for c in range(nlc):
            acc = acc + src[rr, lc(c)].astype(F32)
        mean = jnp.sum(acc, axis=1, keepdims=True) / D
        acc = jnp.zeros((n, LANES), F32)
        for c in range(nlc):
            z = src[rr, lc(c)].astype(F32) - mean
            acc = acc + z * z
        rstd = lax.rsqrt(jnp.sum(acc, axis=1, keepdims=True) / D + EPS)
        for c in range(nlc):
            z = (src[rr, lc(c)].astype(F32) - mean) * rstd
            if dst is not None:
                dst[rr, lc(c)] = (z * vecs[gain, :, lc(c)] + vecs[shift, :, lc(c)]).astype(BF)
            else:
                xh1[:, lc(c)] = z
        return rstd

    ln_block(own, 32, xg, 0, 1, h)
    lb.wait()
    for k in range(3):
        bt = bqkv[k].T
        for hd in range(n_heads):
            at = (hd * 3 + k) * head
            bias[at:at + head, :] = jnp.broadcast_to(bt[:head, hd:hd + 1], (head, seq))
    x_to_sib.wait_recv()
    ln_block(rows(sib), 32, xg, 0, 1, h)
    x_fwd = []
    for k in range(2):
        x_to_cross[k].wait_recv()
        x_fwd.append(remote(xg.at[piece(cross, k), :], xg.at[piece(cross, k), :], sib))
    gy_to_cross = remote(gyg.at[own, :], gyg.at[own, :], cross)
    lwqkv.wait()
    lwout.wait()
    ln_block(rows(cross), 32, xg, 0, 1, h)
    for k in range(2):
        x_fwd[k].wait_recv()
    ln_block(rows(sibcross), 32, xg, 0, 1, h)

    hr = 2 * 3 * head
    hv = h[...]
    for m in range(n_heads // 2):
        mm = slice(m * hr, (m + 1) * hr)
        qkv[mm, :] = (dot_t(wqkv[mm, :], hv) + bias[mm, :]).astype(BF)

    def position(axis):
        i = lax.broadcasted_iota(jnp.int32, (seq, seq), axis)
        b = i >> 5
        return ((((b & 1) << 1) | (b >> 1)) << 5) | (i & 31)

    pos_k = position(0)
    causal = pos_k <= position(1)
    key_f = pos_k.astype(F32)
    slopes = alibi_slopes(n_heads * TP)
    score_scale = head ** -0.5

    def part_of(hd, k):
        at = (hd * 3 + k) * head
        return slice(at, at + head)

    def slope(hd):
        v = jnp.float32(slopes[hd])
        for dev in range(1, TP):
            v = jnp.where(t == dev, jnp.float32(slopes[dev * n_heads + hd]), v)
        return v

    for hd in range(n_heads):
        prob[hd] = dot(qkv[part_of(hd, 1), :].T, qkv[part_of(hd, 0), :])
    for hd in range(n_heads):
        s = jnp.where(causal, prob[hd] * score_scale + slope(hd) * key_f, MASK_VALUE)
        e = jnp.exp(s - jnp.max(s, axis=0, keepdims=True))
        pr = e * (1.0 / jnp.sum(e, axis=0, keepdims=True))
        prob[hd] = pr
        probb[hd] = pr.astype(BF)
    for hd in range(n_heads):
        ctx[hd * head:(hd + 1) * head, :] = dot(qkv[part_of(hd, 2), :], probb[hd]).astype(BF)

    class AllSum:
        widths = ALL_CHUNKS

        def __init__(self, p, rd, s, rs, tt, q, e):
            self.p, self.rd, self.s, self.rs, self.tt, self.q, self.e = p, rd, s, rs, tt, q, e
            self.a, self.b, self.c = {}, {}, {}
            self.last = len(self.widths) - 1

        def ch(self, j):
            return cols(self.widths, j)

        def fill(self, j, value):
            self.p[:, self.ch(j)] = value

        def put(self, j):
            self.a[j] = remote(self.p.at[sibhalf, self.ch(j)], self.rd.at[:, self.ch(j)], sib)

        def pair(self, j):
            self.a[j].wait_recv()
            c = self.ch(j)
            self.s[:, c] = (self.p[half, c].astype(F32) + self.rd[:, c].astype(F32)).astype(BF)

        def step_cross(self, j):
            self.pair(j)
            c = self.ch(j)
            self.b[j] = remote(self.s.at[:, c], self.rs.at[:, c], cross)
            if j == self.last:
                self.c[j] = (remote(self.s.at[:, c], self.e.at[:, :], sibcross), remote(self.s.at[:, c], self.q.at[:, :], sib))

        def step_back(self, j):
            self.b[j].wait_recv()
            c = self.ch(j)
            self.tt[half, c] = (self.s[:, c].astype(F32) + self.rs[:, c].astype(F32)).astype(BF)
            if j < self.last:
                self.c[j] = remote(self.tt.at[half, c], self.tt.at[half, c], sib)

        def finish(self, j):
            if j < self.last:
                self.c[j].wait_recv()
            else:
                for copy in self.c[j]:
                    copy.wait_recv()
                self.tt[sibhalf, self.ch(j)] = (self.q[...].astype(F32) + self.e[...].astype(F32)).astype(BF)

    class ScatterSum(AllSum):
        widths = SCATTER_CHUNKS

        def step_cross(self, j):
            self.pair(j)
            c = self.ch(j)
            self.b[j] = remote(self.s.at[blk_cross, c], self.rs.at[:, c], cross)

        def result(self, c):
            return (self.s[blk_own, c].astype(F32) + self.rs[:, c].astype(F32)).astype(BF).astype(F32)

    o_flat = ctx[...].T
    sum_a = AllSum(p1, rd1, s1, rs1, t1, q1, e1)
    n_all = len(ALL_CHUNKS)
    sum_a.fill(0, dot(o_flat, wout[:, sum_a.ch(0)]).astype(BF))
    sum_a.put(0)
    for j in range(1, n_all):
        sum_a.fill(j, dot(o_flat, wout[:, sum_a.ch(j)]).astype(BF))
    for j in range(1, n_all):
        sum_a.put(j)
    for j in range(n_all):
        sum_a.step_cross(j)

    gy_to_sib.wait_recv()
    gy_to_cross.wait_recv()
    gy_fwd = remote(gyg.at[rows(cross), :], gyg.at[rows(cross), :], sib)
    for hd in range(n_heads):
        vt[hd] = qkv[part_of(hd, 2), :].T
    gy_fwd.wait_recv()
    lwdn.wait()
    lwup.wait()
    fw = wdn_h.shape[0] // N_BLK
    acc = jnp.zeros((seq, LANES), F32)

    def x1_chunk(j, acc):
        sum_a.finish(j)
        for c in groups(ALL_CHUNKS, j):
            z = xg[:, lc(c)].astype(F32) + t1[:, lc(c)].astype(F32) + vecs[4, :, lc(c)]
            x1[:, lc(c)] = z
            acc = acc + z
        return acc

    gyv = gyg[...]
    for j in range(n_all):
        if j < N_BLK:
            ff = slice(j * fw, (j + 1) * fw)
            gact[:, ff] = dot_t(gyv, wdn[ff, :]).astype(BF)
        sum_a.step_back(j)
        if j:
            acc = x1_chunk(j - 1, acc)
    acc = x1_chunk(n_all - 1, acc)

    mean = jnp.sum(acc, axis=1, keepdims=True) / D
    halves = (slice(0, seq // 2), slice(seq // 2, seq))
    rstd2 = []
    for n, hh in enumerate(halves):
        acc = jnp.zeros((seq // 2, LANES), F32)
        for c in range(nlc):
            z = x1[hh, lc(c)] - mean[hh]
            acc = acc + z * z
        rstd2.append(lax.rsqrt(jnp.sum(acc, axis=1, keepdims=True) / D + EPS))
    for n, hh in enumerate(halves):
        for c in range(nlc):
            z = (x1[hh, lc(c)] - mean[hh]) * rstd2[n]
            xhat[hh, lc(c)] = z
            g[hh, lc(c)] = (z * vecs[2, :, lc(c)] + vecs[3, :, lc(c)]).astype(BF)

    gv = g[...]
    for j in range(N_BLK):
        ff = slice(j * fw, (j + 1) * fw)
        pre = dot(gv, wup[:, ff]) + vecs[6, :, ff]
        w = (GELU_C * GELU_A) * (pre * pre)
        th = jnp.tanh(pre * (GELU_C + w))
        hp = 0.5 * pre
        r[:, ff] = (hp + hp * th).astype(BF)
        slope_g = (0.5 + 0.5 * th) + (hp * (1.0 - th * th)) * (GELU_C + 3.0 * w)
        gp = gact[:, ff].astype(F32) * slope_g
        vec[6, :, ff] = jnp.sum(gp, axis=0, keepdims=True)
        dpre[:, ff] = gp.astype(BF)

    dv = dpre[...]
    sum_g = AllSum(p2, rd2, s2, rs2, t2, q2, e2)
    for j in range(n_all):
        for c in [lc(c) for c in groups(ALL_CHUNKS, j)] if j == 0 else [sum_g.ch(j)]:
            p2[:, c] = dot_t(dv, wup[c, :]).astype(BF)
        sum_g.put(j)
        if j:
            sum_g.step_cross(j - 1)
    sum_g.step_cross(n_all - 1)

    acc1 = jnp.zeros((seq, LANES), F32)
    acc2 = jnp.zeros((seq, LANES), F32)

    def ln2_back_chunk(j, acc1, acc2):
        sum_g.finish(j)
        for c in groups(ALL_CHUNKS, j):
            dg = t2[:, lc(c)].astype(F32)
            z = xhat[:, lc(c)]
            dgz = dg * z
            vec[2, :, lc(c)] = jnp.sum(dgz, axis=0, keepdims=True)
            vec[3, :, lc(c)] = jnp.sum(dg, axis=0, keepdims=True)
            gain = vecs[2, :, lc(c)]
            dz = dg * gain
            acc1 = acc1 + dz
            acc2 = acc2 + dgz * gain
            for n, hh in enumerate(halves):
                ubuf[hh, lc(c)] = gyg[hh, lc(c)].astype(F32) + rstd2[n] * dz[hh]
        return acc1, acc2

    yw = D // N_BLK

    def down(j):
        yy = slice(j * yw, (j + 1) * yw)
        py[:, yy] = dot(r[...], wdn[:, yy]).astype(BF)
        for c in range(j * (yw // LANES), (j + 1) * (yw // LANES)):
            gt[lc(c), :] = g[:, lc(c)].T
            rt[lc(c), :] = r[:, lc(c)].T
            vec[5, :, lc(c)] = jnp.sum(gyg[:, lc(c)].astype(F32), axis=0, keepdims=True)
            for n, hh in enumerate(halves):
                xr[hh, lc(c)] = xhat[hh, lc(c)] * rstd2[n]

    def grad_down(m):
        mm = slice(m * GRAD_ROWS, (m + 1) * GRAD_ROWS)
        wdn[mm, :] = dot(rt[mm, :], gyg[...]).astype(BF)

    work = [(down, k) for k in range(N_BLK)] + [(grad_down, m) for m in range(wdn.shape[0] // GRAD_ROWS)]
    for j in range(n_all):
        for step, m in work[WORK_CUTS[j]:WORK_CUTS[j + 1]]:
            step(m)
        if j == 1:
            y_sib = remote(py.at[sibhalf, :], rdy, sib)
        sum_g.step_back(j)
        if j:
            acc1, acc2 = ln2_back_chunk(j - 1, acc1, acc2)
    y_sib.wait_recv()
    sy[...] = (py[half, :].astype(F32) + rdy[...].astype(F32)).astype(BF)
    y_cross = remote(sy.at[blk_cross, :], rsy, cross)
    acc1, acc2 = ln2_back_chunk(n_all - 1, acc1, acc2)

    for n, hh in enumerate(halves):
        mean1 = rstd2[n] * (jnp.sum(acc1[hh], axis=1, keepdims=True) / D)
        mean2 = jnp.sum(acc2[hh], axis=1, keepdims=True) / D
        for c in range(nlc):
            gm = ubuf[hh, lc(c)] - (mean1 + xr[hh, lc(c)] * mean2)
            gmid[hh, lc(c)] = gm
            ga[hh, lc(c)] = gm.astype(BF)

    gav = ga[...]
    hc = ctx.shape[0] // 2
    for k in range(2):
        dctx[k * hc:(k + 1) * hc, :] = dot_t(wout[k * hc:(k + 1) * hc, :], gav).astype(BF)

    def head_rows(hd):
        return slice(hd * head, (hd + 1) * head)

    for hd in range(n_heads):
        dpb[hd] = dot(vt[hd], dctx[head_rows(hd), :]).astype(BF)
    for hd in range(n_heads):
        dqkv[part_of(hd, 2), :] = dot_t(dctx[head_rows(hd), :], probb[hd]).astype(BF)
    for hd in range(n_heads):
        pr = prob[hd]
        dp = dpb[hd].astype(F32)
        dsb[hd] = (pr * (dp - jnp.sum(dp * pr, axis=0, keepdims=True))).astype(BF)
    for hd in range(n_heads):
        dqkv[part_of(hd, 0), :] = (dot(qkv[part_of(hd, 1), :], dsb[hd]) * score_scale).astype(BF)
        dqkv[part_of(hd, 1), :] = (dot_t(qkv[part_of(hd, 0), :], dsb[hd]) * score_scale).astype(BF)

    sum_h = ScatterSum(ph, rdh, sh, rsh, None, None, None)
    n_scat = len(SCATTER_CHUNKS)
    dq = dqkv[...].T
    for j in range(n_scat):
        for c in [lc(c) for c in groups(SCATTER_CHUNKS, j)] if j == 0 else [sum_h.ch(j)]:
            ph[:, c] = dot(dq, wqkv[:, c]).astype(BF)
        sum_h.put(j)
        if j:
            sum_h.step_cross(j - 1)
    sum_h.step_cross(n_scat - 1)

    rstd1 = ln_block(own, 32, xg, 0, 1, None)
    y_cross.wait_recv()
    for c in range(nlc):
        z = (sy[blk_own, lc(c)].astype(F32) + rsy[:, lc(c)].astype(F32)).astype(BF).astype(F32)
        ybuf[:, lc(c)] = (x1[own, lc(c)] + z + vecs[5, :, lc(c)]).astype(BF)
        vec[4, :, lc(c)] = jnp.sum(gmid[:, lc(c)], axis=0, keepdims=True)

    me = slot(t)
    acc1 = jnp.zeros((32, LANES), F32)
    acc2 = jnp.zeros((32, LANES), F32)
    parts = []
    for step, m in work[WORK_CUTS[-1]:]:
        step(m)
    for j in range(n_scat):
        sum_h.b[j].wait_recv()
        for c in groups(SCATTER_CHUNKS, j):
            dh = sum_h.result(lc(c))
            z = xh1[:, lc(c)]
            dhz = dh * z
            part_o[me, 0:1, lc(c)] = jnp.sum(dhz, axis=0, keepdims=True)
            part_o[me, 1:2, lc(c)] = jnp.sum(dh, axis=0, keepdims=True)
            gain = vecs[0, :, lc(c)]
            acc1 = acc1 + dh * gain
            acc2 = acc2 + dhz * gain
        if j >= n_scat - 2:
            c = slice(0, sum_h.ch(j).stop) if j == n_scat - 2 else sum_h.ch(j)
            parts += [remote(part_o.at[me, :, c], part_o.at[me, :, c], dev) for dev in (cross, sibcross, sib)]
    mean1 = jnp.sum(acc1, axis=1, keepdims=True) / D
    mean2 = jnp.sum(acc2, axis=1, keepdims=True) / D
    for c in range(nlc):
        dz = sum_h.result(lc(c)) * vecs[0, :, lc(c)]
        gxbuf[:, lc(c)] = (gmid[own, lc(c)] + rstd1 * (dz - mean1 - xh1[:, lc(c)] * mean2)).astype(BF)
    for copy in sent:
        copy.wait_send()
    for copy in parts:
        copy.wait_recv()


def grad_kernel(h, ga, dpre, dqkv, ctx, gt, dwdn, vec, part, y, gx,
                dwqkv_o, dwout_o, dwup_o, dwdn_o, dbqkv_o, y_o, gx_o, v0, v1, v2, v3, v4, v5, v6,
                buf, small, sums, bq, osem, ssem):
    n_heads, head = dbqkv_o.shape[1], dbqkv_o.shape[2]
    slots, block = buf.shape[0], buf.shape[1]
    tail = []

    def piece(k, start, size):
        small[k, pl.ds(0, size), :] = dot(ctx[start:start + size, :], ga[...]).astype(BF)
        copy = pltpu.make_async_copy(small.at[k, pl.ds(0, size), :], dwout_o.at[pl.ds(start, size), :], ssem.at[k])
        copy.start()
        tail.append(copy)

    def written(slot, out):
        return pltpu.make_async_copy(buf.at[slot], out.at[pl.ds(0, block), :], osem.at[slot])

    for k in range(4):
        n = dwdn.shape[0] // 4
        copy = pltpu.make_async_copy(dwdn.at[pl.ds(k * n, n), :], dwdn_o.at[pl.ds(k * n, n), :], ssem.at[14 + k])
        copy.start()
        tail.append(copy)
    piece(0, 0, 160)
    for k in range(2):
        sums[k] = (part[0, k:k + 1, :] + part[1, k:k + 1, :]) + (part[2, k:k + 1, :] + part[3, k:k + 1, :])

    def send(src, dst):
        copy = pltpu.make_async_copy(src, dst, ssem.at[len(tail) - 2])
        copy.start()
        tail.append(copy)

    send(y, y_o)
    send(gx, gx_o)
    for k, o in enumerate((v2, v3, v4, v5, v6)):
        send(vec.at[k + 2, 0], o)
    for k, o in enumerate((v0, v1)):
        send(sums.at[k, 0], o)
    first = 0
    for left, right, out in ((gt, dpre, dwup_o), (dqkv, h, dwqkv_o)):

        def body(m, carry, left=left, right=right, out=out, first=first):
            slot = lax.rem(first + m, slots)

            @pl.when(first + m >= slots)
            def _():
                written(slot, out).wait()

            at = pl.ds(pl.multiple_of(m * block, block), block)
            buf[slot] = dot(left[at, :], right[...]).astype(BF)
            pltpu.make_async_copy(buf.at[slot], out.at[at, :], osem.at[slot]).start()
            return carry

        count = left.shape[0] // block
        lax.fori_loop(0, count, body, 0)
        first += count
    piece(1, 160, 320)
    ones = jnp.ones((8, dqkv.shape[1]), BF)
    total = dot_t(ones, dqkv[...])[0:1]
    for k in range(3):
        for hd in range(n_heads):
            at = (hd * 3 + k) * head
            bq[k, hd:hd + 1, :] = total[:, at:at + head]
    send(bq, dbqkv_o)
    piece(2, 480, 160)
    for k in range(slots):
        written(k, dwqkv_o).wait()
    for copy in tail:
        copy.wait()


def solution(mesh):
    def local_step(x, ln1_gamma, ln1_beta, w_qkv, b_qkv, w_out, b_out, ln2_gamma, ln2_beta, w_up, b_up, w_down, b_down, grad_y):
        D = x.shape[2]
        S = TP * x.shape[1]
        nh, head = w_qkv.shape[1], w_qkv.shape[3]
        Q = nh * 3 * head
        C = nh * head
        FL = w_up.shape[1]
        any_spec = pl.BlockSpec(memory_space=pl.ANY)
        vspec = pl.BlockSpec(memory_space=pltpu.VMEM)
        vm = pltpu.VMEM
        wqkv_t = jnp.transpose(w_qkv, (1, 2, 3, 0)).reshape(Q, D)
        bq = jnp.transpose(b_qkv, (1, 0, 2))
        sds = jax.ShapeDtypeStruct
        n_loads = 2 + 7 + 1 + 4
        red = [vm((S, D), BF), vm((S // 2, D), BF), vm((S // 2, D), BF), vm((S // 2, D), BF), vm((S, D), BF),
               vm((S // 2, ALL_CHUNKS[-1] * LANES), BF), vm((S // 2, ALL_CHUNKS[-1] * LANES), BF)]
        scat = [vm((S, D), BF), vm((S // 2, D), BF), vm((S // 2, D), BF), vm((S // TP, D), BF)]
        row = lambda v: v
        res = pl.pallas_call(
            layer_kernel,
            name='layer',
            out_shape=[vm((S // TP, D), BF), vm((S // TP, D), BF), vm((7, 1, D), F32), vm((TP, 2, D), F32), vm((S, D), BF), vm((S, D), BF),
                       vm((S, FL), BF), vm((Q, S), BF), vm((C, S), BF), vm((D, S), BF), vm((FL, D), BF)],
            in_specs=[any_spec] * 14,
            out_specs=[vspec] * 11,
            scratch_shapes=[
                vm((Q, D), BF), vm((C, D), BF), vm((D, FL), BF), vm((FL, S), BF), vm((3, nh, head), F32), vm((7, 1, D), F32),
                vm((S, D), BF), vm((S, D), BF), vm((Q, S), F32), vm((Q, S), BF), vm((nh, S, S), F32),
                vm((nh, S, S), BF), vm((S, D), F32), vm((S, D), F32), vm((S, D), BF),
                vm((S, FL), BF), vm((S, FL), BF), vm((S, D), F32), vm((C, S), BF),
                vm((S // TP, D), F32), vm((S, D), F32), vm((S, D), F32),
                vm((nh, S, head), BF), vm((nh, S, S), BF), vm((nh, S, S), BF),
                *red, *red, *scat, *scat,
                pltpu.SemaphoreType.DMA((n_loads,)),
                pltpu.SemaphoreType.DMA((N_REMOTE,)), pltpu.SemaphoreType.DMA((N_REMOTE,)),
            ],
            compiler_params=pltpu.CompilerParams(collective_id=0, has_side_effects=True, vmem_limit_bytes=LAYER_VMEM),
        )(x.reshape(x.shape[1], D), grad_y.reshape(x.shape[1], D), wqkv_t, bq, w_out, w_up, w_down, row(ln1_gamma), row(ln1_beta),
          row(ln2_gamma), row(ln2_beta), row(b_out), row(b_down), row(b_up))
        y, gx, vec, part, h, ga, dpre, dqkv, ctx, gt, dwdn = res
        vshape = sds((D,), F32)
        outs = pl.pallas_call(
            grad_kernel,
            name='weight_grads',
            out_shape=[sds((Q, D), BF), sds((C, D), BF), sds((D, FL), BF), sds((FL, D), BF), sds((3, nh, head), F32),
                       sds((S // TP, D), BF), sds((S // TP, D), BF)] + [vshape] * 7,
            in_specs=[vspec] * 11,
            out_specs=[any_spec] * 14,
            scratch_shapes=[
                vm((3, 640, D), BF), vm((3, 320, D), BF), vm((2, 1, D), F32), vm((3, nh, head), F32),
                pltpu.SemaphoreType.DMA((3,)), pltpu.SemaphoreType.DMA((18,)),
            ],
            compiler_params=pltpu.CompilerParams(vmem_limit_bytes=GRAD_VMEM),
        )(h, ga, dpre, dqkv, ctx, gt, dwdn, vec, part, y, gx)
        dwqkv, dwout, dwup, dwdn, dbqkv, y, gx, g_ln1g, g_ln1b, g_ln2g, g_ln2b, g_bout, g_bdown, g_bup = outs
        dwqkv = jnp.transpose(dwqkv.reshape(nh, 3, head, D), (3, 0, 1, 2))
        dbqkv = jnp.transpose(dbqkv, (1, 0, 2))
        return (y.reshape(x.shape), gx.reshape(x.shape), g_ln1g, g_ln1b, dwqkv, dbqkv, dwout, g_bout,
                g_ln2g, g_ln2b, dwup, g_bup, dwdn, g_bdown)

    row_spec = P('dp', 'tp', None)
    in_specs = (row_spec, P(), P(), P(None, 'tp', None, None), P('tp', None, None), P('tp', None), P(), P(), P(),
                P(None, 'tp'), P('tp'), P('tp', None), P(), row_spec)
    out_specs = (row_spec, row_spec, P('dp'), P('dp'), P('dp', 'tp', None, None), P(('dp', 'tp'), None, None),
                 P(('dp', 'tp'), None), P('dp'), P('dp'), P('dp'), P('dp', 'tp'), P(('dp', 'tp')), P(('dp', 'tp'), None), P('dp'))
    return jax.shard_map(local_step, mesh=mesh, in_specs=in_specs, out_specs=out_specs, check_vma=False)
```

```python
import functools
import math
import jax
import jax.numpy as jnp
from jax import lax
from jax.experimental import pallas as pl
from jax.experimental.pallas import tpu as pltpu
from jax.sharding import PartitionSpec as P

EPS = 1e-5
MASK_VALUE = -1e30
BF = jnp.bfloat16
F32 = jnp.float32
MESH = pl.DeviceIdType.MESH
GELU_C = math.sqrt(2.0 / math.pi)
GELU_A = 0.044715
TP = 4
LANES = 128
ALL_CHUNKS = (2, 4, 4, 5, 4, 1)
SCATTER_CHUNKS = (2, 6, 8, 4)
N_BLK = 5
GRAD_ROWS = 640
WORK_CUTS = (0, 3, 5, 6, 7, 7, 7)
LAYER_VMEM = 47 * 1024 * 1024
GRAD_VMEM = 24 * 1024 * 1024
N_REMOTE = 62


def alibi_slopes(n_heads):
    closest = 2 ** int(math.floor(math.log2(n_heads)))
    base_ratio = 2.0 ** (-8.0 / closest)
    extra_ratio = 2.0 ** (-4.0 / closest)
    remaining = min(closest, n_heads - closest)
    slopes = [base_ratio ** (i + 1) for i in range(closest)]
    return slopes + [extra_ratio ** (2 * i + 1) for i in range(remaining)]


def dot(lhs, rhs):
    return lax.dot_general(lhs, rhs, (((1,), (0,)), ((), ())), preferred_element_type=F32)


def dot_t(lhs, rhs):
    return lax.dot_general(lhs, rhs, (((1,), (1,)), ((), ())), preferred_element_type=F32)


def layer_kernel(x_h, gy_h, wqkv_h, bqkv_h, wout_h, wup_h, wdn_h, ln1g_h, ln1b_h, ln2g_h, ln2b_h, bout_h, bdown_h, bup_h,
                 ybuf, gxbuf, vec, part_o, h, ga, dpre, dqkv, ctx, gt, wdn,
                 wqkv, wout, wup, rt, bqkv, vecs, xg, gyg, bias, qkv, prob, probb, x1, xhat, g, gact, r,
                 gmid, dctx, xh1, ubuf, xr, vt, dpb, dsb,
                 p1, rd1, s1, rs1, t1, q1, e1, p2, rd2, s2, rs2, t2, q2, e2, py, rdy, sy, rsy, ph, rdh, sh, rsh,
                 lsem, ssem, rsem):
    D = x_h.shape[1]
    seq = TP * 32
    head = bqkv_h.shape[2]
    n_heads = bqkv_h.shape[1]
    nlc = D // LANES
    t = lax.axis_index('tp')
    core = lax.rem(t, 2)
    chip = t // 2
    sib = t + 1 - 2 * core
    cross = lax.rem(sib + 2, TP)
    sibcross = lax.rem(t + 2, TP)
    side = lax.rem(core + chip, 2)

    def slot(dev):
        return lax.rem(lax.rem(dev, 2) + dev // 2, 2) * 2 + dev // 2

    def rows(dev):
        return pl.ds(pl.multiple_of(slot(dev) * 32, 32), 32)

    own = rows(t)
    half = pl.ds(pl.multiple_of(side * 64, 64), 64)
    sibhalf = pl.ds(pl.multiple_of((1 - side) * 64, 64), 64)
    blk_own = pl.ds(pl.multiple_of(chip * 32, 32), 32)
    blk_cross = pl.ds(pl.multiple_of((1 - chip) * 32, 32), 32)

    counter = [0, 0]

    def load(src, dst):
        k = counter[0]
        counter[0] += 1
        copy = pltpu.make_async_copy(src, dst, lsem.at[k])
        copy.start()
        return copy

    sent = []

    def remote(src, dst, dev):
        k = counter[1]
        counter[1] += 1
        copy = pltpu.make_async_remote_copy(src_ref=src, dst_ref=dst, send_sem=ssem.at[k], recv_sem=rsem.at[k],
                                            device_id={'tp': dev}, device_id_type=MESH)
        copy.start()
        sent.append(copy)
        return copy

    def lc(c):
        return slice(c * LANES, (c + 1) * LANES)

    def groups(widths, j):
        start = sum(widths[:j])
        return range(start, start + widths[j])

    def cols(widths, j):
        return slice(sum(widths[:j]) * LANES, sum(widths[:j + 1]) * LANES)

    lx = load(x_h, xg.at[own, :])
    lg = load(gy_h, gyg.at[own, :])
    lvec = [load(src, vecs.at[k, 0]) for k, src in enumerate((ln1g_h, ln1b_h, ln2g_h, ln2b_h, bout_h, bdown_h, bup_h))]
    lb = load(bqkv_h, bqkv)
    lwqkv = load(wqkv_h, wqkv)
    lwout = load(wout_h, wout)
    barrier = pltpu.get_barrier_semaphore()
    for dev in (sib, cross, sibcross):
        pl.semaphore_signal(barrier, inc=1, device_id={'tp': dev}, device_id_type=MESH)
    pl.semaphore_wait(barrier, 3)
    lx.wait()
    def piece(dev, k):
        return pl.ds(pl.multiple_of(slot(dev) * 32 + 16 * k, 16), 16)

    x_to_cross = [remote(xg.at[piece(t, k), :], xg.at[piece(t, k), :], cross) for k in range(2)]
    x_to_sib = remote(xg.at[own, :], xg.at[own, :], sib)
    lg.wait()
    gy_to_sib = remote(gyg.at[own, :], gyg.at[own, :], sib)
    lwdn = load(wdn_h, wdn)
    lwup = load(wup_h, wup)
    for copy in lvec:
        copy.wait()

    def ln_block(rr, n, src, gain, shift, dst):
        acc = jnp.zeros((n, LANES), F32)
        for c in range(nlc):
            acc = acc + src[rr, lc(c)].astype(F32)
        mean = jnp.sum(acc, axis=1, keepdims=True) / D
        acc = jnp.zeros((n, LANES), F32)
        for c in range(nlc):
            z = src[rr, lc(c)].astype(F32) - mean
            acc = acc + z * z
        rstd = lax.rsqrt(jnp.sum(acc, axis=1, keepdims=True) / D + EPS)
        for c in range(nlc):
            z = (src[rr, lc(c)].astype(F32) - mean) * rstd
            if dst is not None:
                dst[rr, lc(c)] = (z * vecs[gain, :, lc(c)] + vecs[shift, :, lc(c)]).astype(BF)
            else:
                xh1[:, lc(c)] = z
        return rstd

    ln_block(own, 32, xg, 0, 1, h)
    lb.wait()
    for k in range(3):
        bt = bqkv[k].T
        for hd in range(n_heads):
            at = (hd * 3 + k) * head
            bias[at:at + head, :] = jnp.broadcast_to(bt[:head, hd:hd + 1], (head, seq))
    x_to_sib.wait_recv()
    ln_block(rows(sib), 32, xg, 0, 1, h)
    x_fwd = []
    for k in range(2):
        x_to_cross[k].wait_recv()
        x_fwd.append(remote(xg.at[piece(cross, k), :], xg.at[piece(cross, k), :], sib))
    gy_to_cross = remote(gyg.at[own, :], gyg.at[own, :], cross)
    lwqkv.wait()
    lwout.wait()
    ln_block(rows(cross), 32, xg, 0, 1, h)
    for k in range(2):
        x_fwd[k].wait_recv()
    ln_block(rows(sibcross), 32, xg, 0, 1, h)

    hr = 2 * 3 * head
    hv = h[...]
    for m in range(n_heads // 2):
        mm = slice(m * hr, (m + 1) * hr)
        qkv[mm, :] = (dot_t(wqkv[mm, :], hv) + bias[mm, :]).astype(BF)

    def position(axis):
        i = lax.broadcasted_iota(jnp.int32, (seq, seq), axis)
        b = i >> 5
        return ((((b & 1) << 1) | (((b >> 1) ^ b) & 1)) << 5) | (i & 31)

    pos_k = position(0)
    causal = pos_k <= position(1)
    key_f = pos_k.astype(F32)
    slopes = alibi_slopes(n_heads * TP)
    score_scale = head ** -0.5

    def part_of(hd, k):
        at = (hd * 3 + k) * head
        return slice(at, at + head)

    def slope(hd):
        v = jnp.float32(slopes[hd])
        for dev in range(1, TP):
            v = jnp.where(t == dev, jnp.float32(slopes[dev * n_heads + hd]), v)
        return v

    for hd in range(n_heads):
        prob[hd] = dot(qkv[part_of(hd, 1), :].T, qkv[part_of(hd, 0), :])
    for hd in range(n_heads):
        s = jnp.where(causal, prob[hd] * score_scale + slope(hd) * key_f, MASK_VALUE)
        e = jnp.exp(s - jnp.max(s, axis=0, keepdims=True))
        pr = e * (1.0 / jnp.sum(e, axis=0, keepdims=True))
        prob[hd] = pr
        probb[hd] = pr.astype(BF)
    for hd in range(n_heads):
        ctx[hd * head:(hd + 1) * head, :] = dot(qkv[part_of(hd, 2), :], probb[hd]).astype(BF)

    class AllSum:
        widths = ALL_CHUNKS

        def __init__(self, p, rd, s, rs, tt, q, e):
            self.p, self.rd, self.s, self.rs, self.tt, self.q, self.e = p, rd, s, rs, tt, q, e
            self.a, self.b, self.c = {}, {}, {}
            self.last = len(self.widths) - 1

        def ch(self, j):
            return cols(self.widths, j)

        def fill(self, j, value):
            self.p[:, self.ch(j)] = value

        def put(self, j):
            self.a[j] = remote(self.p.at[sibhalf, self.ch(j)], self.rd.at[:, self.ch(j)], sib)

        def pair(self, j):
            self.a[j].wait_recv()
            c = self.ch(j)
            self.s[:, c] = (self.p[half, c].astype(F32) + self.rd[:, c].astype(F32)).astype(BF)

        def step_cross(self, j):
            self.pair(j)
            c = self.ch(j)
            self.b[j] = remote(self.s.at[:, c], self.rs.at[:, c], cross)
            if j == self.last:
                self.c[j] = (remote(self.s.at[:, c], self.e.at[:, :], sibcross), remote(self.s.at[:, c], self.q.at[:, :], sib))

        def step_back(self, j):
            self.b[j].wait_recv()
            c = self.ch(j)
            self.tt[half, c] = (self.s[:, c].astype(F32) + self.rs[:, c].astype(F32)).astype(BF)
            if j < self.last:
                self.c[j] = remote(self.tt.at[half, c], self.tt.at[half, c], sib)

        def finish(self, j):
            if j < self.last:
                self.c[j].wait_recv()
            else:
                for copy in self.c[j]:
                    copy.wait_recv()
                self.tt[sibhalf, self.ch(j)] = (self.q[...].astype(F32) + self.e[...].astype(F32)).astype(BF)

    class ScatterSum(AllSum):
        widths = SCATTER_CHUNKS

        def step_cross(self, j):
            self.pair(j)
            c = self.ch(j)
            self.b[j] = remote(self.s.at[blk_cross, c], self.rs.at[:, c], cross)

        def result(self, c):
            return (self.s[blk_own, c].astype(F32) + self.rs[:, c].astype(F32)).astype(BF).astype(F32)

    o_flat = ctx[...].T
    sum_a = AllSum(p1, rd1, s1, rs1, t1, q1, e1)
    n_all = len(ALL_CHUNKS)
    sum_a.fill(0, dot(o_flat, wout[:, sum_a.ch(0)]).astype(BF))
    sum_a.put(0)
    for j in range(1, n_all):
        sum_a.fill(j, dot(o_flat, wout[:, sum_a.ch(j)]).astype(BF))
    for j in range(1, n_all):
        sum_a.put(j)
    for j in range(n_all):
        sum_a.step_cross(j)

    gy_to_sib.wait_recv()
    gy_to_cross.wait_recv()
    gy_fwd = remote(gyg.at[rows(cross), :], gyg.at[rows(cross), :], sib)
    for hd in range(n_heads):
        vt[hd] = qkv[part_of(hd, 2), :].T
    gy_fwd.wait_recv()
    lwdn.wait()
    lwup.wait()
    fw = wdn_h.shape[0] // N_BLK
    acc = jnp.zeros((seq, LANES), F32)

    def x1_chunk(j, acc):
        sum_a.finish(j)
        for c in groups(ALL_CHUNKS, j):
            z = xg[:, lc(c)].astype(F32) + t1[:, lc(c)].astype(F32) + vecs[4, :, lc(c)]
            x1[:, lc(c)] = z
            acc = acc + z
        return acc

    gyv = gyg[...]
    for j in range(n_all):
        if j < N_BLK:
            ff = slice(j * fw, (j + 1) * fw)
            gact[:, ff] = dot_t(gyv, wdn[ff, :]).astype(BF)
        sum_a.step_back(j)
        if j:
            acc = x1_chunk(j - 1, acc)
    acc = x1_chunk(n_all - 1, acc)

    mean = jnp.sum(acc, axis=1, keepdims=True) / D
    halves = (slice(0, seq // 2), slice(seq // 2, seq))
    rstd2 = []
    for n, hh in enumerate(halves):
        acc = jnp.zeros((seq // 2, LANES), F32)
        for c in range(nlc):
            z = x1[hh, lc(c)] - mean[hh]
            acc = acc + z * z
        rstd2.append(lax.rsqrt(jnp.sum(acc, axis=1, keepdims=True) / D + EPS))
    for n, hh in enumerate(halves):
        for c in range(nlc):
            z = (x1[hh, lc(c)] - mean[hh]) * rstd2[n]
            xhat[hh, lc(c)] = z
            g[hh, lc(c)] = (z * vecs[2, :, lc(c)] + vecs[3, :, lc(c)]).astype(BF)

    gv = g[...]
    for j in range(N_BLK):
        ff = slice(j * fw, (j + 1) * fw)
        pre = dot(gv, wup[:, ff]) + vecs[6, :, ff]
        w = (GELU_C * GELU_A) * (pre * pre)
        th = jnp.tanh(pre * (GELU_C + w))
        hp = 0.5 * pre
        r[:, ff] = (hp + hp * th).astype(BF)
        slope_g = (0.5 + 0.5 * th) + (hp * (1.0 - th * th)) * (GELU_C + 3.0 * w)
        gp = gact[:, ff].astype(F32) * slope_g
        vec[6, :, ff] = jnp.sum(gp, axis=0, keepdims=True)
        dpre[:, ff] = gp.astype(BF)

    dv = dpre[...]
    sum_g = AllSum(p2, rd2, s2, rs2, t2, q2, e2)
    for j in range(n_all):
        for c in [lc(c) for c in groups(ALL_CHUNKS, j)] if j == 0 else [sum_g.ch(j)]:
            p2[:, c] = dot_t(dv, wup[c, :]).astype(BF)
        sum_g.put(j)
        if j:
            sum_g.step_cross(j - 1)
    sum_g.step_cross(n_all - 1)

    acc1 = jnp.zeros((seq, LANES), F32)
    acc2 = jnp.zeros((seq, LANES), F32)

    def ln2_back_chunk(j, acc1, acc2):
        sum_g.finish(j)
        for c in groups(ALL_CHUNKS, j):
            dg = t2[:, lc(c)].astype(F32)
            z = xhat[:, lc(c)]
            dgz = dg * z
            vec[2, :, lc(c)] = jnp.sum(dgz, axis=0, keepdims=True)
            vec[3, :, lc(c)] = jnp.sum(dg, axis=0, keepdims=True)
            gain = vecs[2, :, lc(c)]
            dz = dg * gain
            acc1 = acc1 + dz
            acc2 = acc2 + dgz * gain
            for n, hh in enumerate(halves):
                ubuf[hh, lc(c)] = gyg[hh, lc(c)].astype(F32) + rstd2[n] * dz[hh]
        return acc1, acc2

    yw = D // N_BLK

    def down(j):
        yy = slice(j * yw, (j + 1) * yw)
        py[:, yy] = dot(r[...], wdn[:, yy]).astype(BF)
        for c in range(j * (yw // LANES), (j + 1) * (yw // LANES)):
            gt[lc(c), :] = g[:, lc(c)].T
            rt[lc(c), :] = r[:, lc(c)].T
            vec[5, :, lc(c)] = jnp.sum(gyg[:, lc(c)].astype(F32), axis=0, keepdims=True)
            for n, hh in enumerate(halves):
                xr[hh, lc(c)] = xhat[hh, lc(c)] * rstd2[n]

    def grad_down(m):
        mm = slice(m * GRAD_ROWS, (m + 1) * GRAD_ROWS)
        wdn[mm, :] = dot(rt[mm, :], gyg[...]).astype(BF)

    work = [(down, k) for k in range(N_BLK)] + [(grad_down, m) for m in range(wdn.shape[0] // GRAD_ROWS)]
    for j in range(n_all):
        for step, m in work[WORK_CUTS[j]:WORK_CUTS[j + 1]]:
            step(m)
        if j == 1:
            y_sib = remote(py.at[sibhalf, :], rdy, sib)
        sum_g.step_back(j)
        if j:
            acc1, acc2 = ln2_back_chunk(j - 1, acc1, acc2)
    y_sib.wait_recv()
    sy[...] = (py[half, :].astype(F32) + rdy[...].astype(F32)).astype(BF)
    y_cross = remote(sy.at[blk_cross, :], rsy, cross)
    acc1, acc2 = ln2_back_chunk(n_all - 1, acc1, acc2)

    for n, hh in enumerate(halves):
        mean1 = rstd2[n] * (jnp.sum(acc1[hh], axis=1, keepdims=True) / D)
        mean2 = jnp.sum(acc2[hh], axis=1, keepdims=True) / D
        for c in range(nlc):
            gm = ubuf[hh, lc(c)] - (mean1 + xr[hh, lc(c)] * mean2)
            gmid[hh, lc(c)] = gm
            ga[hh, lc(c)] = gm.astype(BF)

    gav = ga[...]
    hc = ctx.shape[0] // 2
    for k in range(2):
        dctx[k * hc:(k + 1) * hc, :] = dot_t(wout[k * hc:(k + 1) * hc, :], gav).astype(BF)

    def head_rows(hd):
        return slice(hd * head, (hd + 1) * head)

    for hd in range(n_heads):
        dpb[hd] = dot(vt[hd], dctx[head_rows(hd), :]).astype(BF)
    for hd in range(n_heads):
        dqkv[part_of(hd, 2), :] = dot_t(dctx[head_rows(hd), :], probb[hd]).astype(BF)
    for hd in range(n_heads):
        pr = prob[hd]
        dp = dpb[hd].astype(F32)
        dsb[hd] = (pr * (dp - jnp.sum(dp * pr, axis=0, keepdims=True))).astype(BF)
    for hd in range(n_heads):
        dqkv[part_of(hd, 0), :] = (dot(qkv[part_of(hd, 1), :], dsb[hd]) * score_scale).astype(BF)
        dqkv[part_of(hd, 1), :] = (dot_t(qkv[part_of(hd, 0), :], dsb[hd]) * score_scale).astype(BF)

    sum_h = ScatterSum(ph, rdh, sh, rsh, None, None, None)
    n_scat = len(SCATTER_CHUNKS)
    dq = dqkv[...].T
    for j in range(n_scat):
        for c in [lc(c) for c in groups(SCATTER_CHUNKS, j)] if j == 0 else [sum_h.ch(j)]:
            ph[:, c] = dot(dq, wqkv[:, c]).astype(BF)
        sum_h.put(j)
        if j:
            sum_h.step_cross(j - 1)
    sum_h.step_cross(n_scat - 1)

    rstd1 = ln_block(own, 32, xg, 0, 1, None)
    y_cross.wait_recv()
    for c in range(nlc):
        z = (sy[blk_own, lc(c)].astype(F32) + rsy[:, lc(c)].astype(F32)).astype(BF).astype(F32)
        ybuf[:, lc(c)] = (x1[own, lc(c)] + z + vecs[5, :, lc(c)]).astype(BF)
        vec[4, :, lc(c)] = jnp.sum(gmid[:, lc(c)], axis=0, keepdims=True)

    me = slot(t)
    acc1 = jnp.zeros((32, LANES), F32)
    acc2 = jnp.zeros((32, LANES), F32)
    parts = []
    for step, m in work[WORK_CUTS[-1]:]:
        step(m)
    for j in range(n_scat):
        sum_h.b[j].wait_recv()
        for c in groups(SCATTER_CHUNKS, j):
            dh = sum_h.result(lc(c))
            z = xh1[:, lc(c)]
            dhz = dh * z
            part_o[me, 0:1, lc(c)] = jnp.sum(dhz, axis=0, keepdims=True)
            part_o[me, 1:2, lc(c)] = jnp.sum(dh, axis=0, keepdims=True)
            gain = vecs[0, :, lc(c)]
            acc1 = acc1 + dh * gain
            acc2 = acc2 + dhz * gain
        if j >= n_scat - 2:
            c = slice(0, sum_h.ch(j).stop) if j == n_scat - 2 else sum_h.ch(j)
            parts += [remote(part_o.at[me, :, c], part_o.at[me, :, c], dev) for dev in (cross, sibcross, sib)]
    mean1 = jnp.sum(acc1, axis=1, keepdims=True) / D
    mean2 = jnp.sum(acc2, axis=1, keepdims=True) / D
    for c in range(nlc):
        dz = sum_h.result(lc(c)) * vecs[0, :, lc(c)]
        gxbuf[:, lc(c)] = (gmid[own, lc(c)] + rstd1 * (dz - mean1 - xh1[:, lc(c)] * mean2)).astype(BF)
    for copy in sent:
        copy.wait_send()
    for copy in parts:
        copy.wait_recv()


def grad_kernel(h, ga, dpre, dqkv, ctx, gt, dwdn, vec, part, y, gx,
                dwqkv_o, dwout_o, dwup_o, dwdn_o, dbqkv_o, y_o, gx_o, v0, v1, v2, v3, v4, v5, v6,
                buf, small, sums, bq, osem, ssem):
    n_heads, head = dbqkv_o.shape[1], dbqkv_o.shape[2]
    slots, block = buf.shape[0], buf.shape[1]
    tail = []

    def piece(k, start, size):
        small[k, pl.ds(0, size), :] = dot(ctx[start:start + size, :], ga[...]).astype(BF)
        copy = pltpu.make_async_copy(small.at[k, pl.ds(0, size), :], dwout_o.at[pl.ds(start, size), :], ssem.at[k])
        copy.start()
        tail.append(copy)

    def written(slot, out):
        return pltpu.make_async_copy(buf.at[slot], out.at[pl.ds(0, block), :], osem.at[slot])

    for k in range(4):
        n = dwdn.shape[0] // 4
        copy = pltpu.make_async_copy(dwdn.at[pl.ds(k * n, n), :], dwdn_o.at[pl.ds(k * n, n), :], ssem.at[14 + k])
        copy.start()
        tail.append(copy)
    piece(0, 0, 160)
    for k in range(2):
        sums[k] = (part[0, k:k + 1, :] + part[1, k:k + 1, :]) + (part[2, k:k + 1, :] + part[3, k:k + 1, :])

    def send(src, dst):
        copy = pltpu.make_async_copy(src, dst, ssem.at[len(tail) - 2])
        copy.start()
        tail.append(copy)

    send(y, y_o)
    send(gx, gx_o)
    for k, o in enumerate((v2, v3, v4, v5, v6)):
        send(vec.at[k + 2, 0], o)
    for k, o in enumerate((v0, v1)):
        send(sums.at[k, 0], o)
    first = 0
    for left, right, out in ((gt, dpre, dwup_o), (dqkv, h, dwqkv_o)):

        def body(m, carry, left=left, right=right, out=out, first=first):
            slot = lax.rem(first + m, slots)

            @pl.when(first + m >= slots)
            def _():
                written(slot, out).wait()

            at = pl.ds(pl.multiple_of(m * block, block), block)
            buf[slot] = dot(left[at, :], right[...]).astype(BF)
            pltpu.make_async_copy(buf.at[slot], out.at[at, :], osem.at[slot]).start()
            return carry

        count = left.shape[0] // block
        lax.fori_loop(0, count, body, 0)
        first += count
    piece(1, 160, 320)
    ones = jnp.ones((8, dqkv.shape[1]), BF)
    total = dot_t(ones, dqkv[...])[0:1]
    for k in range(3):
        for hd in range(n_heads):
            at = (hd * 3 + k) * head
            bq[k, hd:hd + 1, :] = total[:, at:at + head]
    send(bq, dbqkv_o)
    piece(2, 480, 160)
    for k in range(slots):
        written(k, dwqkv_o).wait()
    for copy in tail:
        copy.wait()


def solution(mesh):
    def local_step(x, ln1_gamma, ln1_beta, w_qkv, b_qkv, w_out, b_out, ln2_gamma, ln2_beta, w_up, b_up, w_down, b_down, grad_y):
        D = x.shape[2]
        S = TP * x.shape[1]
        nh, head = w_qkv.shape[1], w_qkv.shape[3]
        Q = nh * 3 * head
        C = nh * head
        FL = w_up.shape[1]
        any_spec = pl.BlockSpec(memory_space=pl.ANY)
        vspec = pl.BlockSpec(memory_space=pltpu.VMEM)
        vm = pltpu.VMEM
        wqkv_t = jnp.transpose(w_qkv, (1, 2, 3, 0)).reshape(Q, D)
        bq = jnp.transpose(b_qkv, (1, 0, 2))
        sds = jax.ShapeDtypeStruct
        n_loads = 2 + 7 + 1 + 4
        red = [vm((S, D), BF), vm((S // 2, D), BF), vm((S // 2, D), BF), vm((S // 2, D), BF), vm((S, D), BF),
               vm((S // 2, ALL_CHUNKS[-1] * LANES), BF), vm((S // 2, ALL_CHUNKS[-1] * LANES), BF)]
        scat = [vm((S, D), BF), vm((S // 2, D), BF), vm((S // 2, D), BF), vm((S // TP, D), BF)]
        row = lambda v: v
        res = pl.pallas_call(
            layer_kernel,
            name='layer',
            out_shape=[vm((S // TP, D), BF), vm((S // TP, D), BF), vm((7, 1, D), F32), vm((TP, 2, D), F32), vm((S, D), BF), vm((S, D), BF),
                       vm((S, FL), BF), vm((Q, S), BF), vm((C, S), BF), vm((D, S), BF), vm((FL, D), BF)],
            in_specs=[any_spec] * 14,
            out_specs=[vspec] * 11,
            scratch_shapes=[
                vm((Q, D), BF), vm((C, D), BF), vm((D, FL), BF), vm((FL, S), BF), vm((3, nh, head), F32), vm((7, 1, D), F32),
                vm((S, D), BF), vm((S, D), BF), vm((Q, S), F32), vm((Q, S), BF), vm((nh, S, S), F32),
                vm((nh, S, S), BF), vm((S, D), F32), vm((S, D), F32), vm((S, D), BF),
                vm((S, FL), BF), vm((S, FL), BF), vm((S, D), F32), vm((C, S), BF),
                vm((S // TP, D), F32), vm((S, D), F32), vm((S, D), F32),
                vm((nh, S, head), BF), vm((nh, S, S), BF), vm((nh, S, S), BF),
                *red, *red, *scat, *scat,
                pltpu.SemaphoreType.DMA((n_loads,)),
                pltpu.SemaphoreType.DMA((N_REMOTE,)), pltpu.SemaphoreType.DMA((N_REMOTE,)),
            ],
            compiler_params=pltpu.CompilerParams(collective_id=0, has_side_effects=True, vmem_limit_bytes=LAYER_VMEM),
        )(x.reshape(x.shape[1], D), grad_y.reshape(x.shape[1], D), wqkv_t, bq, w_out, w_up, w_down, row(ln1_gamma), row(ln1_beta),
          row(ln2_gamma), row(ln2_beta), row(b_out), row(b_down), row(b_up))
        y, gx, vec, part, h, ga, dpre, dqkv, ctx, gt, dwdn = res
        vshape = sds((D,), F32)
        outs = pl.pallas_call(
            grad_kernel,
            name='weight_grads',
            out_shape=[sds((Q, D), BF), sds((C, D), BF), sds((D, FL), BF), sds((FL, D), BF), sds((3, nh, head), F32),
                       sds((S // TP, D), BF), sds((S // TP, D), BF)] + [vshape] * 7,
            in_specs=[vspec] * 11,
            out_specs=[any_spec] * 14,
            scratch_shapes=[
                vm((3, 640, D), BF), vm((3, 320, D), BF), vm((2, 1, D), F32), vm((3, nh, head), F32),
                pltpu.SemaphoreType.DMA((3,)), pltpu.SemaphoreType.DMA((18,)),
            ],
            compiler_params=pltpu.CompilerParams(vmem_limit_bytes=GRAD_VMEM),
        )(h, ga, dpre, dqkv, ctx, gt, dwdn, vec, part, y, gx)
        dwqkv, dwout, dwup, dwdn, dbqkv, y, gx, g_ln1g, g_ln1b, g_ln2g, g_ln2b, g_bout, g_bdown, g_bup = outs
        dwqkv = jnp.transpose(dwqkv.reshape(nh, 3, head, D), (3, 0, 1, 2))
        dbqkv = jnp.transpose(dbqkv, (1, 0, 2))
        return (y.reshape(x.shape), gx.reshape(x.shape), g_ln1g, g_ln1b, dwqkv, dbqkv, dwout, g_bout,
                g_ln2g, g_ln2b, dwup, g_bup, dwdn, g_bdown)

    row_spec = P('dp', 'tp', None)
    in_specs = (row_spec, P(), P(), P(None, 'tp', None, None), P('tp', None, None), P('tp', None), P(), P(), P(),
                P(None, 'tp'), P('tp'), P('tp', None), P(), row_spec)
    out_specs = (row_spec, row_spec, P('dp'), P('dp'), P('dp', 'tp', None, None), P(('dp', 'tp'), None, None),
                 P(('dp', 'tp'), None), P('dp'), P('dp'), P('dp'), P('dp', 'tp'), P(('dp', 'tp')), P(('dp', 'tp'), None), P('dp'))
    return jax.shard_map(local_step, mesh=mesh, in_specs=in_specs, out_specs=out_specs, check_vma=False)
```

```python
import functools
import math
import jax
import jax.numpy as jnp
from jax import lax
from jax.experimental import pallas as pl
from jax.experimental.pallas import tpu as pltpu
from jax.sharding import PartitionSpec as P

EPS = 1e-5
MASK_VALUE = -1e30
BF = jnp.bfloat16
F32 = jnp.float32
MESH = pl.DeviceIdType.MESH
GELU_C = math.sqrt(2.0 / math.pi)
GELU_A = 0.044715
TP = 4
LANES = 128
ALL_CHUNKS = (2, 4, 4, 5, 4, 1)
SCATTER_CHUNKS = (2, 6, 8, 4)
N_BLK = 5
GRAD_ROWS = 640
WORK_CUTS = (0, 3, 5, 6, 7, 7, 7)
LAYER_VMEM = 47 * 1024 * 1024
GRAD_VMEM = 24 * 1024 * 1024
N_REMOTE = 62


def alibi_slopes(n_heads):
    closest = 2 ** int(math.floor(math.log2(n_heads)))
    base_ratio = 2.0 ** (-8.0 / closest)
    extra_ratio = 2.0 ** (-4.0 / closest)
    remaining = min(closest, n_heads - closest)
    slopes = [base_ratio ** (i + 1) for i in range(closest)]
    return slopes + [extra_ratio ** (2 * i + 1) for i in range(remaining)]


def dot(lhs, rhs):
    return lax.dot_general(lhs, rhs, (((1,), (0,)), ((), ())), preferred_element_type=F32)


def dot_t(lhs, rhs):
    return lax.dot_general(lhs, rhs, (((1,), (1,)), ((), ())), preferred_element_type=F32)


def layer_kernel(x_h, gy_h, wqkv_h, bqkv_h, wout_h, wup_h, wdn_h, ln1g_h, ln1b_h, ln2g_h, ln2b_h, bout_h, bdown_h, bup_h,
                 ybuf, gxbuf, vec, part_o, h, ga, dpre, dqkv, ctx, gt, wdn,
                 wqkv, wout, wup, rt, bqkv, vecs, xg, gyg, bias, qkv, prob, probb, x1, xhat, g, gact, r,
                 gmid, dctx, xh1, ubuf, xr, vt, dpb, dsb,
                 p1, rd1, s1, rs1, t1, q1, e1, p2, rd2, s2, rs2, t2, q2, e2, py, rdy, sy, rsy, ph, rdh, sh, rsh,
                 lsem, ssem, rsem):
    D = x_h.shape[1]
    seq = TP * 32
    head = bqkv_h.shape[2]
    n_heads = bqkv_h.shape[1]
    nlc = D // LANES
    t = lax.axis_index('tp')
    core = lax.rem(t, 2)
    chip = t // 2
    sib = t + 1 - 2 * core
    cross = lax.rem(sib + 2, TP)
    sibcross = lax.rem(t + 2, TP)
    side = lax.rem(core + chip, 2)

    def slot(dev):
        return lax.rem(lax.rem(dev, 2) + dev // 2, 2) * 2 + dev // 2

    def rows(dev):
        return pl.ds(pl.multiple_of(slot(dev) * 32, 32), 32)

    own = rows(t)
    half = pl.ds(pl.multiple_of(side * 64, 64), 64)
    sibhalf = pl.ds(pl.multiple_of((1 - side) * 64, 64), 64)
    blk_own = pl.ds(pl.multiple_of(chip * 32, 32), 32)
    blk_cross = pl.ds(pl.multiple_of((1 - chip) * 32, 32), 32)

    counter = [0, 0]

    def load(src, dst):
        k = counter[0]
        counter[0] += 1
        copy = pltpu.make_async_copy(src, dst, lsem.at[k])
        copy.start()
        return copy

    sent = []

    def remote(src, dst, dev):
        k = counter[1]
        counter[1] += 1
        copy = pltpu.make_async_remote_copy(src_ref=src, dst_ref=dst, send_sem=ssem.at[k], recv_sem=rsem.at[k],
                                            device_id={'tp': dev}, device_id_type=MESH)
        copy.start()
        sent.append(copy)
        return copy

    def lc(c):
        return slice(c * LANES, (c + 1) * LANES)

    def groups(widths, j):
        start = sum(widths[:j])
        return range(start, start + widths[j])

    def cols(widths, j):
        return slice(sum(widths[:j]) * LANES, sum(widths[:j + 1]) * LANES)

    lx = load(x_h, xg.at[own, :])
    lg = load(gy_h, gyg.at[own, :])
    lvec = [load(src, vecs.at[k, 0]) for k, src in enumerate((ln1g_h, ln1b_h, ln2g_h, ln2b_h, bout_h, bdown_h, bup_h))]
    lb = load(bqkv_h, bqkv)
    lwqkv = load(wqkv_h, wqkv)
    lwout = load(wout_h, wout)
    barrier = pltpu.get_barrier_semaphore()
    for dev in (sib, cross, sibcross):
        pl.semaphore_signal(barrier, inc=1, device_id={'tp': dev}, device_id_type=MESH)
    pl.semaphore_wait(barrier, 3)
    lx.wait()
    def piece(dev, k):
        return pl.ds(pl.multiple_of(slot(dev) * 32 + 16 * k, 16), 16)

    x_to_cross = [remote(xg.at[piece(t, k), :], xg.at[piece(t, k), :], cross) for k in range(2)]
    x_to_sib = remote(xg.at[own, :], xg.at[own, :], sib)
    lg.wait()
    gy_to_sib = remote(gyg.at[own, :], gyg.at[own, :], sib)
    lwdn = load(wdn_h, wdn)
    lwup = load(wup_h, wup)
    for copy in lvec:
        copy.wait()

    def ln_block(rr, n, src, gain, shift, dst):
        acc = jnp.zeros((n, LANES), F32)
        for c in range(nlc):
            acc = acc + src[rr, lc(c)].astype(F32)
        mean = jnp.sum(acc, axis=1, keepdims=True) / D
        acc = jnp.zeros((n, LANES), F32)
        for c in range(nlc):
            z = src[rr, lc(c)].astype(F32) - mean
            acc = acc + z * z
        rstd = lax.rsqrt(jnp.sum(acc, axis=1, keepdims=True) / D + EPS)
        for c in range(nlc):
            z = (src[rr, lc(c)].astype(F32) - mean) * rstd
            if dst is not None:
                dst[rr, lc(c)] = (z * vecs[gain, :, lc(c)] + vecs[shift, :, lc(c)]).astype(BF)
            else:
                xh1[:, lc(c)] = z
        return rstd

    ln_block(own, 32, xg, 0, 1, h)
    lb.wait()
    for k in range(3):
        bt = bqkv[k].T
        for hd in range(n_heads):
            at = (hd * 3 + k) * head
            bias[at:at + head, :] = jnp.broadcast_to(bt[:head, hd:hd + 1], (head, seq))
    x_to_sib.wait_recv()
    ln_block(rows(sib), 32, xg, 0, 1, h)
    x_fwd = []
    for k in range(2):
        x_to_cross[k].wait_recv()
        x_fwd.append(remote(xg.at[piece(cross, k), :], xg.at[piece(cross, k), :], sib))
    gy_to_cross = remote(gyg.at[own, :], gyg.at[own, :], cross)
    lwqkv.wait()
    lwout.wait()
    ln_block(rows(cross), 32, xg, 0, 1, h)
    for k in range(2):
        x_fwd[k].wait_recv()
    ln_block(rows(sibcross), 32, xg, 0, 1, h)

    hr = 2 * 3 * head
    hv = h[...]
    for m in range(n_heads // 2):
        mm = slice(m * hr, (m + 1) * hr)
        qkv[mm, :] = (dot_t(wqkv[mm, :], hv) + bias[mm, :]).astype(BF)

    def position(axis):
        i = lax.broadcasted_iota(jnp.int32, (seq, seq), axis)
        b = i >> 5
        return ((((b & 1) << 1) | (((b >> 1) ^ b) & 1)) << 5) | (i & 31)

    pos_k = position(0)
    causal = pos_k <= position(1)
    key_f = pos_k.astype(F32)
    slopes = alibi_slopes(n_heads * TP)
    score_scale = head ** -0.5

    def part_of(hd, k):
        at = (hd * 3 + k) * head
        return slice(at, at + head)

    def slope(hd):
        v = jnp.float32(slopes[hd])
        for dev in range(1, TP):
            v = jnp.where(t == dev, jnp.float32(slopes[dev * n_heads + hd]), v)
        return v

    for hd in range(n_heads):
        prob[hd] = dot(qkv[part_of(hd, 1), :].T, qkv[part_of(hd, 0), :])
    for hd in range(n_heads):
        s = jnp.where(causal, prob[hd] * score_scale + slope(hd) * key_f, MASK_VALUE)
        e = jnp.exp(s - jnp.max(s, axis=0, keepdims=True))
        pr = e * (1.0 / jnp.sum(e, axis=0, keepdims=True))
        prob[hd] = pr
        probb[hd] = pr.astype(BF)
    for hd in range(n_heads):
        ctx[hd * head:(hd + 1) * head, :] = dot(qkv[part_of(hd, 2), :], probb[hd]).astype(BF)

    class AllSum:
        widths = ALL_CHUNKS

        def __init__(self, p, rd, s, rs, tt, q, e):
            self.p, self.rd, self.s, self.rs, self.tt, self.q, self.e = p, rd, s, rs, tt, q, e
            self.a, self.b, self.c = {}, {}, {}
            self.last = len(self.widths) - 1

        def ch(self, j):
            return cols(self.widths, j)

        def fill(self, j, value):
            self.p[:, self.ch(j)] = value

        def put(self, j):
            self.a[j] = remote(self.p.at[sibhalf, self.ch(j)], self.rd.at[:, self.ch(j)], sib)

        def pair(self, j):
            self.a[j].wait_recv()
            c = self.ch(j)
            self.s[:, c] = (self.p[half, c].astype(F32) + self.rd[:, c].astype(F32)).astype(BF)

        def step_cross(self, j):
            self.pair(j)
            c = self.ch(j)
            if j == self.last:
                self.c[j] = (remote(self.s.at[:, c], self.e.at[:, :], sibcross), remote(self.s.at[:, c], self.q.at[:, :], sib))
            self.b[j] = remote(self.s.at[:, c], self.rs.at[:, c], cross)

        def step_back(self, j):
            self.b[j].wait_recv()
            c = self.ch(j)
            self.tt[half, c] = (self.s[:, c].astype(F32) + self.rs[:, c].astype(F32)).astype(BF)
            if j < self.last:
                self.c[j] = remote(self.tt.at[half, c], self.tt.at[half, c], sib)

        def finish(self, j):
            if j < self.last:
                self.c[j].wait_recv()
            else:
                for copy in self.c[j]:
                    copy.wait_recv()
                self.tt[sibhalf, self.ch(j)] = (self.q[...].astype(F32) + self.e[...].astype(F32)).astype(BF)

    class ScatterSum(AllSum):
        widths = SCATTER_CHUNKS

        def step_cross(self, j):
            self.pair(j)
            c = self.ch(j)
            self.b[j] = remote(self.s.at[blk_cross, c], self.rs.at[:, c], cross)

        def result(self, c):
            return (self.s[blk_own, c].astype(F32) + self.rs[:, c].astype(F32)).astype(BF).astype(F32)

    o_flat = ctx[...].T
    sum_a = AllSum(p1, rd1, s1, rs1, t1, q1, e1)
    n_all = len(ALL_CHUNKS)
    sum_a.fill(0, dot(o_flat, wout[:, sum_a.ch(0)]).astype(BF))
    sum_a.put(0)
    for j in range(1, n_all):
        sum_a.fill(j, dot(o_flat, wout[:, sum_a.ch(j)]).astype(BF))
    for j in range(1, n_all):
        sum_a.put(j)
    for j in range(n_all):
        sum_a.step_cross(j)

    gy_to_sib.wait_recv()
    gy_to_cross.wait_recv()
    gy_fwd = remote(gyg.at[rows(cross), :], gyg.at[rows(cross), :], sib)
    for hd in range(n_heads):
        vt[hd] = qkv[part_of(hd, 2), :].T
    gy_fwd.wait_recv()
    lwdn.wait()
    lwup.wait()
    fw = wdn_h.shape[0] // N_BLK
    shift = None
    acc1 = jnp.zeros((seq, LANES), F32)
    acc2 = jnp.zeros((seq, LANES), F32)

    def x1_chunk(j, shift, acc1, acc2):
        sum_a.finish(j)
        total = jnp.zeros((seq, LANES), F32)
        for c in groups(ALL_CHUNKS, j):
            z = xg[:, lc(c)].astype(F32) + t1[:, lc(c)].astype(F32) + vecs[4, :, lc(c)]
            x1[:, lc(c)] = z
            if j == 0:
                total = total + z
            else:
                d = z - shift
                acc1 = acc1 + d
                acc2 = acc2 + d * d
        if j == 0:
            shift = jnp.sum(total, axis=1, keepdims=True) / (ALL_CHUNKS[0] * LANES)
            for c in groups(ALL_CHUNKS, j):
                d = x1[:, lc(c)] - shift
                acc1 = acc1 + d
                acc2 = acc2 + d * d
        return shift, acc1, acc2

    gyv = gyg[...]
    for j in range(n_all):
        if j < N_BLK:
            ff = slice(j * fw, (j + 1) * fw)
            gact[:, ff] = dot_t(gyv, wdn[ff, :]).astype(BF)
        sum_a.step_back(j)
        if j:
            shift, acc1, acc2 = x1_chunk(j - 1, shift, acc1, acc2)
    shift, acc1, acc2 = x1_chunk(n_all - 1, shift, acc1, acc2)

    off = jnp.sum(acc1, axis=1, keepdims=True) / D
    mean = shift + off
    rstd = lax.rsqrt(jnp.sum(acc2, axis=1, keepdims=True) / D - off * off + EPS)
    halves = (slice(0, seq // 2), slice(seq // 2, seq))
    rstd2 = [rstd[hh] for hh in halves]
    for n, hh in enumerate(halves):
        for c in range(nlc):
            z = (x1[hh, lc(c)] - mean[hh]) * rstd2[n]
            xhat[hh, lc(c)] = z
            g[hh, lc(c)] = (z * vecs[2, :, lc(c)] + vecs[3, :, lc(c)]).astype(BF)

    gv = g[...]
    for j in range(N_BLK):
        ff = slice(j * fw, (j + 1) * fw)
        pre = dot(gv, wup[:, ff]) + vecs[6, :, ff]
        w = (GELU_C * GELU_A) * (pre * pre)
        th = jnp.tanh(pre * (GELU_C + w))
        hp = 0.5 * pre
        r[:, ff] = (hp + hp * th).astype(BF)
        slope_g = (0.5 + 0.5 * th) + (hp * (1.0 - th * th)) * (GELU_C + 3.0 * w)
        gp = gact[:, ff].astype(F32) * slope_g
        vec[6, :, ff] = jnp.sum(gp, axis=0, keepdims=True)
        dpre[:, ff] = gp.astype(BF)

    dv = dpre[...]
    sum_g = AllSum(p2, rd2, s2, rs2, t2, q2, e2)
    for j in range(n_all):
        for c in [lc(c) for c in groups(ALL_CHUNKS, j)] if j == 0 else [sum_g.ch(j)]:
            p2[:, c] = dot_t(dv, wup[c, :]).astype(BF)
        sum_g.put(j)
        if j:
            sum_g.step_cross(j - 1)
    sum_g.step_cross(n_all - 1)

    acc1 = jnp.zeros((seq, LANES), F32)
    acc2 = jnp.zeros((seq, LANES), F32)

    def ln2_back_chunk(j, acc1, acc2):
        sum_g.finish(j)
        for c in groups(ALL_CHUNKS, j):
            dg = t2[:, lc(c)].astype(F32)
            z = xhat[:, lc(c)]
            dgz = dg * z
            vec[2, :, lc(c)] = jnp.sum(dgz, axis=0, keepdims=True)
            vec[3, :, lc(c)] = jnp.sum(dg, axis=0, keepdims=True)
            gain = vecs[2, :, lc(c)]
            dz = dg * gain
            acc1 = acc1 + dz
            acc2 = acc2 + dgz * gain
            for n, hh in enumerate(halves):
                ubuf[hh, lc(c)] = gyg[hh, lc(c)].astype(F32) + rstd2[n] * dz[hh]
        return acc1, acc2

    yw = D // N_BLK

    def down(j):
        yy = slice(j * yw, (j + 1) * yw)
        py[:, yy] = dot(r[...], wdn[:, yy]).astype(BF)
        for c in range(j * (yw // LANES), (j + 1) * (yw // LANES)):
            gt[lc(c), :] = g[:, lc(c)].T
            rt[lc(c), :] = r[:, lc(c)].T
            vec[5, :, lc(c)] = jnp.sum(gyg[:, lc(c)].astype(F32), axis=0, keepdims=True)
            for n, hh in enumerate(halves):
                xr[hh, lc(c)] = xhat[hh, lc(c)] * rstd2[n]

    def grad_down(m):
        mm = slice(m * GRAD_ROWS, (m + 1) * GRAD_ROWS)
        wdn[mm, :] = dot(rt[mm, :], gyg[...]).astype(BF)

    work = [(down, k) for k in range(N_BLK)] + [(grad_down, m) for m in range(wdn.shape[0] // GRAD_ROWS)]
    for j in range(n_all):
        for step, m in work[WORK_CUTS[j]:WORK_CUTS[j + 1]]:
            step(m)
        if j == 1:
            y_sib = remote(py.at[sibhalf, :], rdy, sib)
        sum_g.step_back(j)
        if j:
            acc1, acc2 = ln2_back_chunk(j - 1, acc1, acc2)
    y_sib.wait_recv()
    sy[...] = (py[half, :].astype(F32) + rdy[...].astype(F32)).astype(BF)
    y_cross = remote(sy.at[blk_cross, :], rsy, cross)
    acc1, acc2 = ln2_back_chunk(n_all - 1, acc1, acc2)

    for n, hh in enumerate(halves):
        mean1 = rstd2[n] * (jnp.sum(acc1[hh], axis=1, keepdims=True) / D)
        mean2 = jnp.sum(acc2[hh], axis=1, keepdims=True) / D
        for c in range(nlc):
            gm = ubuf[hh, lc(c)] - (mean1 + xr[hh, lc(c)] * mean2)
            gmid[hh, lc(c)] = gm
            ga[hh, lc(c)] = gm.astype(BF)

    gav = ga[...]
    hc = ctx.shape[0] // 2
    for k in range(2):
        dctx[k * hc:(k + 1) * hc, :] = dot_t(wout[k * hc:(k + 1) * hc, :], gav).astype(BF)

    def head_rows(hd):
        return slice(hd * head, (hd + 1) * head)

    for hd in range(n_heads):
        dpb[hd] = dot(vt[hd], dctx[head_rows(hd), :]).astype(BF)
    for hd in range(n_heads):
        dqkv[part_of(hd, 2), :] = dot_t(dctx[head_rows(hd), :], probb[hd]).astype(BF)
    for hd in range(n_heads):
        pr = prob[hd]
        dp = dpb[hd].astype(F32)
        dsb[hd] = (pr * (dp - jnp.sum(dp * pr, axis=0, keepdims=True))).astype(BF)
    for hd in range(n_heads):
        dqkv[part_of(hd, 0), :] = (dot(qkv[part_of(hd, 1), :], dsb[hd]) * score_scale).astype(BF)
        dqkv[part_of(hd, 1), :] = (dot_t(qkv[part_of(hd, 0), :], dsb[hd]) * score_scale).astype(BF)

    sum_h = ScatterSum(ph, rdh, sh, rsh, None, None, None)
    n_scat = len(SCATTER_CHUNKS)
    dq = dqkv[...].T
    for j in range(n_scat):
        for c in [lc(c) for c in groups(SCATTER_CHUNKS, j)] if j == 0 else [sum_h.ch(j)]:
            ph[:, c] = dot(dq, wqkv[:, c]).astype(BF)
        sum_h.put(j)
        if j:
            sum_h.step_cross(j - 1)
    sum_h.step_cross(n_scat - 1)

    rstd1 = ln_block(own, 32, xg, 0, 1, None)
    y_cross.wait_recv()
    for c in range(nlc):
        z = (sy[blk_own, lc(c)].astype(F32) + rsy[:, lc(c)].astype(F32)).astype(BF).astype(F32)
        ybuf[:, lc(c)] = (x1[own, lc(c)] + z + vecs[5, :, lc(c)]).astype(BF)
        vec[4, :, lc(c)] = jnp.sum(gmid[:, lc(c)], axis=0, keepdims=True)

    me = slot(t)
    acc1 = jnp.zeros((32, LANES), F32)
    acc2 = jnp.zeros((32, LANES), F32)
    parts = []
    for step, m in work[WORK_CUTS[-1]:]:
        step(m)
    for j in range(n_scat):
        sum_h.b[j].wait_recv()
        for c in groups(SCATTER_CHUNKS, j):
            dh = sum_h.result(lc(c))
            z = xh1[:, lc(c)]
            dhz = dh * z
            part_o[me, 0:1, lc(c)] = jnp.sum(dhz, axis=0, keepdims=True)
            part_o[me, 1:2, lc(c)] = jnp.sum(dh, axis=0, keepdims=True)
            gain = vecs[0, :, lc(c)]
            acc1 = acc1 + dh * gain
            acc2 = acc2 + dhz * gain
        if j >= n_scat - 2:
            c = slice(0, sum_h.ch(j).stop) if j == n_scat - 2 else sum_h.ch(j)
            parts += [remote(part_o.at[me, :, c], part_o.at[me, :, c], dev) for dev in (sibcross, cross, sib)]
    mean1 = jnp.sum(acc1, axis=1, keepdims=True) / D
    mean2 = jnp.sum(acc2, axis=1, keepdims=True) / D
    for c in range(nlc):
        dz = sum_h.result(lc(c)) * vecs[0, :, lc(c)]
        gxbuf[:, lc(c)] = (gmid[own, lc(c)] + rstd1 * (dz - mean1 - xh1[:, lc(c)] * mean2)).astype(BF)
    for copy in sent:
        copy.wait_send()
    for copy in parts:
        copy.wait_recv()


def grad_kernel(h, ga, dpre, dqkv, ctx, gt, dwdn, vec, part, y, gx,
                dwqkv_o, dwout_o, dwup_o, dwdn_o, dbqkv_o, y_o, gx_o, v0, v1, v2, v3, v4, v5, v6,
                buf, small, sums, bq, osem, ssem):
    n_heads, head = dbqkv_o.shape[1], dbqkv_o.shape[2]
    slots, block = buf.shape[0], buf.shape[1]
    tail = []

    def piece(k, start, size):
        small[k, pl.ds(0, size), :] = dot(ctx[start:start + size, :], ga[...]).astype(BF)
        copy = pltpu.make_async_copy(small.at[k, pl.ds(0, size), :], dwout_o.at[pl.ds(start, size), :], ssem.at[k])
        copy.start()
        tail.append(copy)

    def written(slot, out):
        return pltpu.make_async_copy(buf.at[slot], out.at[pl.ds(0, block), :], osem.at[slot])

    for k in range(4):
        n = dwdn.shape[0] // 4
        copy = pltpu.make_async_copy(dwdn.at[pl.ds(k * n, n), :], dwdn_o.at[pl.ds(k * n, n), :], ssem.at[14 + k])
        copy.start()
        tail.append(copy)
    piece(0, 0, 160)
    for k in range(2):
        sums[k] = (part[0, k:k + 1, :] + part[1, k:k + 1, :]) + (part[2, k:k + 1, :] + part[3, k:k + 1, :])

    def send(src, dst):
        copy = pltpu.make_async_copy(src, dst, ssem.at[len(tail) - 2])
        copy.start()
        tail.append(copy)

    send(y, y_o)
    send(gx, gx_o)
    for k, o in enumerate((v2, v3, v4, v5, v6)):
        send(vec.at[k + 2, 0], o)
    for k, o in enumerate((v0, v1)):
        send(sums.at[k, 0], o)
    first = 0
    for left, right, out in ((gt, dpre, dwup_o), (dqkv, h, dwqkv_o)):

        def body(m, carry, left=left, right=right, out=out, first=first):
            slot = lax.rem(first + m, slots)

            @pl.when(first + m >= slots)
            def _():
                written(slot, out).wait()

            at = pl.ds(pl.multiple_of(m * block, block), block)
            buf[slot] = dot(left[at, :], right[...]).astype(BF)
            pltpu.make_async_copy(buf.at[slot], out.at[at, :], osem.at[slot]).start()
            return carry

        count = left.shape[0] // block
        lax.fori_loop(0, count, body, 0)
        first += count
    piece(1, 160, 320)
    ones = jnp.ones((8, dqkv.shape[1]), BF)
    total = dot_t(ones, dqkv[...])[0:1]
    for k in range(3):
        for hd in range(n_heads):
            at = (hd * 3 + k) * head
            bq[k, hd:hd + 1, :] = total[:, at:at + head]
    send(bq, dbqkv_o)
    piece(2, 480, 160)
    for k in range(slots):
        written(k, dwqkv_o).wait()
    for copy in tail:
        copy.wait()


def solution(mesh):
    def local_step(x, ln1_gamma, ln1_beta, w_qkv, b_qkv, w_out, b_out, ln2_gamma, ln2_beta, w_up, b_up, w_down, b_down, grad_y):
        D = x.shape[2]
        S = TP * x.shape[1]
        nh, head = w_qkv.shape[1], w_qkv.shape[3]
        Q = nh * 3 * head
        C = nh * head
        FL = w_up.shape[1]
        any_spec = pl.BlockSpec(memory_space=pl.ANY)
        vspec = pl.BlockSpec(memory_space=pltpu.VMEM)
        vm = pltpu.VMEM
        wqkv_t = jnp.transpose(w_qkv, (1, 2, 3, 0)).reshape(Q, D)
        bq = jnp.transpose(b_qkv, (1, 0, 2))
        sds = jax.ShapeDtypeStruct
        n_loads = 2 + 7 + 1 + 4
        red = [vm((S, D), BF), vm((S // 2, D), BF), vm((S // 2, D), BF), vm((S // 2, D), BF), vm((S, D), BF),
               vm((S // 2, ALL_CHUNKS[-1] * LANES), BF), vm((S // 2, ALL_CHUNKS[-1] * LANES), BF)]
        scat = [vm((S, D), BF), vm((S // 2, D), BF), vm((S // 2, D), BF), vm((S // TP, D), BF)]
        row = lambda v: v
        res = pl.pallas_call(
            layer_kernel,
            name='layer',
            out_shape=[vm((S // TP, D), BF), vm((S // TP, D), BF), vm((7, 1, D), F32), vm((TP, 2, D), F32), vm((S, D), BF), vm((S, D), BF),
                       vm((S, FL), BF), vm((Q, S), BF), vm((C, S), BF), vm((D, S), BF), vm((FL, D), BF)],
            in_specs=[any_spec] * 14,
            out_specs=[vspec] * 11,
            scratch_shapes=[
                vm((Q, D), BF), vm((C, D), BF), vm((D, FL), BF), vm((FL, S), BF), vm((3, nh, head), F32), vm((7, 1, D), F32),
                vm((S, D), BF), vm((S, D), BF), vm((Q, S), F32), vm((Q, S), BF), vm((nh, S, S), F32),
                vm((nh, S, S), BF), vm((S, D), F32), vm((S, D), F32), vm((S, D), BF),
                vm((S, FL), BF), vm((S, FL), BF), vm((S, D), F32), vm((C, S), BF),
                vm((S // TP, D), F32), vm((S, D), F32), vm((S, D), F32),
                vm((nh, S, head), BF), vm((nh, S, S), BF), vm((nh, S, S), BF),
                *red, *red, *scat, *scat,
                pltpu.SemaphoreType.DMA((n_loads,)),
                pltpu.SemaphoreType.DMA((N_REMOTE,)), pltpu.SemaphoreType.DMA((N_REMOTE,)),
            ],
            compiler_params=pltpu.CompilerParams(collective_id=0, has_side_effects=True, vmem_limit_bytes=LAYER_VMEM),
        )(x.reshape(x.shape[1], D), grad_y.reshape(x.shape[1], D), wqkv_t, bq, w_out, w_up, w_down, row(ln1_gamma), row(ln1_beta),
          row(ln2_gamma), row(ln2_beta), row(b_out), row(b_down), row(b_up))
        y, gx, vec, part, h, ga, dpre, dqkv, ctx, gt, dwdn = res
        vshape = sds((D,), F32)
        outs = pl.pallas_call(
            grad_kernel,
            name='weight_grads',
            out_shape=[sds((Q, D), BF), sds((C, D), BF), sds((D, FL), BF), sds((FL, D), BF), sds((3, nh, head), F32),
                       sds((S // TP, D), BF), sds((S // TP, D), BF)] + [vshape] * 7,
            in_specs=[vspec] * 11,
            out_specs=[any_spec] * 14,
            scratch_shapes=[
                vm((3, 640, D), BF), vm((3, 320, D), BF), vm((2, 1, D), F32), vm((3, nh, head), F32),
                pltpu.SemaphoreType.DMA((3,)), pltpu.SemaphoreType.DMA((18,)),
            ],
            compiler_params=pltpu.CompilerParams(vmem_limit_bytes=GRAD_VMEM),
        )(h, ga, dpre, dqkv, ctx, gt, dwdn, vec, part, y, gx)
        dwqkv, dwout, dwup, dwdn, dbqkv, y, gx, g_ln1g, g_ln1b, g_ln2g, g_ln2b, g_bout, g_bdown, g_bup = outs
        dwqkv = jnp.transpose(dwqkv.reshape(nh, 3, head, D), (3, 0, 1, 2))
        dbqkv = jnp.transpose(dbqkv, (1, 0, 2))
        return (y.reshape(x.shape), gx.reshape(x.shape), g_ln1g, g_ln1b, dwqkv, dbqkv, dwout, g_bout,
                g_ln2g, g_ln2b, dwup, g_bup, dwdn, g_bdown)

    row_spec = P('dp', 'tp', None)
    in_specs = (row_spec, P(), P(), P(None, 'tp', None, None), P('tp', None, None), P('tp', None), P(), P(), P(),
                P(None, 'tp'), P('tp'), P('tp', None), P(), row_spec)
    out_specs = (row_spec, row_spec, P('dp'), P('dp'), P('dp', 'tp', None, None), P(('dp', 'tp'), None, None),
                 P(('dp', 'tp'), None), P('dp'), P('dp'), P('dp'), P('dp', 'tp'), P(('dp', 'tp')), P(('dp', 'tp'), None), P('dp'))
    return jax.shard_map(local_step, mesh=mesh, in_specs=in_specs, out_specs=out_specs, check_vma=False)
```

```python
import functools
import math
import jax
import jax.numpy as jnp
from jax import lax
from jax.experimental import pallas as pl
from jax.experimental.pallas import tpu as pltpu
from jax.sharding import PartitionSpec as P

EPS = 1e-5
MASK_VALUE = -1e30
BF = jnp.bfloat16
F32 = jnp.float32
MESH = pl.DeviceIdType.MESH
GELU_C = math.sqrt(2.0 / math.pi)
GELU_A = 0.044715
TP = 4
LANES = 128
ALL_CHUNKS = (2, 4, 4, 5, 4, 1)
SCATTER_CHUNKS = (2, 6, 8, 4)
N_BLK = 5
GRAD_ROWS = 640
WORK_CUTS = (0, 3, 5, 6, 7, 7, 7)
LAYER_VMEM = 47 * 1024 * 1024
GRAD_VMEM = 24 * 1024 * 1024
N_REMOTE = 62


def alibi_slopes(n_heads):
    closest = 2 ** int(math.floor(math.log2(n_heads)))
    base_ratio = 2.0 ** (-8.0 / closest)
    extra_ratio = 2.0 ** (-4.0 / closest)
    remaining = min(closest, n_heads - closest)
    slopes = [base_ratio ** (i + 1) for i in range(closest)]
    return slopes + [extra_ratio ** (2 * i + 1) for i in range(remaining)]


def dot(lhs, rhs):
    return lax.dot_general(lhs, rhs, (((1,), (0,)), ((), ())), preferred_element_type=F32)


def dot_t(lhs, rhs):
    return lax.dot_general(lhs, rhs, (((1,), (1,)), ((), ())), preferred_element_type=F32)


def layer_kernel(x_h, gy_h, wqkv_h, bqkv_h, wout_h, wup_h, wdn_h, ln1g_h, ln1b_h, ln2g_h, ln2b_h, bout_h, bdown_h, bup_h,
                 ybuf, gxbuf, vec, part_o, h, ga, dpre, dqkv, ctx, gt, wdn,
                 wqkv, wout, wup, rt, bqkv, vecs, xg, gyg, bias, qkv, prob, probb, x1, xhat, g, gact, r,
                 gmid, dctx, xh1, ubuf, xr, vt, dpb, dsb,
                 p1, rd1, s1, rs1, t1, q1, e1, p2, rd2, s2, rs2, t2, q2, e2, py, rdy, sy, rsy, ph, rdh, sh, rsh,
                 lsem, ssem, rsem):
    D = x_h.shape[1]
    seq = TP * 32
    head = bqkv_h.shape[2]
    n_heads = bqkv_h.shape[1]
    nlc = D // LANES
    t = lax.axis_index('tp')
    core = lax.rem(t, 2)
    chip = t // 2
    sib = t + 1 - 2 * core
    cross = lax.rem(sib + 2, TP)
    sibcross = lax.rem(t + 2, TP)
    side = lax.rem(core + chip, 2)

    def slot(dev):
        return lax.rem(lax.rem(dev, 2) + dev // 2, 2) * 2 + dev // 2

    def rows(dev):
        return pl.ds(pl.multiple_of(slot(dev) * 32, 32), 32)

    own = rows(t)
    half = pl.ds(pl.multiple_of(side * 64, 64), 64)
    sibhalf = pl.ds(pl.multiple_of((1 - side) * 64, 64), 64)
    blk_own = pl.ds(pl.multiple_of(chip * 32, 32), 32)
    blk_cross = pl.ds(pl.multiple_of((1 - chip) * 32, 32), 32)

    counter = [0, 0]

    def load(src, dst):
        k = counter[0]
        counter[0] += 1
        copy = pltpu.make_async_copy(src, dst, lsem.at[k])
        copy.start()
        return copy

    sent = []

    def remote(src, dst, dev):
        k = counter[1]
        counter[1] += 1
        copy = pltpu.make_async_remote_copy(src_ref=src, dst_ref=dst, send_sem=ssem.at[k], recv_sem=rsem.at[k],
                                            device_id={'tp': dev}, device_id_type=MESH)
        copy.start()
        sent.append(copy)
        return copy

    def lc(c):
        return slice(c * LANES, (c + 1) * LANES)

    def groups(widths, j):
        start = sum(widths[:j])
        return range(start, start + widths[j])

    def cols(widths, j):
        return slice(sum(widths[:j]) * LANES, sum(widths[:j + 1]) * LANES)

    lx = load(x_h, xg.at[own, :])
    lg = load(gy_h, gyg.at[own, :])
    lvec = [load(src, vecs.at[k, 0]) for k, src in enumerate((ln1g_h, ln1b_h, ln2g_h, ln2b_h, bout_h, bdown_h, bup_h))]
    lb = load(bqkv_h, bqkv)
    lwqkv = load(wqkv_h, wqkv)
    lwout = load(wout_h, wout)
    barrier = pltpu.get_barrier_semaphore()
    for dev in (sib, cross, sibcross):
        pl.semaphore_signal(barrier, inc=1, device_id={'tp': dev}, device_id_type=MESH)
    pl.semaphore_wait(barrier, 3)
    lx.wait()
    def piece(dev, k):
        return pl.ds(pl.multiple_of(slot(dev) * 32 + 16 * k, 16), 16)

    x_to_cross = [remote(xg.at[piece(t, k), :], xg.at[piece(t, k), :], cross) for k in range(2)]
    x_to_sib = remote(xg.at[own, :], xg.at[own, :], sib)
    lg.wait()
    gy_to_sib = remote(gyg.at[own, :], gyg.at[own, :], sib)
    lwdn = load(wdn_h, wdn)
    lwup = load(wup_h, wup)
    for copy in lvec:
        copy.wait()

    def ln_block(rr, n, src, gain, shift, dst):
        acc = jnp.zeros((n, LANES), F32)
        for c in range(nlc):
            acc = acc + src[rr, lc(c)].astype(F32)
        mean = jnp.sum(acc, axis=1, keepdims=True) / D
        acc = jnp.zeros((n, LANES), F32)
        for c in range(nlc):
            z = src[rr, lc(c)].astype(F32) - mean
            acc = acc + z * z
        rstd = lax.rsqrt(jnp.sum(acc, axis=1, keepdims=True) / D + EPS)
        for c in range(nlc):
            z = (src[rr, lc(c)].astype(F32) - mean) * rstd
            if dst is not None:
                dst[rr, lc(c)] = (z * vecs[gain, :, lc(c)] + vecs[shift, :, lc(c)]).astype(BF)
            else:
                xh1[:, lc(c)] = z
        return rstd

    ln_block(own, 32, xg, 0, 1, h)
    lb.wait()
    for k in range(3):
        bt = bqkv[k].T
        for hd in range(n_heads):
            at = (hd * 3 + k) * head
            bias[at:at + head, :] = jnp.broadcast_to(bt[:head, hd:hd + 1], (head, seq))
    x_to_sib.wait_recv()
    ln_block(rows(sib), 32, xg, 0, 1, h)
    x_fwd = []
    for k in range(2):
        x_to_cross[k].wait_recv()
        x_fwd.append(remote(xg.at[piece(cross, k), :], xg.at[piece(cross, k), :], sib))
    gy_to_cross = remote(gyg.at[own, :], gyg.at[own, :], cross)
    lwqkv.wait()
    lwout.wait()
    ln_block(rows(cross), 32, xg, 0, 1, h)
    for k in range(2):
        x_fwd[k].wait_recv()
    ln_block(rows(sibcross), 32, xg, 0, 1, h)

    hr = 2 * 3 * head
    hv = h[...]
    for m in range(n_heads // 2):
        mm = slice(m * hr, (m + 1) * hr)
        qkv[mm, :] = (dot_t(wqkv[mm, :], hv) + bias[mm, :]).astype(BF)

    def position(axis):
        i = lax.broadcasted_iota(jnp.int32, (seq, seq), axis)
        b = i >> 5
        return ((((b & 1) << 1) | (((b >> 1) ^ b) & 1)) << 5) | (i & 31)

    pos_k = position(0)
    causal = pos_k <= position(1)
    key_f = pos_k.astype(F32)
    slopes = alibi_slopes(n_heads * TP)
    score_scale = head ** -0.5

    def part_of(hd, k):
        at = (hd * 3 + k) * head
        return slice(at, at + head)

    def slope(hd):
        v = jnp.float32(slopes[hd])
        for dev in range(1, TP):
            v = jnp.where(t == dev, jnp.float32(slopes[dev * n_heads + hd]), v)
        return v

    for hd in range(n_heads):
        prob[hd] = dot(qkv[part_of(hd, 1), :].T, qkv[part_of(hd, 0), :])
    for hd in range(n_heads):
        s = jnp.where(causal, prob[hd] * score_scale + slope(hd) * key_f, MASK_VALUE)
        e = jnp.exp(s - jnp.max(s, axis=0, keepdims=True))
        pr = e * (1.0 / jnp.sum(e, axis=0, keepdims=True))
        prob[hd] = pr
        probb[hd] = pr.astype(BF)
    for hd in range(n_heads):
        ctx[hd * head:(hd + 1) * head, :] = dot(qkv[part_of(hd, 2), :], probb[hd]).astype(BF)

    class AllSum:
        widths = ALL_CHUNKS

        def __init__(self, p, rd, s, rs, tt, q, e):
            self.p, self.rd, self.s, self.rs, self.tt, self.q, self.e = p, rd, s, rs, tt, q, e
            self.a, self.b, self.c = {}, {}, {}
            self.last = len(self.widths) - 1

        def ch(self, j):
            return cols(self.widths, j)

        def fill(self, j, value):
            self.p[:, self.ch(j)] = value

        def put(self, j):
            self.a[j] = remote(self.p.at[sibhalf, self.ch(j)], self.rd.at[:, self.ch(j)], sib)

        def pair(self, j):
            self.a[j].wait_recv()
            c = self.ch(j)
            self.s[:, c] = (self.p[half, c].astype(F32) + self.rd[:, c].astype(F32)).astype(BF)

        def step_cross(self, j):
            self.pair(j)
            c = self.ch(j)
            self.b[j] = remote(self.s.at[:, c], self.rs.at[:, c], cross)
            if j == self.last:
                self.c[j] = (remote(self.s.at[:, c], self.e.at[:, :], sibcross), remote(self.s.at[:, c], self.q.at[:, :], sib))

        def step_back(self, j):
            self.b[j].wait_recv()
            c = self.ch(j)
            self.tt[half, c] = (self.s[:, c].astype(F32) + self.rs[:, c].astype(F32)).astype(BF)
            if j < self.last:
                self.c[j] = remote(self.tt.at[half, c], self.tt.at[half, c], sib)

        def finish(self, j):
            if j < self.last:
                self.c[j].wait_recv()
            else:
                for copy in self.c[j]:
                    copy.wait_recv()
                self.tt[sibhalf, self.ch(j)] = (self.q[...].astype(F32) + self.e[...].astype(F32)).astype(BF)

    class ScatterSum(AllSum):
        widths = SCATTER_CHUNKS

        def step_cross(self, j):
            self.pair(j)
            c = self.ch(j)
            self.b[j] = remote(self.s.at[blk_cross, c], self.rs.at[:, c], cross)

        def result(self, c):
            return (self.s[blk_own, c].astype(F32) + self.rs[:, c].astype(F32)).astype(BF).astype(F32)

    o_flat = ctx[...].T
    sum_a = AllSum(p1, rd1, s1, rs1, t1, q1, e1)
    n_all = len(ALL_CHUNKS)
    sum_a.fill(0, dot(o_flat, wout[:, sum_a.ch(0)]).astype(BF))
    sum_a.put(0)
    for j in range(1, n_all):
        sum_a.fill(j, dot(o_flat, wout[:, sum_a.ch(j)]).astype(BF))
    for j in range(1, n_all):
        sum_a.put(j)
    for j in range(n_all):
        sum_a.step_cross(j)

    gy_to_sib.wait_recv()
    gy_to_cross.wait_recv()
    gy_fwd = remote(gyg.at[rows(cross), :], gyg.at[rows(cross), :], sib)
    for hd in range(n_heads):
        vt[hd] = qkv[part_of(hd, 2), :].T
    gy_fwd.wait_recv()
    lwdn.wait()
    lwup.wait()
    fw = wdn_h.shape[0] // N_BLK
    shift = None
    acc1 = jnp.zeros((seq, LANES), F32)
    acc2 = jnp.zeros((seq, LANES), F32)

    def x1_chunk(j, shift, acc1, acc2):
        sum_a.finish(j)
        total = jnp.zeros((seq, LANES), F32)
        for c in groups(ALL_CHUNKS, j):
            z = xg[:, lc(c)].astype(F32) + t1[:, lc(c)].astype(F32) + vecs[4, :, lc(c)]
            x1[:, lc(c)] = z
            if j == 0:
                total = total + z
            else:
                d = z - shift
                acc1 = acc1 + d
                acc2 = acc2 + d * d
        if j == 0:
            shift = jnp.sum(total, axis=1, keepdims=True) / (ALL_CHUNKS[0] * LANES)
            for c in groups(ALL_CHUNKS, j):
                d = x1[:, lc(c)] - shift
                acc1 = acc1 + d
                acc2 = acc2 + d * d
        return shift, acc1, acc2

    gyv = gyg[...]
    for j in range(n_all):
        if j < N_BLK:
            ff = slice(j * fw, (j + 1) * fw)
            gact[:, ff] = dot_t(gyv, wdn[ff, :]).astype(BF)
        sum_a.step_back(j)
        if j:
            shift, acc1, acc2 = x1_chunk(j - 1, shift, acc1, acc2)
    shift, acc1, acc2 = x1_chunk(n_all - 1, shift, acc1, acc2)

    off = jnp.sum(acc1, axis=1, keepdims=True) / D
    mean = shift + off
    rstd = lax.rsqrt(jnp.sum(acc2, axis=1, keepdims=True) / D - off * off + EPS)
    halves = (slice(0, seq // 2), slice(seq // 2, seq))
    rstd2 = [rstd[hh] for hh in halves]
    for n, hh in enumerate(halves):
        for c in range(nlc):
            z = (x1[hh, lc(c)] - mean[hh]) * rstd2[n]
            xhat[hh, lc(c)] = z
            g[hh, lc(c)] = (z * vecs[2, :, lc(c)] + vecs[3, :, lc(c)]).astype(BF)

    gv = g[...]
    for j in range(N_BLK):
        ff = slice(j * fw, (j + 1) * fw)
        pre = dot(gv, wup[:, ff]) + vecs[6, :, ff]
        w = (GELU_C * GELU_A) * (pre * pre)
        th = jnp.tanh(pre * (GELU_C + w))
        hp = 0.5 * pre
        r[:, ff] = (hp + hp * th).astype(BF)
        slope_g = (0.5 + 0.5 * th) + (hp * (1.0 - th * th)) * (GELU_C + 3.0 * w)
        gp = gact[:, ff].astype(F32) * slope_g
        vec[6, :, ff] = jnp.sum(gp, axis=0, keepdims=True)
        dpre[:, ff] = gp.astype(BF)

    dv = dpre[...]
    sum_g = AllSum(p2, rd2, s2, rs2, t2, q2, e2)
    for j in range(n_all):
        for c in [lc(c) for c in groups(ALL_CHUNKS, j)] if j == 0 else [sum_g.ch(j)]:
            p2[:, c] = dot_t(dv, wup[c, :]).astype(BF)
        sum_g.put(j)
        if j:
            sum_g.step_cross(j - 1)
    sum_g.step_cross(n_all - 1)

    acc1 = jnp.zeros((seq, LANES), F32)
    acc2 = jnp.zeros((seq, LANES), F32)

    def ln2_back_chunk(j, acc1, acc2):
        sum_g.finish(j)
        for c in groups(ALL_CHUNKS, j):
            dg = t2[:, lc(c)].astype(F32)
            z = xhat[:, lc(c)]
            dgz = dg * z
            vec[2, :, lc(c)] = jnp.sum(dgz, axis=0, keepdims=True)
            vec[3, :, lc(c)] = jnp.sum(dg, axis=0, keepdims=True)
            gain = vecs[2, :, lc(c)]
            dz = dg * gain
            acc1 = acc1 + dz
            acc2 = acc2 + dgz * gain
            for n, hh in enumerate(halves):
                ubuf[hh, lc(c)] = gyg[hh, lc(c)].astype(F32) + rstd2[n] * dz[hh]
        return acc1, acc2

    yw = D // N_BLK

    def down(j):
        yy = slice(j * yw, (j + 1) * yw)
        py[:, yy] = dot(r[...], wdn[:, yy]).astype(BF)
        for c in range(j * (yw // LANES), (j + 1) * (yw // LANES)):
            gt[lc(c), :] = g[:, lc(c)].T
            rt[lc(c), :] = r[:, lc(c)].T
            vec[5, :, lc(c)] = jnp.sum(gyg[:, lc(c)].astype(F32), axis=0, keepdims=True)
            for n, hh in enumerate(halves):
                xr[hh, lc(c)] = xhat[hh, lc(c)] * rstd2[n]

    def grad_down(m):
        mm = slice(m * GRAD_ROWS, (m + 1) * GRAD_ROWS)
        wdn[mm, :] = dot(rt[mm, :], gyg[...]).astype(BF)

    work = [(down, k) for k in range(N_BLK)] + [(grad_down, m) for m in range(wdn.shape[0] // GRAD_ROWS)]
    for j in range(n_all):
        for step, m in work[WORK_CUTS[j]:WORK_CUTS[j + 1]]:
            step(m)
        if j == 1:
            y_sib = remote(py.at[sibhalf, :], rdy, sib)
        sum_g.step_back(j)
        if j:
            acc1, acc2 = ln2_back_chunk(j - 1, acc1, acc2)
    y_sib.wait_recv()
    sy[...] = (py[half, :].astype(F32) + rdy[...].astype(F32)).astype(BF)
    y_cross = remote(sy.at[blk_cross, :], rsy, cross)
    acc1, acc2 = ln2_back_chunk(n_all - 1, acc1, acc2)

    for n, hh in enumerate(halves):
        mean1 = rstd2[n] * (jnp.sum(acc1[hh], axis=1, keepdims=True) / D)
        mean2 = jnp.sum(acc2[hh], axis=1, keepdims=True) / D
        for c in range(nlc):
            gm = ubuf[hh, lc(c)] - (mean1 + xr[hh, lc(c)] * mean2)
            gmid[hh, lc(c)] = gm
            ga[hh, lc(c)] = gm.astype(BF)

    gav = ga[...]
    hc = ctx.shape[0] // 2
    for k in range(2):
        dctx[k * hc:(k + 1) * hc, :] = dot_t(wout[k * hc:(k + 1) * hc, :], gav).astype(BF)

    def head_rows(hd):
        return slice(hd * head, (hd + 1) * head)

    for hd in range(n_heads):
        dpb[hd] = dot(vt[hd], dctx[head_rows(hd), :]).astype(BF)
    for hd in range(n_heads):
        dqkv[part_of(hd, 2), :] = dot_t(dctx[head_rows(hd), :], probb[hd]).astype(BF)
    for hd in range(n_heads):
        pr = prob[hd]
        dp = dpb[hd].astype(F32)
        dsb[hd] = (pr * (dp - jnp.sum(dp * pr, axis=0, keepdims=True))).astype(BF)
    for hd in range(n_heads):
        dqkv[part_of(hd, 0), :] = (dot(qkv[part_of(hd, 1), :], dsb[hd]) * score_scale).astype(BF)
        dqkv[part_of(hd, 1), :] = (dot_t(qkv[part_of(hd, 0), :], dsb[hd]) * score_scale).astype(BF)

    sum_h = ScatterSum(ph, rdh, sh, rsh, None, None, None)
    n_scat = len(SCATTER_CHUNKS)
    dq = dqkv[...].T
    for j in range(n_scat):
        for c in [lc(c) for c in groups(SCATTER_CHUNKS, j)] if j == 0 else [sum_h.ch(j)]:
            ph[:, c] = dot(dq, wqkv[:, c]).astype(BF)
        sum_h.put(j)
        if j:
            sum_h.step_cross(j - 1)
    sum_h.step_cross(n_scat - 1)

    rstd1 = ln_block(own, 32, xg, 0, 1, None)
    y_cross.wait_recv()
    for c in range(nlc):
        z = (sy[blk_own, lc(c)].astype(F32) + rsy[:, lc(c)].astype(F32)).astype(BF).astype(F32)
        ybuf[:, lc(c)] = (x1[own, lc(c)] + z + vecs[5, :, lc(c)]).astype(BF)
        vec[4, :, lc(c)] = jnp.sum(gmid[:, lc(c)], axis=0, keepdims=True)

    me = slot(t)
    acc1 = jnp.zeros((32, LANES), F32)
    acc2 = jnp.zeros((32, LANES), F32)
    parts = []
    for step, m in work[WORK_CUTS[-1]:]:
        step(m)
    for j in range(n_scat):
        sum_h.b[j].wait_recv()
        for c in groups(SCATTER_CHUNKS, j):
            dh = sum_h.result(lc(c))
            z = xh1[:, lc(c)]
            dhz = dh * z
            part_o[me, 0:1, lc(c)] = jnp.sum(dhz, axis=0, keepdims=True)
            part_o[me, 1:2, lc(c)] = jnp.sum(dh, axis=0, keepdims=True)
            gain = vecs[0, :, lc(c)]
            acc1 = acc1 + dh * gain
            acc2 = acc2 + dhz * gain
        if j >= n_scat - 2:
            c = slice(0, sum_h.ch(j).stop) if j == n_scat - 2 else sum_h.ch(j)
            parts += [remote(part_o.at[me, :, c], part_o.at[me, :, c], dev) for dev in (cross, sibcross, sib)]
    mean1 = jnp.sum(acc1, axis=1, keepdims=True) / D
    mean2 = jnp.sum(acc2, axis=1, keepdims=True) / D
    for c in range(nlc):
        dz = sum_h.result(lc(c)) * vecs[0, :, lc(c)]
        gxbuf[:, lc(c)] = (gmid[own, lc(c)] + rstd1 * (dz - mean1 - xh1[:, lc(c)] * mean2)).astype(BF)
    for copy in sent:
        copy.wait_send()
    for copy in parts:
        copy.wait_recv()


def grad_kernel(h, ga, dpre, dqkv, ctx, gt, dwdn, vec, part, y, gx,
                dwqkv_o, dwout_o, dwup_o, dwdn_o, dbqkv_o, y_o, gx_o, v0, v1, v2, v3, v4, v5, v6,
                buf, small, sums, bq, osem, ssem):
    n_heads, head = dbqkv_o.shape[1], dbqkv_o.shape[2]
    slots, block = buf.shape[0], buf.shape[1]
    tail = []

    def piece(k, start, size):
        small[k, pl.ds(0, size), :] = dot(ctx[start:start + size, :], ga[...]).astype(BF)
        copy = pltpu.make_async_copy(small.at[k, pl.ds(0, size), :], dwout_o.at[pl.ds(start, size), :], ssem.at[k])
        copy.start()
        tail.append(copy)

    def written(slot, out):
        return pltpu.make_async_copy(buf.at[slot], out.at[pl.ds(0, block), :], osem.at[slot])

    for k in range(4):
        n = dwdn.shape[0] // 4
        copy = pltpu.make_async_copy(dwdn.at[pl.ds(k * n, n), :], dwdn_o.at[pl.ds(k * n, n), :], ssem.at[14 + k])
        copy.start()
        tail.append(copy)
    piece(0, 0, 160)
    for k in range(2):
        sums[k] = (part[0, k:k + 1, :] + part[1, k:k + 1, :]) + (part[2, k:k + 1, :] + part[3, k:k + 1, :])

    def send(src, dst):
        copy = pltpu.make_async_copy(src, dst, ssem.at[len(tail) - 2])
        copy.start()
        tail.append(copy)

    send(y, y_o)
    send(gx, gx_o)
    for k, o in enumerate((v2, v3, v4, v5, v6)):
        send(vec.at[k + 2, 0], o)
    for k, o in enumerate((v0, v1)):
        send(sums.at[k, 0], o)
    first = 0
    for left, right, out in ((gt, dpre, dwup_o), (dqkv, h, dwqkv_o)):

        def body(m, carry, left=left, right=right, out=out, first=first):
            slot = lax.rem(first + m, slots)

            @pl.when(first + m >= slots)
            def _():
                written(slot, out).wait()

            at = pl.ds(pl.multiple_of(m * block, block), block)
            buf[slot] = dot(left[at, :], right[...]).astype(BF)
            pltpu.make_async_copy(buf.at[slot], out.at[at, :], osem.at[slot]).start()
            return carry

        count = left.shape[0] // block
        lax.fori_loop(0, count, body, 0)
        first += count
    piece(1, 160, 320)
    ones = jnp.ones((8, dqkv.shape[1]), BF)
    total = dot_t(ones, dqkv[...])[0:1]
    for k in range(3):
        for hd in range(n_heads):
            at = (hd * 3 + k) * head
            bq[k, hd:hd + 1, :] = total[:, at:at + head]
    send(bq, dbqkv_o)
    piece(2, 480, 160)
    for k in range(slots):
        written(k, dwqkv_o).wait()
    for copy in tail:
        copy.wait()


def solution(mesh):
    def local_step(x, ln1_gamma, ln1_beta, w_qkv, b_qkv, w_out, b_out, ln2_gamma, ln2_beta, w_up, b_up, w_down, b_down, grad_y):
        D = x.shape[2]
        S = TP * x.shape[1]
        nh, head = w_qkv.shape[1], w_qkv.shape[3]
        Q = nh * 3 * head
        C = nh * head
        FL = w_up.shape[1]
        any_spec = pl.BlockSpec(memory_space=pl.ANY)
        vspec = pl.BlockSpec(memory_space=pltpu.VMEM)
        vm = pltpu.VMEM
        wqkv_t = jnp.transpose(w_qkv, (1, 2, 3, 0)).reshape(Q, D)
        bq = jnp.transpose(b_qkv, (1, 0, 2))
        sds = jax.ShapeDtypeStruct
        n_loads = 2 + 7 + 1 + 4
        red = [vm((S, D), BF), vm((S // 2, D), BF), vm((S // 2, D), BF), vm((S // 2, D), BF), vm((S, D), BF),
               vm((S // 2, ALL_CHUNKS[-1] * LANES), BF), vm((S // 2, ALL_CHUNKS[-1] * LANES), BF)]
        scat = [vm((S, D), BF), vm((S // 2, D), BF), vm((S // 2, D), BF), vm((S // TP, D), BF)]
        row = lambda v: v
        res = pl.pallas_call(
            layer_kernel,
            name='layer',
            out_shape=[vm((S // TP, D), BF), vm((S // TP, D), BF), vm((7, 1, D), F32), vm((TP, 2, D), F32), vm((S, D), BF), vm((S, D), BF),
                       vm((S, FL), BF), vm((Q, S), BF), vm((C, S), BF), vm((D, S), BF), vm((FL, D), BF)],
            in_specs=[any_spec] * 14,
            out_specs=[vspec] * 11,
            scratch_shapes=[
                vm((Q, D), BF), vm((C, D), BF), vm((D, FL), BF), vm((FL, S), BF), vm((3, nh, head), F32), vm((7, 1, D), F32),
                vm((S, D), BF), vm((S, D), BF), vm((Q, S), F32), vm((Q, S), BF), vm((nh, S, S), F32),
                vm((nh, S, S), BF), vm((S, D), F32), vm((S, D), F32), vm((S, D), BF),
                vm((S, FL), BF), vm((S, FL), BF), vm((S, D), F32), vm((C, S), BF),
                vm((S // TP, D), F32), vm((S, D), F32), vm((S, D), F32),
                vm((nh, S, head), BF), vm((nh, S, S), BF), vm((nh, S, S), BF),
                *red, *red, *scat, *scat,
                pltpu.SemaphoreType.DMA((n_loads,)),
                pltpu.SemaphoreType.DMA((N_REMOTE,)), pltpu.SemaphoreType.DMA((N_REMOTE,)),
            ],
            compiler_params=pltpu.CompilerParams(collective_id=0, has_side_effects=True, vmem_limit_bytes=LAYER_VMEM),
        )(x.reshape(x.shape[1], D), grad_y.reshape(x.shape[1], D), wqkv_t, bq, w_out, w_up, w_down, row(ln1_gamma), row(ln1_beta),
          row(ln2_gamma), row(ln2_beta), row(b_out), row(b_down), row(b_up))
        y, gx, vec, part, h, ga, dpre, dqkv, ctx, gt, dwdn = res
        vshape = sds((D,), F32)
        outs = pl.pallas_call(
            grad_kernel,
            name='weight_grads',
            out_shape=[sds((Q, D), BF), sds((C, D), BF), sds((D, FL), BF), sds((FL, D), BF), sds((3, nh, head), F32),
                       sds((S // TP, D), BF), sds((S // TP, D), BF)] + [vshape] * 7,
            in_specs=[vspec] * 11,
            out_specs=[any_spec] * 14,
            scratch_shapes=[
                vm((3, 640, D), BF), vm((3, 320, D), BF), vm((2, 1, D), F32), vm((3, nh, head), F32),
                pltpu.SemaphoreType.DMA((3,)), pltpu.SemaphoreType.DMA((18,)),
            ],
            compiler_params=pltpu.CompilerParams(vmem_limit_bytes=GRAD_VMEM),
        )(h, ga, dpre, dqkv, ctx, gt, dwdn, vec, part, y, gx)
        dwqkv, dwout, dwup, dwdn, dbqkv, y, gx, g_ln1g, g_ln1b, g_ln2g, g_ln2b, g_bout, g_bdown, g_bup = outs
        dwqkv = jnp.transpose(dwqkv.reshape(nh, 3, head, D), (3, 0, 1, 2))
        dbqkv = jnp.transpose(dbqkv, (1, 0, 2))
        return (y.reshape(x.shape), gx.reshape(x.shape), g_ln1g, g_ln1b, dwqkv, dbqkv, dwout, g_bout,
                g_ln2g, g_ln2b, dwup, g_bup, dwdn, g_bdown)

    row_spec = P('dp', 'tp', None)
    in_specs = (row_spec, P(), P(), P(None, 'tp', None, None), P('tp', None, None), P('tp', None), P(), P(), P(),
                P(None, 'tp'), P('tp'), P('tp', None), P(), row_spec)
    out_specs = (row_spec, row_spec, P('dp'), P('dp'), P('dp', 'tp', None, None), P(('dp', 'tp'), None, None),
                 P(('dp', 'tp'), None), P('dp'), P('dp'), P('dp'), P('dp', 'tp'), P(('dp', 'tp')), P(('dp', 'tp'), None), P('dp'))
    return jax.shard_map(local_step, mesh=mesh, in_specs=in_specs, out_specs=out_specs, check_vma=False)
```

```python
import functools
import math
import jax
import jax.numpy as jnp
from jax import lax
from jax.experimental import pallas as pl
from jax.experimental.pallas import tpu as pltpu
from jax.sharding import PartitionSpec as P

EPS = 1e-5
MASK_VALUE = -1e30
BF = jnp.bfloat16
F32 = jnp.float32
MESH = pl.DeviceIdType.MESH
GELU_C = math.sqrt(2.0 / math.pi)
GELU_A = 0.044715
TP = 4
LANES = 128
ALL_CHUNKS = (2, 4, 4, 5, 4, 1)
SCATTER_CHUNKS = (2, 6, 8, 4)
N_BLK = 5
GRAD_ROWS = 640
WORK_CUTS = (0, 3, 5, 6, 7, 7, 7)
LAYER_VMEM = 47 * 1024 * 1024
GRAD_VMEM = 24 * 1024 * 1024
N_REMOTE = 62
N_SEND = 42


def alibi_slopes(n_heads):
    closest = 2 ** int(math.floor(math.log2(n_heads)))
    base_ratio = 2.0 ** (-8.0 / closest)
    extra_ratio = 2.0 ** (-4.0 / closest)
    remaining = min(closest, n_heads - closest)
    slopes = [base_ratio ** (i + 1) for i in range(closest)]
    return slopes + [extra_ratio ** (2 * i + 1) for i in range(remaining)]


def dot(lhs, rhs):
    return lax.dot_general(lhs, rhs, (((1,), (0,)), ((), ())), preferred_element_type=F32)


def dot_t(lhs, rhs):
    return lax.dot_general(lhs, rhs, (((1,), (1,)), ((), ())), preferred_element_type=F32)


def layer_kernel(x_h, gy_h, wqkv_h, bqkv_h, wout_h, wup_h, wdn_h, ln1g_h, ln1b_h, ln2g_h, ln2b_h, bout_h, bdown_h, bup_h,
                 ybuf, gxbuf, vec, part_o, h, ga, dpre, dqkv, ctx, gt, wdn,
                 wqkv, wout, wup, rt, bqkv, vecs, xg, gyg, bias, qkv, prob, probb, x1, xhat, g, gact, r,
                 gmid, dctx, xh1, ubuf, xr, vt, dpb, dsb,
                 p1, rd1, s1, rs1, t1, q1, e1, p2, rd2, s2, rs2, t2, q2, e2, py, rdy, sy, rsy, ph, rdh, sh, rsh,
                 lsem, ssem, rsem):
    D = x_h.shape[1]
    seq = TP * 32
    head = bqkv_h.shape[2]
    n_heads = bqkv_h.shape[1]
    nlc = D // LANES
    t = lax.axis_index('tp')
    core = lax.rem(t, 2)
    chip = t // 2
    sib = t + 1 - 2 * core
    cross = lax.rem(sib + 2, TP)
    sibcross = lax.rem(t + 2, TP)
    side = lax.rem(core + chip, 2)

    def slot(dev):
        return lax.rem(lax.rem(dev, 2) + dev // 2, 2) * 2 + dev // 2

    def rows(dev):
        return pl.ds(pl.multiple_of(slot(dev) * 32, 32), 32)

    own = rows(t)
    half = pl.ds(pl.multiple_of(side * 64, 64), 64)
    sibhalf = pl.ds(pl.multiple_of((1 - side) * 64, 64), 64)
    blk_own = pl.ds(pl.multiple_of(chip * 32, 32), 32)
    blk_cross = pl.ds(pl.multiple_of((1 - chip) * 32, 32), 32)

    counter = [0, 0]

    def load(src, dst):
        k = counter[0]
        counter[0] += 1
        copy = pltpu.make_async_copy(src, dst, lsem.at[k])
        copy.start()
        return copy

    sent = []
    free = list(range(N_SEND))

    def remote(src, dst, dev):
        k = counter[1]
        counter[1] += 1
        at = free.pop(0)
        copy = pltpu.make_async_remote_copy(src_ref=src, dst_ref=dst, send_sem=ssem.at[at], recv_sem=rsem.at[k],
                                            device_id={'tp': dev}, device_id_type=MESH)
        copy.start()
        sent.append((copy, at))
        return copy

    def sends_done(n):
        for copy, at in sent[:n]:
            copy.wait_send()
            free.append(at)
        del sent[:n]

    def lc(c):
        return slice(c * LANES, (c + 1) * LANES)

    def groups(widths, j):
        start = sum(widths[:j])
        return range(start, start + widths[j])

    def cols(widths, j):
        return slice(sum(widths[:j]) * LANES, sum(widths[:j + 1]) * LANES)

    lx = load(x_h, xg.at[own, :])
    lg = load(gy_h, gyg.at[own, :])
    lvec = [load(src, vecs.at[k, 0]) for k, src in enumerate((ln1g_h, ln1b_h, ln2g_h, ln2b_h, bout_h, bdown_h, bup_h))]
    lb = load(bqkv_h, bqkv)
    lwqkv = load(wqkv_h, wqkv)
    lwout = load(wout_h, wout)
    barrier = pltpu.get_barrier_semaphore()
    for dev in (sib, cross, sibcross):
        pl.semaphore_signal(barrier, inc=1, device_id={'tp': dev}, device_id_type=MESH)
    pl.semaphore_wait(barrier, 3)
    lx.wait()
    def piece(dev, k):
        return pl.ds(pl.multiple_of(slot(dev) * 32 + 16 * k, 16), 16)

    x_to_cross = [remote(xg.at[piece(t, k), :], xg.at[piece(t, k), :], cross) for k in range(2)]
    x_to_sib = remote(xg.at[own, :], xg.at[own, :], sib)
    lg.wait()
    gy_to_sib = remote(gyg.at[own, :], gyg.at[own, :], sib)
    lwdn = load(wdn_h, wdn)
    lwup = load(wup_h, wup)
    for copy in lvec:
        copy.wait()

    def ln_block(rr, n, src, gain, shift, dst):
        acc = jnp.zeros((n, LANES), F32)
        for c in range(nlc):
            acc = acc + src[rr, lc(c)].astype(F32)
        mean = jnp.sum(acc, axis=1, keepdims=True) / D
        acc = jnp.zeros((n, LANES), F32)
        for c in range(nlc):
            z = src[rr, lc(c)].astype(F32) - mean
            acc = acc + z * z
        rstd = lax.rsqrt(jnp.sum(acc, axis=1, keepdims=True) / D + EPS)
        for c in range(nlc):
            z = (src[rr, lc(c)].astype(F32) - mean) * rstd
            if dst is not None:
                dst[rr, lc(c)] = (z * vecs[gain, :, lc(c)] + vecs[shift, :, lc(c)]).astype(BF)
            else:
                xh1[:, lc(c)] = z
        return rstd

    ln_block(own, 32, xg, 0, 1, h)
    lb.wait()
    for k in range(3):
        bt = bqkv[k].T
        for hd in range(n_heads):
            at = (hd * 3 + k) * head
            bias[at:at + head, :] = jnp.broadcast_to(bt[:head, hd:hd + 1], (head, seq))
    x_to_sib.wait_recv()
    ln_block(rows(sib), 32, xg, 0, 1, h)
    x_fwd = []
    for k in range(2):
        x_to_cross[k].wait_recv()
        x_fwd.append(remote(xg.at[piece(cross, k), :], xg.at[piece(cross, k), :], sib))
    gy_to_cross = remote(gyg.at[own, :], gyg.at[own, :], cross)
    lwqkv.wait()
    lwout.wait()
    ln_block(rows(cross), 32, xg, 0, 1, h)
    for k in range(2):
        x_fwd[k].wait_recv()
    ln_block(rows(sibcross), 32, xg, 0, 1, h)

    hr = 2 * 3 * head
    hv = h[...]
    for m in range(n_heads // 2):
        mm = slice(m * hr, (m + 1) * hr)
        qkv[mm, :] = (dot_t(wqkv[mm, :], hv) + bias[mm, :]).astype(BF)

    def position(axis):
        i = lax.broadcasted_iota(jnp.int32, (seq, seq), axis)
        b = i >> 5
        return ((((b & 1) << 1) | (((b >> 1) ^ b) & 1)) << 5) | (i & 31)

    pos_k = position(0)
    causal = pos_k <= position(1)
    key_f = pos_k.astype(F32)
    slopes = alibi_slopes(n_heads * TP)
    score_scale = head ** -0.5

    def part_of(hd, k):
        at = (hd * 3 + k) * head
        return slice(at, at + head)

    def slope(hd):
        v = jnp.float32(slopes[hd])
        for dev in range(1, TP):
            v = jnp.where(t == dev, jnp.float32(slopes[dev * n_heads + hd]), v)
        return v

    for hd in range(n_heads):
        prob[hd] = dot(qkv[part_of(hd, 1), :].T, qkv[part_of(hd, 0), :])
    for hd in range(n_heads):
        s = jnp.where(causal, prob[hd] * score_scale + slope(hd) * key_f, MASK_VALUE)
        e = jnp.exp(s - jnp.max(s, axis=0, keepdims=True))
        pr = e * (1.0 / jnp.sum(e, axis=0, keepdims=True))
        prob[hd] = pr
        probb[hd] = pr.astype(BF)
    for hd in range(n_heads):
        ctx[hd * head:(hd + 1) * head, :] = dot(qkv[part_of(hd, 2), :], probb[hd]).astype(BF)

    class AllSum:
        widths = ALL_CHUNKS

        def __init__(self, p, rd, s, rs, tt, q, e):
            self.p, self.rd, self.s, self.rs, self.tt, self.q, self.e = p, rd, s, rs, tt, q, e
            self.a, self.b, self.c = {}, {}, {}
            self.last = len(self.widths) - 1

        def ch(self, j):
            return cols(self.widths, j)

        def fill(self, j, value):
            self.p[:, self.ch(j)] = value

        def put(self, j):
            self.a[j] = remote(self.p.at[sibhalf, self.ch(j)], self.rd.at[:, self.ch(j)], sib)

        def pair(self, j):
            self.a[j].wait_recv()
            c = self.ch(j)
            self.s[:, c] = (self.p[half, c].astype(F32) + self.rd[:, c].astype(F32)).astype(BF)

        def step_cross(self, j):
            self.pair(j)
            c = self.ch(j)
            self.b[j] = remote(self.s.at[:, c], self.rs.at[:, c], cross)
            if j == self.last:
                self.c[j] = (remote(self.s.at[:, c], self.e.at[:, :], sibcross), remote(self.s.at[:, c], self.q.at[:, :], sib))

        def step_back(self, j):
            self.b[j].wait_recv()
            c = self.ch(j)
            self.tt[half, c] = (self.s[:, c].astype(F32) + self.rs[:, c].astype(F32)).astype(BF)
            if j < self.last:
                self.c[j] = remote(self.tt.at[half, c], self.tt.at[half, c], sib)

        def finish(self, j):
            if j < self.last:
                self.c[j].wait_recv()
            else:
                for copy in self.c[j]:
                    copy.wait_recv()
                self.tt[sibhalf, self.ch(j)] = (self.q[...].astype(F32) + self.e[...].astype(F32)).astype(BF)

    class ScatterSum(AllSum):
        widths = SCATTER_CHUNKS

        def step_cross(self, j):
            self.pair(j)
            c = self.ch(j)
            self.b[j] = remote(self.s.at[blk_cross, c], self.rs.at[:, c], cross)

        def result(self, c):
            return (self.s[blk_own, c].astype(F32) + self.rs[:, c].astype(F32)).astype(BF).astype(F32)

    o_flat = ctx[...].T
    sum_a = AllSum(p1, rd1, s1, rs1, t1, q1, e1)
    n_all = len(ALL_CHUNKS)
    sum_a.fill(0, dot(o_flat, wout[:, sum_a.ch(0)]).astype(BF))
    sum_a.put(0)
    for j in range(1, n_all):
        sum_a.fill(j, dot(o_flat, wout[:, sum_a.ch(j)]).astype(BF))
    for j in range(1, n_all):
        sum_a.put(j)
    for j in range(n_all):
        sum_a.step_cross(j)

    gy_to_sib.wait_recv()
    gy_to_cross.wait_recv()
    gy_fwd = remote(gyg.at[rows(cross), :], gyg.at[rows(cross), :], sib)
    for hd in range(n_heads):
        vt[hd] = qkv[part_of(hd, 2), :].T
    gy_fwd.wait_recv()
    lwdn.wait()
    lwup.wait()
    fw = wdn_h.shape[0] // N_BLK
    shift = None
    acc1 = jnp.zeros((seq, LANES), F32)
    acc2 = jnp.zeros((seq, LANES), F32)

    def x1_chunk(j, shift, acc1, acc2):
        sum_a.finish(j)
        total = jnp.zeros((seq, LANES), F32)
        for c in groups(ALL_CHUNKS, j):
            z = xg[:, lc(c)].astype(F32) + t1[:, lc(c)].astype(F32) + vecs[4, :, lc(c)]
            x1[:, lc(c)] = z
            if j == 0:
                total = total + z
            else:
                d = z - shift
                acc1 = acc1 + d
                acc2 = acc2 + d * d
        if j == 0:
            shift = jnp.sum(total, axis=1, keepdims=True) / (ALL_CHUNKS[0] * LANES)
            for c in groups(ALL_CHUNKS, j):
                d = x1[:, lc(c)] - shift
                acc1 = acc1 + d
                acc2 = acc2 + d * d
        return shift, acc1, acc2

    gyv = gyg[...]
    for j in range(n_all):
        if j < N_BLK:
            ff = slice(j * fw, (j + 1) * fw)
            gact[:, ff] = dot_t(gyv, wdn[ff, :]).astype(BF)
        sum_a.step_back(j)
        if j:
            shift, acc1, acc2 = x1_chunk(j - 1, shift, acc1, acc2)
    shift, acc1, acc2 = x1_chunk(n_all - 1, shift, acc1, acc2)

    off = jnp.sum(acc1, axis=1, keepdims=True) / D
    mean = shift + off
    rstd = lax.rsqrt(jnp.sum(acc2, axis=1, keepdims=True) / D - off * off + EPS)
    halves = (slice(0, seq // 2), slice(seq // 2, seq))
    rstd2 = [rstd[hh] for hh in halves]
    for n, hh in enumerate(halves):
        for c in range(nlc):
            z = (x1[hh, lc(c)] - mean[hh]) * rstd2[n]
            xhat[hh, lc(c)] = z
            g[hh, lc(c)] = (z * vecs[2, :, lc(c)] + vecs[3, :, lc(c)]).astype(BF)

    gv = g[...]
    for j in range(N_BLK):
        ff = slice(j * fw, (j + 1) * fw)
        pre = dot(gv, wup[:, ff]) + vecs[6, :, ff]
        w = (GELU_C * GELU_A) * (pre * pre)
        th = jnp.tanh(pre * (GELU_C + w))
        hp = 0.5 * pre
        r[:, ff] = (hp + hp * th).astype(BF)
        slope_g = (0.5 + 0.5 * th) + (hp * (1.0 - th * th)) * (GELU_C + 3.0 * w)
        gp = gact[:, ff].astype(F32) * slope_g
        vec[6, :, ff] = jnp.sum(gp, axis=0, keepdims=True)
        dpre[:, ff] = gp.astype(BF)

    dv = dpre[...]
    n_before = len(sent)
    sum_g = AllSum(p2, rd2, s2, rs2, t2, q2, e2)
    for j in range(n_all):
        for c in [lc(c) for c in groups(ALL_CHUNKS, j)] if j == 0 else [sum_g.ch(j)]:
            p2[:, c] = dot_t(dv, wup[c, :]).astype(BF)
        sum_g.put(j)
        if j:
            sum_g.step_cross(j - 1)
    sum_g.step_cross(n_all - 1)

    sends_done(n_before)
    acc1 = jnp.zeros((seq, LANES), F32)
    acc2 = jnp.zeros((seq, LANES), F32)

    def ln2_back_chunk(j, acc1, acc2):
        sum_g.finish(j)
        for c in groups(ALL_CHUNKS, j):
            dg = t2[:, lc(c)].astype(F32)
            z = xhat[:, lc(c)]
            dgz = dg * z
            vec[2, :, lc(c)] = jnp.sum(dgz, axis=0, keepdims=True)
            vec[3, :, lc(c)] = jnp.sum(dg, axis=0, keepdims=True)
            gain = vecs[2, :, lc(c)]
            dz = dg * gain
            acc1 = acc1 + dz
            acc2 = acc2 + dgz * gain
            for n, hh in enumerate(halves):
                ubuf[hh, lc(c)] = gyg[hh, lc(c)].astype(F32) + rstd2[n] * dz[hh]
        return acc1, acc2

    yw = D // N_BLK

    def down(j):
        yy = slice(j * yw, (j + 1) * yw)
        py[:, yy] = dot(r[...], wdn[:, yy]).astype(BF)
        for c in range(j * (yw // LANES), (j + 1) * (yw // LANES)):
            gt[lc(c), :] = g[:, lc(c)].T
            rt[lc(c), :] = r[:, lc(c)].T
            vec[5, :, lc(c)] = jnp.sum(gyg[:, lc(c)].astype(F32), axis=0, keepdims=True)
            for n, hh in enumerate(halves):
                xr[hh, lc(c)] = xhat[hh, lc(c)] * rstd2[n]

    def grad_down(m):
        mm = slice(m * GRAD_ROWS, (m + 1) * GRAD_ROWS)
        wdn[mm, :] = dot(rt[mm, :], gyg[...]).astype(BF)

    work = [(down, k) for k in range(N_BLK)] + [(grad_down, m) for m in range(wdn.shape[0] // GRAD_ROWS)]
    for j in range(n_all):
        for step, m in work[WORK_CUTS[j]:WORK_CUTS[j + 1]]:
            step(m)
        if j == 1:
            y_sib = remote(py.at[sibhalf, :], rdy, sib)
        sum_g.step_back(j)
        if j:
            acc1, acc2 = ln2_back_chunk(j - 1, acc1, acc2)
    y_sib.wait_recv()
    sy[...] = (py[half, :].astype(F32) + rdy[...].astype(F32)).astype(BF)
    y_cross = remote(sy.at[blk_cross, :], rsy, cross)
    acc1, acc2 = ln2_back_chunk(n_all - 1, acc1, acc2)

    for n, hh in enumerate(halves):
        mean1 = rstd2[n] * (jnp.sum(acc1[hh], axis=1, keepdims=True) / D)
        mean2 = jnp.sum(acc2[hh], axis=1, keepdims=True) / D
        for c in range(nlc):
            gm = ubuf[hh, lc(c)] - (mean1 + xr[hh, lc(c)] * mean2)
            gmid[hh, lc(c)] = gm
            ga[hh, lc(c)] = gm.astype(BF)

    gav = ga[...]
    hc = ctx.shape[0] // 2
    for k in range(2):
        dctx[k * hc:(k + 1) * hc, :] = dot_t(wout[k * hc:(k + 1) * hc, :], gav).astype(BF)

    def head_rows(hd):
        return slice(hd * head, (hd + 1) * head)

    for hd in range(n_heads):
        dpb[hd] = dot(vt[hd], dctx[head_rows(hd), :]).astype(BF)
    for hd in range(n_heads):
        dqkv[part_of(hd, 2), :] = dot_t(dctx[head_rows(hd), :], probb[hd]).astype(BF)
    for hd in range(n_heads):
        pr = prob[hd]
        dp = dpb[hd].astype(F32)
        dsb[hd] = (pr * (dp - jnp.sum(dp * pr, axis=0, keepdims=True))).astype(BF)
    for hd in range(n_heads):
        dqkv[part_of(hd, 0), :] = (dot(qkv[part_of(hd, 1), :], dsb[hd]) * score_scale).astype(BF)
        dqkv[part_of(hd, 1), :] = (dot_t(qkv[part_of(hd, 0), :], dsb[hd]) * score_scale).astype(BF)

    n_before = len(sent)
    sum_h = ScatterSum(ph, rdh, sh, rsh, None, None, None)
    n_scat = len(SCATTER_CHUNKS)
    dq = dqkv[...].T
    for j in range(n_scat):
        for c in [lc(c) for c in groups(SCATTER_CHUNKS, j)] if j == 0 else [sum_h.ch(j)]:
            ph[:, c] = dot(dq, wqkv[:, c]).astype(BF)
        sum_h.put(j)
        if j:
            sum_h.step_cross(j - 1)
    sum_h.step_cross(n_scat - 1)

    rstd1 = ln_block(own, 32, xg, 0, 1, None)
    y_cross.wait_recv()
    for c in range(nlc):
        z = (sy[blk_own, lc(c)].astype(F32) + rsy[:, lc(c)].astype(F32)).astype(BF).astype(F32)
        ybuf[:, lc(c)] = (x1[own, lc(c)] + z + vecs[5, :, lc(c)]).astype(BF)
        vec[4, :, lc(c)] = jnp.sum(gmid[:, lc(c)], axis=0, keepdims=True)

    me = slot(t)
    acc1 = jnp.zeros((32, LANES), F32)
    acc2 = jnp.zeros((32, LANES), F32)
    parts = []
    for step, m in work[WORK_CUTS[-1]:]:
        step(m)
    sends_done(n_before)
    for j in range(n_scat):
        sum_h.b[j].wait_recv()
        for c in groups(SCATTER_CHUNKS, j):
            dh = sum_h.result(lc(c))
            z = xh1[:, lc(c)]
            dhz = dh * z
            part_o[me, 0:1, lc(c)] = jnp.sum(dhz, axis=0, keepdims=True)
            part_o[me, 1:2, lc(c)] = jnp.sum(dh, axis=0, keepdims=True)
            gain = vecs[0, :, lc(c)]
            acc1 = acc1 + dh * gain
            acc2 = acc2 + dhz * gain
        if j >= n_scat - 2:
            c = slice(0, sum_h.ch(j).stop) if j == n_scat - 2 else sum_h.ch(j)
            parts += [remote(part_o.at[me, :, c], part_o.at[me, :, c], dev) for dev in (cross, sibcross, sib)]
    mean1 = jnp.sum(acc1, axis=1, keepdims=True) / D
    mean2 = jnp.sum(acc2, axis=1, keepdims=True) / D
    for c in range(nlc):
        dz = sum_h.result(lc(c)) * vecs[0, :, lc(c)]
        gxbuf[:, lc(c)] = (gmid[own, lc(c)] + rstd1 * (dz - mean1 - xh1[:, lc(c)] * mean2)).astype(BF)
    sends_done(len(sent))
    for copy in parts:
        copy.wait_recv()


def grad_kernel(h, ga, dpre, dqkv, ctx, gt, dwdn, vec, part, y, gx,
                dwqkv_o, dwout_o, dwup_o, dwdn_o, dbqkv_o, y_o, gx_o, v0, v1, v2, v3, v4, v5, v6,
                buf, small, sums, bq, osem, ssem):
    n_heads, head = dbqkv_o.shape[1], dbqkv_o.shape[2]
    slots, block = buf.shape[0], buf.shape[1]
    tail = []

    def piece(k, start, size):
        small[k, pl.ds(0, size), :] = dot(ctx[start:start + size, :], ga[...]).astype(BF)
        copy = pltpu.make_async_copy(small.at[k, pl.ds(0, size), :], dwout_o.at[pl.ds(start, size), :], ssem.at[k])
        copy.start()
        tail.append(copy)

    def written(slot, out):
        return pltpu.make_async_copy(buf.at[slot], out.at[pl.ds(0, block), :], osem.at[slot])

    for k in range(4):
        n = dwdn.shape[0] // 4
        copy = pltpu.make_async_copy(dwdn.at[pl.ds(k * n, n), :], dwdn_o.at[pl.ds(k * n, n), :], ssem.at[14 + k])
        copy.start()
        tail.append(copy)
    piece(0, 0, 160)
    for k in range(2):
        sums[k] = (part[0, k:k + 1, :] + part[1, k:k + 1, :]) + (part[2, k:k + 1, :] + part[3, k:k + 1, :])

    def send(src, dst):
        copy = pltpu.make_async_copy(src, dst, ssem.at[len(tail) - 2])
        copy.start()
        tail.append(copy)

    send(y, y_o)
    send(gx, gx_o)
    for k, o in enumerate((v2, v3, v4, v5, v6)):
        send(vec.at[k + 2, 0], o)
    for k, o in enumerate((v0, v1)):
        send(sums.at[k, 0], o)
    first = 0
    for left, right, out in ((gt, dpre, dwup_o), (dqkv, h, dwqkv_o)):

        def body(m, carry, left=left, right=right, out=out, first=first):
            slot = lax.rem(first + m, slots)

            @pl.when(first + m >= slots)
            def _():
                written(slot, out).wait()

            at = pl.ds(pl.multiple_of(m * block, block), block)
            buf[slot] = dot(left[at, :], right[...]).astype(BF)
            pltpu.make_async_copy(buf.at[slot], out.at[at, :], osem.at[slot]).start()
            return carry

        count = left.shape[0] // block
        lax.fori_loop(0, count, body, 0)
        first += count
    piece(1, 160, 320)
    ones = jnp.ones((8, dqkv.shape[1]), BF)
    total = dot_t(ones, dqkv[...])[0:1]
    for k in range(3):
        for hd in range(n_heads):
            at = (hd * 3 + k) * head
            bq[k, hd:hd + 1, :] = total[:, at:at + head]
    send(bq, dbqkv_o)
    piece(2, 480, 160)
    for k in range(slots):
        written(k, dwqkv_o).wait()
    for copy in tail:
        copy.wait()


def solution(mesh):
    def local_step(x, ln1_gamma, ln1_beta, w_qkv, b_qkv, w_out, b_out, ln2_gamma, ln2_beta, w_up, b_up, w_down, b_down, grad_y):
        D = x.shape[2]
        S = TP * x.shape[1]
        nh, head = w_qkv.shape[1], w_qkv.shape[3]
        Q = nh * 3 * head
        C = nh * head
        FL = w_up.shape[1]
        any_spec = pl.BlockSpec(memory_space=pl.ANY)
        vspec = pl.BlockSpec(memory_space=pltpu.VMEM)
        vm = pltpu.VMEM
        wqkv_t = jnp.transpose(w_qkv, (1, 2, 3, 0)).reshape(Q, D)
        bq = jnp.transpose(b_qkv, (1, 0, 2))
        sds = jax.ShapeDtypeStruct
        n_loads = 2 + 7 + 1 + 4
        red = [vm((S, D), BF), vm((S // 2, D), BF), vm((S // 2, D), BF), vm((S // 2, D), BF), vm((S, D), BF),
               vm((S // 2, ALL_CHUNKS[-1] * LANES), BF), vm((S // 2, ALL_CHUNKS[-1] * LANES), BF)]
        scat = [vm((S, D), BF), vm((S // 2, D), BF), vm((S // 2, D), BF), vm((S // TP, D), BF)]
        row = lambda v: v
        res = pl.pallas_call(
            layer_kernel,
            name='layer',
            out_shape=[vm((S // TP, D), BF), vm((S // TP, D), BF), vm((7, 1, D), F32), vm((TP, 2, D), F32), vm((S, D), BF), vm((S, D), BF),
                       vm((S, FL), BF), vm((Q, S), BF), vm((C, S), BF), vm((D, S), BF), vm((FL, D), BF)],
            in_specs=[any_spec] * 14,
            out_specs=[vspec] * 11,
            scratch_shapes=[
                vm((Q, D), BF), vm((C, D), BF), vm((D, FL), BF), vm((FL, S), BF), vm((3, nh, head), F32), vm((7, 1, D), F32),
                vm((S, D), BF), vm((S, D), BF), vm((Q, S), F32), vm((Q, S), BF), vm((nh, S, S), F32),
                vm((nh, S, S), BF), vm((S, D), F32), vm((S, D), F32), vm((S, D), BF),
                vm((S, FL), BF), vm((S, FL), BF), vm((S, D), F32), vm((C, S), BF),
                vm((S // TP, D), F32), vm((S, D), F32), vm((S, D), F32),
                vm((nh, S, head), BF), vm((nh, S, S), BF), vm((nh, S, S), BF),
                *red, *red, *scat, *scat,
                pltpu.SemaphoreType.DMA((n_loads,)),
                pltpu.SemaphoreType.DMA((N_SEND,)), pltpu.SemaphoreType.DMA((N_REMOTE,)),
            ],
            compiler_params=pltpu.CompilerParams(collective_id=0, has_side_effects=True, vmem_limit_bytes=LAYER_VMEM),
        )(x.reshape(x.shape[1], D), grad_y.reshape(x.shape[1], D), wqkv_t, bq, w_out, w_up, w_down, row(ln1_gamma), row(ln1_beta),
          row(ln2_gamma), row(ln2_beta), row(b_out), row(b_down), row(b_up))
        y, gx, vec, part, h, ga, dpre, dqkv, ctx, gt, dwdn = res
        vshape = sds((D,), F32)
        outs = pl.pallas_call(
            grad_kernel,
            name='weight_grads',
            out_shape=[sds((Q, D), BF), sds((C, D), BF), sds((D, FL), BF), sds((FL, D), BF), sds((3, nh, head), F32),
                       sds((S // TP, D), BF), sds((S // TP, D), BF)] + [vshape] * 7,
            in_specs=[vspec] * 11,
            out_specs=[any_spec] * 14,
            scratch_shapes=[
                vm((3, 640, D), BF), vm((3, 320, D), BF), vm((2, 1, D), F32), vm((3, nh, head), F32),
                pltpu.SemaphoreType.DMA((3,)), pltpu.SemaphoreType.DMA((18,)),
            ],
            compiler_params=pltpu.CompilerParams(vmem_limit_bytes=GRAD_VMEM),
        )(h, ga, dpre, dqkv, ctx, gt, dwdn, vec, part, y, gx)
        dwqkv, dwout, dwup, dwdn, dbqkv, y, gx, g_ln1g, g_ln1b, g_ln2g, g_ln2b, g_bout, g_bdown, g_bup = outs
        dwqkv = jnp.transpose(dwqkv.reshape(nh, 3, head, D), (3, 0, 1, 2))
        dbqkv = jnp.transpose(dbqkv, (1, 0, 2))
        return (y.reshape(x.shape), gx.reshape(x.shape), g_ln1g, g_ln1b, dwqkv, dbqkv, dwout, g_bout,
                g_ln2g, g_ln2b, dwup, g_bup, dwdn, g_bdown)

    row_spec = P('dp', 'tp', None)
    in_specs = (row_spec, P(), P(), P(None, 'tp', None, None), P('tp', None, None), P('tp', None), P(), P(), P(),
                P(None, 'tp'), P('tp'), P('tp', None), P(), row_spec)
    out_specs = (row_spec, row_spec, P('dp'), P('dp'), P('dp', 'tp', None, None), P(('dp', 'tp'), None, None),
                 P(('dp', 'tp'), None), P('dp'), P('dp'), P('dp'), P('dp', 'tp'), P(('dp', 'tp')), P(('dp', 'tp'), None), P('dp'))
    return jax.shard_map(local_step, mesh=mesh, in_specs=in_specs, out_specs=out_specs, check_vma=False)
```

```python
import functools
import math
import jax
import jax.numpy as jnp
from jax import lax
from jax.experimental import pallas as pl
from jax.experimental.pallas import tpu as pltpu
from jax.sharding import PartitionSpec as P

EPS = 1e-5
MASK_VALUE = -1e30
BF = jnp.bfloat16
F32 = jnp.float32
MESH = pl.DeviceIdType.MESH
GELU_C = math.sqrt(2.0 / math.pi)
GELU_A = 0.044715
TP = 4
LANES = 128
ALL_CHUNKS = (2, 4, 4, 5, 4, 1)
SCATTER_CHUNKS = (2, 8, 8, 2)
N_BLK = 5
GRAD_ROWS = 640
WORK_CUTS = (0, 3, 5, 6, 7, 7, 7)
LAYER_VMEM = 47 * 1024 * 1024
GRAD_VMEM = 24 * 1024 * 1024
N_REMOTE = 62
N_SEND = 42


def alibi_slopes(n_heads):
    closest = 2 ** int(math.floor(math.log2(n_heads)))
    base_ratio = 2.0 ** (-8.0 / closest)
    extra_ratio = 2.0 ** (-4.0 / closest)
    remaining = min(closest, n_heads - closest)
    slopes = [base_ratio ** (i + 1) for i in range(closest)]
    return slopes + [extra_ratio ** (2 * i + 1) for i in range(remaining)]


def dot(lhs, rhs):
    return lax.dot_general(lhs, rhs, (((1,), (0,)), ((), ())), preferred_element_type=F32)


def dot_t(lhs, rhs):
    return lax.dot_general(lhs, rhs, (((1,), (1,)), ((), ())), preferred_element_type=F32)


def layer_kernel(x_h, gy_h, wqkv_h, bqkv_h, wout_h, wup_h, wdn_h, ln1g_h, ln1b_h, ln2g_h, ln2b_h, bout_h, bdown_h, bup_h,
                 ybuf, gxbuf, vec, part_o, h, ga, dpre, dqkv, ctx, gt, wdn,
                 wqkv, wout, wup, rt, bqkv, vecs, xg, gyg, bias, qkv, prob, probb, x1, xhat, g, gact, r,
                 gmid, dctx, xh1, ubuf, xr, vt, dpb, dsb,
                 p1, rd1, s1, rs1, t1, q1, e1, p2, rd2, s2, rs2, t2, q2, e2, py, rdy, sy, rsy, ph, rdh, sh, rsh,
                 lsem, ssem, rsem):
    D = x_h.shape[1]
    seq = TP * 32
    head = bqkv_h.shape[2]
    n_heads = bqkv_h.shape[1]
    nlc = D // LANES
    t = lax.axis_index('tp')
    core = lax.rem(t, 2)
    chip = t // 2
    sib = t + 1 - 2 * core
    cross = lax.rem(sib + 2, TP)
    sibcross = lax.rem(t + 2, TP)
    side = lax.rem(core + chip, 2)

    def slot(dev):
        return lax.rem(lax.rem(dev, 2) + dev // 2, 2) * 2 + dev // 2

    def rows(dev):
        return pl.ds(pl.multiple_of(slot(dev) * 32, 32), 32)

    own = rows(t)
    half = pl.ds(pl.multiple_of(side * 64, 64), 64)
    sibhalf = pl.ds(pl.multiple_of((1 - side) * 64, 64), 64)
    blk_own = pl.ds(pl.multiple_of(chip * 32, 32), 32)
    blk_cross = pl.ds(pl.multiple_of((1 - chip) * 32, 32), 32)

    counter = [0, 0]

    def load(src, dst):
        k = counter[0]
        counter[0] += 1
        copy = pltpu.make_async_copy(src, dst, lsem.at[k])
        copy.start()
        return copy

    sent = []
    free = list(range(N_SEND))

    def remote(src, dst, dev):
        k = counter[1]
        counter[1] += 1
        at = free.pop(0)
        copy = pltpu.make_async_remote_copy(src_ref=src, dst_ref=dst, send_sem=ssem.at[at], recv_sem=rsem.at[k],
                                            device_id={'tp': dev}, device_id_type=MESH)
        copy.start()
        sent.append((copy, at))
        return copy

    def sends_done(n):
        for copy, at in sent[:n]:
            copy.wait_send()
            free.append(at)
        del sent[:n]

    def lc(c):
        return slice(c * LANES, (c + 1) * LANES)

    def groups(widths, j):
        start = sum(widths[:j])
        return range(start, start + widths[j])

    def cols(widths, j):
        return slice(sum(widths[:j]) * LANES, sum(widths[:j + 1]) * LANES)

    lx = load(x_h, xg.at[own, :])
    lg = load(gy_h, gyg.at[own, :])
    lvec = [load(src, vecs.at[k, 0]) for k, src in enumerate((ln1g_h, ln1b_h, ln2g_h, ln2b_h, bout_h, bdown_h, bup_h))]
    lb = load(bqkv_h, bqkv)
    lwqkv = load(wqkv_h, wqkv)
    lwout = load(wout_h, wout)
    barrier = pltpu.get_barrier_semaphore()
    for dev in (sib, cross, sibcross):
        pl.semaphore_signal(barrier, inc=1, device_id={'tp': dev}, device_id_type=MESH)
    pl.semaphore_wait(barrier, 3)
    lx.wait()
    def piece(dev, k):
        return pl.ds(pl.multiple_of(slot(dev) * 32 + 16 * k, 16), 16)

    x_to_cross = [remote(xg.at[piece(t, k), :], xg.at[piece(t, k), :], cross) for k in range(2)]
    x_to_sib = remote(xg.at[own, :], xg.at[own, :], sib)
    lg.wait()
    gy_to_sib = remote(gyg.at[own, :], gyg.at[own, :], sib)
    lwdn = load(wdn_h, wdn)
    lwup = load(wup_h, wup)
    for copy in lvec:
        copy.wait()

    def ln_block(rr, n, src, gain, shift, dst):
        acc = jnp.zeros((n, LANES), F32)
        for c in range(nlc):
            acc = acc + src[rr, lc(c)].astype(F32)
        mean = jnp.sum(acc, axis=1, keepdims=True) / D
        acc = jnp.zeros((n, LANES), F32)
        for c in range(nlc):
            z = src[rr, lc(c)].astype(F32) - mean
            acc = acc + z * z
        rstd = lax.rsqrt(jnp.sum(acc, axis=1, keepdims=True) / D + EPS)
        for c in range(nlc):
            z = (src[rr, lc(c)].astype(F32) - mean) * rstd
            if dst is not None:
                dst[rr, lc(c)] = (z * vecs[gain, :, lc(c)] + vecs[shift, :, lc(c)]).astype(BF)
            else:
                xh1[:, lc(c)] = z
        return rstd

    ln_block(own, 32, xg, 0, 1, h)
    lb.wait()
    for k in range(3):
        bt = bqkv[k].T
        for hd in range(n_heads):
            at = (hd * 3 + k) * head
            bias[at:at + head, :] = jnp.broadcast_to(bt[:head, hd:hd + 1], (head, seq))
    x_to_sib.wait_recv()
    ln_block(rows(sib), 32, xg, 0, 1, h)
    x_fwd = []
    for k in range(2):
        x_to_cross[k].wait_recv()
        x_fwd.append(remote(xg.at[piece(cross, k), :], xg.at[piece(cross, k), :], sib))
    gy_to_cross = remote(gyg.at[own, :], gyg.at[own, :], cross)
    lwqkv.wait()
    lwout.wait()
    ln_block(rows(cross), 32, xg, 0, 1, h)
    for k in range(2):
        x_fwd[k].wait_recv()
    ln_block(rows(sibcross), 32, xg, 0, 1, h)

    hr = 2 * 3 * head
    hv = h[...]
    for m in range(n_heads // 2):
        mm = slice(m * hr, (m + 1) * hr)
        qkv[mm, :] = (dot_t(wqkv[mm, :], hv) + bias[mm, :]).astype(BF)

    def position(axis):
        i = lax.broadcasted_iota(jnp.int32, (seq, seq), axis)
        b = i >> 5
        return ((((b & 1) << 1) | (((b >> 1) ^ b) & 1)) << 5) | (i & 31)

    pos_k = position(0)
    causal = pos_k <= position(1)
    key_f = pos_k.astype(F32)
    slopes = alibi_slopes(n_heads * TP)
    score_scale = head ** -0.5

    def part_of(hd, k):
        at = (hd * 3 + k) * head
        return slice(at, at + head)

    def slope(hd):
        v = jnp.float32(slopes[hd])
        for dev in range(1, TP):
            v = jnp.where(t == dev, jnp.float32(slopes[dev * n_heads + hd]), v)
        return v

    for hd in range(n_heads):
        prob[hd] = dot(qkv[part_of(hd, 1), :].T, qkv[part_of(hd, 0), :])
    for hd in range(n_heads):
        s = jnp.where(causal, prob[hd] * score_scale + slope(hd) * key_f, MASK_VALUE)
        e = jnp.exp(s - jnp.max(s, axis=0, keepdims=True))
        pr = e * (1.0 / jnp.sum(e, axis=0, keepdims=True))
        prob[hd] = pr
        probb[hd] = pr.astype(BF)
    for hd in range(n_heads):
        ctx[hd * head:(hd + 1) * head, :] = dot(qkv[part_of(hd, 2), :], probb[hd]).astype(BF)

    class AllSum:
        widths = ALL_CHUNKS

        def __init__(self, p, rd, s, rs, tt, q, e):
            self.p, self.rd, self.s, self.rs, self.tt, self.q, self.e = p, rd, s, rs, tt, q, e
            self.a, self.b, self.c = {}, {}, {}
            self.last = len(self.widths) - 1

        def ch(self, j):
            return cols(self.widths, j)

        def fill(self, j, value):
            self.p[:, self.ch(j)] = value

        def put(self, j):
            self.a[j] = remote(self.p.at[sibhalf, self.ch(j)], self.rd.at[:, self.ch(j)], sib)

        def pair(self, j):
            self.a[j].wait_recv()
            c = self.ch(j)
            self.s[:, c] = (self.p[half, c].astype(F32) + self.rd[:, c].astype(F32)).astype(BF)

        def step_cross(self, j):
            self.pair(j)
            c = self.ch(j)
            self.b[j] = remote(self.s.at[:, c], self.rs.at[:, c], cross)
            if j == self.last:
                self.c[j] = (remote(self.s.at[:, c], self.e.at[:, :], sibcross), remote(self.s.at[:, c], self.q.at[:, :], sib))

        def step_back(self, j):
            self.b[j].wait_recv()
            c = self.ch(j)
            self.tt[half, c] = (self.s[:, c].astype(F32) + self.rs[:, c].astype(F32)).astype(BF)
            if j < self.last:
                self.c[j] = remote(self.tt.at[half, c], self.tt.at[half, c], sib)

        def finish(self, j):
            if j < self.last:
                self.c[j].wait_recv()
            else:
                for copy in self.c[j]:
                    copy.wait_recv()
                self.tt[sibhalf, self.ch(j)] = (self.q[...].astype(F32) + self.e[...].astype(F32)).astype(BF)

    class ScatterSum(AllSum):
        widths = SCATTER_CHUNKS

        def step_cross(self, j):
            self.pair(j)
            c = self.ch(j)
            self.b[j] = remote(self.s.at[blk_cross, c], self.rs.at[:, c], cross)

        def result(self, c):
            return (self.s[blk_own, c].astype(F32) + self.rs[:, c].astype(F32)).astype(BF).astype(F32)

    o_flat = ctx[...].T
    sum_a = AllSum(p1, rd1, s1, rs1, t1, q1, e1)
    n_all = len(ALL_CHUNKS)
    sum_a.fill(0, dot(o_flat, wout[:, sum_a.ch(0)]).astype(BF))
    sum_a.put(0)
    for j in range(1, n_all):
        sum_a.fill(j, dot(o_flat, wout[:, sum_a.ch(j)]).astype(BF))
    for j in range(1, n_all):
        sum_a.put(j)
    for j in range(n_all):
        sum_a.step_cross(j)

    gy_to_sib.wait_recv()
    gy_to_cross.wait_recv()
    gy_fwd = remote(gyg.at[rows(cross), :], gyg.at[rows(cross), :], sib)
    for hd in range(n_heads):
        vt[hd] = qkv[part_of(hd, 2), :].T
    gy_fwd.wait_recv()
    lwdn.wait()
    lwup.wait()
    fw = wdn_h.shape[0] // N_BLK
    shift = None
    acc1 = jnp.zeros((seq, LANES), F32)
    acc2 = jnp.zeros((seq, LANES), F32)

    def x1_chunk(j, shift, acc1, acc2):
        sum_a.finish(j)
        total = jnp.zeros((seq, LANES), F32)
        for c in groups(ALL_CHUNKS, j):
            z = xg[:, lc(c)].astype(F32) + t1[:, lc(c)].astype(F32) + vecs[4, :, lc(c)]
            x1[:, lc(c)] = z
            if j == 0:
                total = total + z
            else:
                d = z - shift
                acc1 = acc1 + d
                acc2 = acc2 + d * d
        if j == 0:
            shift = jnp.sum(total, axis=1, keepdims=True) / (ALL_CHUNKS[0] * LANES)
            for c in groups(ALL_CHUNKS, j):
                d = x1[:, lc(c)] - shift
                acc1 = acc1 + d
                acc2 = acc2 + d * d
        return shift, acc1, acc2

    gyv = gyg[...]
    for j in range(n_all):
        if j < N_BLK:
            ff = slice(j * fw, (j + 1) * fw)
            gact[:, ff] = dot_t(gyv, wdn[ff, :]).astype(BF)
        sum_a.step_back(j)
        if j:
            shift, acc1, acc2 = x1_chunk(j - 1, shift, acc1, acc2)
    shift, acc1, acc2 = x1_chunk(n_all - 1, shift, acc1, acc2)

    off = jnp.sum(acc1, axis=1, keepdims=True) / D
    mean = shift + off
    rstd = lax.rsqrt(jnp.sum(acc2, axis=1, keepdims=True) / D - off * off + EPS)
    halves = (slice(0, seq // 2), slice(seq // 2, seq))
    rstd2 = [rstd[hh] for hh in halves]
    for n, hh in enumerate(halves):
        for c in range(nlc):
            z = (x1[hh, lc(c)] - mean[hh]) * rstd2[n]
            xhat[hh, lc(c)] = z
            g[hh, lc(c)] = (z * vecs[2, :, lc(c)] + vecs[3, :, lc(c)]).astype(BF)

    gv = g[...]
    for j in range(N_BLK):
        ff = slice(j * fw, (j + 1) * fw)
        pre = dot(gv, wup[:, ff]) + vecs[6, :, ff]
        w = (GELU_C * GELU_A) * (pre * pre)
        th = jnp.tanh(pre * (GELU_C + w))
        hp = 0.5 * pre
        r[:, ff] = (hp + hp * th).astype(BF)
        slope_g = (0.5 + 0.5 * th) + (hp * (1.0 - th * th)) * (GELU_C + 3.0 * w)
        gp = gact[:, ff].astype(F32) * slope_g
        vec[6, :, ff] = jnp.sum(gp, axis=0, keepdims=True)
        dpre[:, ff] = gp.astype(BF)

    dv = dpre[...]
    n_before = len(sent)
    sum_g = AllSum(p2, rd2, s2, rs2, t2, q2, e2)
    for j in range(n_all):
        for c in [lc(c) for c in groups(ALL_CHUNKS, j)] if j == 0 else [sum_g.ch(j)]:
            p2[:, c] = dot_t(dv, wup[c, :]).astype(BF)
        sum_g.put(j)
        if j:
            sum_g.step_cross(j - 1)
    sum_g.step_cross(n_all - 1)

    sends_done(n_before)
    acc1 = jnp.zeros((seq, LANES), F32)
    acc2 = jnp.zeros((seq, LANES), F32)

    def ln2_back_chunk(j, acc1, acc2):
        sum_g.finish(j)
        for c in groups(ALL_CHUNKS, j):
            dg = t2[:, lc(c)].astype(F32)
            z = xhat[:, lc(c)]
            dgz = dg * z
            vec[2, :, lc(c)] = jnp.sum(dgz, axis=0, keepdims=True)
            vec[3, :, lc(c)] = jnp.sum(dg, axis=0, keepdims=True)
            gain = vecs[2, :, lc(c)]
            dz = dg * gain
            acc1 = acc1 + dz
            acc2 = acc2 + dgz * gain
            for n, hh in enumerate(halves):
                ubuf[hh, lc(c)] = gyg[hh, lc(c)].astype(F32) + rstd2[n] * dz[hh]
        return acc1, acc2

    yw = D // N_BLK

    def down(j):
        yy = slice(j * yw, (j + 1) * yw)
        py[:, yy] = dot(r[...], wdn[:, yy]).astype(BF)
        for c in range(j * (yw // LANES), (j + 1) * (yw // LANES)):
            gt[lc(c), :] = g[:, lc(c)].T
            rt[lc(c), :] = r[:, lc(c)].T
            vec[5, :, lc(c)] = jnp.sum(gyg[:, lc(c)].astype(F32), axis=0, keepdims=True)
            for n, hh in enumerate(halves):
                xr[hh, lc(c)] = xhat[hh, lc(c)] * rstd2[n]

    def grad_down(m):
        mm = slice(m * GRAD_ROWS, (m + 1) * GRAD_ROWS)
        wdn[mm, :] = dot(rt[mm, :], gyg[...]).astype(BF)

    work = [(down, k) for k in range(N_BLK)] + [(grad_down, m) for m in range(wdn.shape[0] // GRAD_ROWS)]
    for j in range(n_all):
        for step, m in work[WORK_CUTS[j]:WORK_CUTS[j + 1]]:
            step(m)
        if j == 1:
            y_sib = remote(py.at[sibhalf, :], rdy, sib)
        sum_g.step_back(j)
        if j:
            acc1, acc2 = ln2_back_chunk(j - 1, acc1, acc2)
    y_sib.wait_recv()
    sy[...] = (py[half, :].astype(F32) + rdy[...].astype(F32)).astype(BF)
    y_cross = remote(sy.at[blk_cross, :], rsy, cross)
    acc1, acc2 = ln2_back_chunk(n_all - 1, acc1, acc2)

    for n, hh in enumerate(halves):
        mean1 = rstd2[n] * (jnp.sum(acc1[hh], axis=1, keepdims=True) / D)
        mean2 = jnp.sum(acc2[hh], axis=1, keepdims=True) / D
        for c in range(nlc):
            gm = ubuf[hh, lc(c)] - (mean1 + xr[hh, lc(c)] * mean2)
            gmid[hh, lc(c)] = gm
            ga[hh, lc(c)] = gm.astype(BF)

    gav = ga[...]
    hc = ctx.shape[0] // 2
    for k in range(2):
        dctx[k * hc:(k + 1) * hc, :] = dot_t(wout[k * hc:(k + 1) * hc, :], gav).astype(BF)

    def head_rows(hd):
        return slice(hd * head, (hd + 1) * head)

    for hd in range(n_heads):
        dpb[hd] = dot(vt[hd], dctx[head_rows(hd), :]).astype(BF)
    for hd in range(n_heads):
        dqkv[part_of(hd, 2), :] = dot_t(dctx[head_rows(hd), :], probb[hd]).astype(BF)
    for hd in range(n_heads):
        pr = prob[hd]
        dp = dpb[hd].astype(F32)
        dsb[hd] = (pr * (dp - jnp.sum(dp * pr, axis=0, keepdims=True))).astype(BF)
    for hd in range(n_heads):
        dqkv[part_of(hd, 0), :] = (dot(qkv[part_of(hd, 1), :], dsb[hd]) * score_scale).astype(BF)
        dqkv[part_of(hd, 1), :] = (dot_t(qkv[part_of(hd, 0), :], dsb[hd]) * score_scale).astype(BF)

    n_before = len(sent)
    sum_h = ScatterSum(ph, rdh, sh, rsh, None, None, None)
    n_scat = len(SCATTER_CHUNKS)
    dq = dqkv[...].T
    for j in range(n_scat):
        for c in [lc(c) for c in groups(SCATTER_CHUNKS, j)] if j == 0 else [sum_h.ch(j)]:
            ph[:, c] = dot(dq, wqkv[:, c]).astype(BF)
        sum_h.put(j)
        if j:
            sum_h.step_cross(j - 1)
    sum_h.step_cross(n_scat - 1)

    rstd1 = ln_block(own, 32, xg, 0, 1, None)
    y_cross.wait_recv()
    for c in range(nlc):
        z = (sy[blk_own, lc(c)].astype(F32) + rsy[:, lc(c)].astype(F32)).astype(BF).astype(F32)
        ybuf[:, lc(c)] = (x1[own, lc(c)] + z + vecs[5, :, lc(c)]).astype(BF)
        vec[4, :, lc(c)] = jnp.sum(gmid[:, lc(c)], axis=0, keepdims=True)

    me = slot(t)
    acc1 = jnp.zeros((32, LANES), F32)
    acc2 = jnp.zeros((32, LANES), F32)
    parts = []
    for step, m in work[WORK_CUTS[-1]:]:
        step(m)
    sends_done(n_before)
    for j in range(n_scat):
        sum_h.b[j].wait_recv()
        for c in groups(SCATTER_CHUNKS, j):
            dh = sum_h.result(lc(c))
            z = xh1[:, lc(c)]
            dhz = dh * z
            part_o[me, 0:1, lc(c)] = jnp.sum(dhz, axis=0, keepdims=True)
            part_o[me, 1:2, lc(c)] = jnp.sum(dh, axis=0, keepdims=True)
            gain = vecs[0, :, lc(c)]
            acc1 = acc1 + dh * gain
            acc2 = acc2 + dhz * gain
        if j >= n_scat - 2:
            c = slice(0, sum_h.ch(j).stop) if j == n_scat - 2 else sum_h.ch(j)
            parts += [remote(part_o.at[me, :, c], part_o.at[me, :, c], dev) for dev in (cross, sibcross, sib)]
    mean1 = jnp.sum(acc1, axis=1, keepdims=True) / D
    mean2 = jnp.sum(acc2, axis=1, keepdims=True) / D
    for c in range(nlc):
        dz = sum_h.result(lc(c)) * vecs[0, :, lc(c)]
        gxbuf[:, lc(c)] = (gmid[own, lc(c)] + rstd1 * (dz - mean1 - xh1[:, lc(c)] * mean2)).astype(BF)
    sends_done(len(sent))
    for copy in parts:
        copy.wait_recv()


def grad_kernel(h, ga, dpre, dqkv, ctx, gt, dwdn, vec, part, y, gx,
                dwqkv_o, dwout_o, dwup_o, dwdn_o, dbqkv_o, y_o, gx_o, v0, v1, v2, v3, v4, v5, v6,
                buf, small, sums, bq, osem, ssem):
    n_heads, head = dbqkv_o.shape[1], dbqkv_o.shape[2]
    slots, block = buf.shape[0], buf.shape[1]
    tail = []

    def piece(k, start, size):
        small[k, pl.ds(0, size), :] = dot(ctx[start:start + size, :], ga[...]).astype(BF)
        copy = pltpu.make_async_copy(small.at[k, pl.ds(0, size), :], dwout_o.at[pl.ds(start, size), :], ssem.at[k])
        copy.start()
        tail.append(copy)

    def written(slot, out):
        return pltpu.make_async_copy(buf.at[slot], out.at[pl.ds(0, block), :], osem.at[slot])

    for k in range(4):
        n = dwdn.shape[0] // 4
        copy = pltpu.make_async_copy(dwdn.at[pl.ds(k * n, n), :], dwdn_o.at[pl.ds(k * n, n), :], ssem.at[14 + k])
        copy.start()
        tail.append(copy)
    piece(0, 0, 160)
    for k in range(2):
        sums[k] = (part[0, k:k + 1, :] + part[1, k:k + 1, :]) + (part[2, k:k + 1, :] + part[3, k:k + 1, :])

    def send(src, dst):
        copy = pltpu.make_async_copy(src, dst, ssem.at[len(tail) - 2])
        copy.start()
        tail.append(copy)

    send(y, y_o)
    send(gx, gx_o)
    for k, o in enumerate((v2, v3, v4, v5, v6)):
        send(vec.at[k + 2, 0], o)
    for k, o in enumerate((v0, v1)):
        send(sums.at[k, 0], o)
    first = 0
    for left, right, out in ((gt, dpre, dwup_o), (dqkv, h, dwqkv_o)):

        def body(m, carry, left=left, right=right, out=out, first=first):
            slot = lax.rem(first + m, slots)

            @pl.when(first + m >= slots)
            def _():
                written(slot, out).wait()

            at = pl.ds(pl.multiple_of(m * block, block), block)
            buf[slot] = dot(left[at, :], right[...]).astype(BF)
            pltpu.make_async_copy(buf.at[slot], out.at[at, :], osem.at[slot]).start()
            return carry

        count = left.shape[0] // block
        lax.fori_loop(0, count, body, 0)
        first += count
    piece(1, 160, 320)
    ones = jnp.ones((8, dqkv.shape[1]), BF)
    total = dot_t(ones, dqkv[...])[0:1]
    for k in range(3):
        for hd in range(n_heads):
            at = (hd * 3 + k) * head
            bq[k, hd:hd + 1, :] = total[:, at:at + head]
    send(bq, dbqkv_o)
    piece(2, 480, 160)
    for k in range(slots):
        written(k, dwqkv_o).wait()
    for copy in tail:
        copy.wait()


def solution(mesh):
    def local_step(x, ln1_gamma, ln1_beta, w_qkv, b_qkv, w_out, b_out, ln2_gamma, ln2_beta, w_up, b_up, w_down, b_down, grad_y):
        D = x.shape[2]
        S = TP * x.shape[1]
        nh, head = w_qkv.shape[1], w_qkv.shape[3]
        Q = nh * 3 * head
        C = nh * head
        FL = w_up.shape[1]
        any_spec = pl.BlockSpec(memory_space=pl.ANY)
        vspec = pl.BlockSpec(memory_space=pltpu.VMEM)
        vm = pltpu.VMEM
        wqkv_t = jnp.transpose(w_qkv, (1, 2, 3, 0)).reshape(Q, D)
        bq = jnp.transpose(b_qkv, (1, 0, 2))
        sds = jax.ShapeDtypeStruct
        n_loads = 2 + 7 + 1 + 4
        red = [vm((S, D), BF), vm((S // 2, D), BF), vm((S // 2, D), BF), vm((S // 2, D), BF), vm((S, D), BF),
               vm((S // 2, ALL_CHUNKS[-1] * LANES), BF), vm((S // 2, ALL_CHUNKS[-1] * LANES), BF)]
        scat = [vm((S, D), BF), vm((S // 2, D), BF), vm((S // 2, D), BF), vm((S // TP, D), BF)]
        row = lambda v: v
        res = pl.pallas_call(
            layer_kernel,
            name='layer',
            out_shape=[vm((S // TP, D), BF), vm((S // TP, D), BF), vm((7, 1, D), F32), vm((TP, 2, D), F32), vm((S, D), BF), vm((S, D), BF),
                       vm((S, FL), BF), vm((Q, S), BF), vm((C, S), BF), vm((D, S), BF), vm((FL, D), BF)],
            in_specs=[any_spec] * 14,
            out_specs=[vspec] * 11,
            scratch_shapes=[
                vm((Q, D), BF), vm((C, D), BF), vm((D, FL), BF), vm((FL, S), BF), vm((3, nh, head), F32), vm((7, 1, D), F32),
                vm((S, D), BF), vm((S, D), BF), vm((Q, S), F32), vm((Q, S), BF), vm((nh, S, S), F32),
                vm((nh, S, S), BF), vm((S, D), F32), vm((S, D), F32), vm((S, D), BF),
                vm((S, FL), BF), vm((S, FL), BF), vm((S, D), F32), vm((C, S), BF),
                vm((S // TP, D), F32), vm((S, D), F32), vm((S, D), F32),
                vm((nh, S, head), BF), vm((nh, S, S), BF), vm((nh, S, S), BF),
                *red, *red, *scat, *scat,
                pltpu.SemaphoreType.DMA((n_loads,)),
                pltpu.SemaphoreType.DMA((N_SEND,)), pltpu.SemaphoreType.DMA((N_REMOTE,)),
            ],
            compiler_params=pltpu.CompilerParams(collective_id=0, has_side_effects=True, vmem_limit_bytes=LAYER_VMEM),
        )(x.reshape(x.shape[1], D), grad_y.reshape(x.shape[1], D), wqkv_t, bq, w_out, w_up, w_down, row(ln1_gamma), row(ln1_beta),
          row(ln2_gamma), row(ln2_beta), row(b_out), row(b_down), row(b_up))
        y, gx, vec, part, h, ga, dpre, dqkv, ctx, gt, dwdn = res
        vshape = sds((D,), F32)
        outs = pl.pallas_call(
            grad_kernel,
            name='weight_grads',
            out_shape=[sds((Q, D), BF), sds((C, D), BF), sds((D, FL), BF), sds((FL, D), BF), sds((3, nh, head), F32),
                       sds((S // TP, D), BF), sds((S // TP, D), BF)] + [vshape] * 7,
            in_specs=[vspec] * 11,
            out_specs=[any_spec] * 14,
            scratch_shapes=[
                vm((3, 640, D), BF), vm((3, 320, D), BF), vm((2, 1, D), F32), vm((3, nh, head), F32),
                pltpu.SemaphoreType.DMA((3,)), pltpu.SemaphoreType.DMA((18,)),
            ],
            compiler_params=pltpu.CompilerParams(vmem_limit_bytes=GRAD_VMEM),
        )(h, ga, dpre, dqkv, ctx, gt, dwdn, vec, part, y, gx)
        dwqkv, dwout, dwup, dwdn, dbqkv, y, gx, g_ln1g, g_ln1b, g_ln2g, g_ln2b, g_bout, g_bdown, g_bup = outs
        dwqkv = jnp.transpose(dwqkv.reshape(nh, 3, head, D), (3, 0, 1, 2))
        dbqkv = jnp.transpose(dbqkv, (1, 0, 2))
        return (y.reshape(x.shape), gx.reshape(x.shape), g_ln1g, g_ln1b, dwqkv, dbqkv, dwout, g_bout,
                g_ln2g, g_ln2b, dwup, g_bup, dwdn, g_bdown)

    row_spec = P('dp', 'tp', None)
    in_specs = (row_spec, P(), P(), P(None, 'tp', None, None), P('tp', None, None), P('tp', None), P(), P(), P(),
                P(None, 'tp'), P('tp'), P('tp', None), P(), row_spec)
    out_specs = (row_spec, row_spec, P('dp'), P('dp'), P('dp', 'tp', None, None), P(('dp', 'tp'), None, None),
                 P(('dp', 'tp'), None), P('dp'), P('dp'), P('dp'), P('dp', 'tp'), P(('dp', 'tp')), P(('dp', 'tp'), None), P('dp'))
    return jax.shard_map(local_step, mesh=mesh, in_specs=in_specs, out_specs=out_specs, check_vma=False)
```
